128 devices in a mesh: ka: 16 (over x_hi, z, core), band: 8 (over x_lo, y).
Axes of the slice: x: 4 (x_hi: 2, x_lo: 2; x = x_hi * 2 + x_lo), y: 4, z: 4, core: 2. Of those that a mesh axis runs over, the one named last changes fastest.
Arguments:
- occ_rows: bfloat16 [16, 2048, 128], P('ka', 'band'), may hold values from -0.5 to 0.5
- vir_rows: bfloat16 [16, 2048, 896], P('ka', 'band'), may hold values from -0.1875 to 0.1875
- trial_vectors: float32 [16, 2, 128, 896], P('ka', None, None, 'band'), may hold values from -6 to 6
- occ_energy: float32 [16, 128], P('ka'), may hold values from -1.2 to -0.3
- vir_energy: float32 [16, 896], P('ka', 'band'), may hold values from 0.1 to 1.5
- coulomb: bfloat16 [2048, 2048], P('band'), may hold values from -0.0625 to 0.0625
- exch_kernel: bfloat16 [16, 2048, 2048], P(None, 'band'), as said below
- minus_table: int32 [16, 16], replicated, may hold values from 0 to 15, as said below
Outputs:
- sigma_vectors: float32 [16, 2, 128, 896], P('ka', None, None, 'band')
The draws below stay inside these ranges and needn't reach their ends.
Inputs may be any that keep to these rules, and one draw needn't show every extreme that they name: minus_table[k, q] is the k-point k - q on a group of 16 k-points: every row and every column holds each index once, and one q gives minus_table[k, q] == k for every k. Each exch_kernel[q] is symmetric.
All inputs are finite; a program needn't handle non-finite values.
Results may differ from the reference program's by a relative error of at most 0.0051.
Values may be sent and summed in bfloat16 or wider, within the bound.
A program may use at most 128 MiB of HBM per device.

```python
import jax
import jax.numpy as jnp
from jax import lax

NOCC = 128
NVIR = 896
NAUX = 2048
NVEC = 2
NK = 16


def draw_minus_table(key, part):
    labels = jax.random.permutation(jax.random.fold_in(key, 11), NK).astype(jnp.int32)
    difference = (labels[:, None] - labels[None, :]) % NK
    inverse = jnp.argsort(labels).astype(jnp.int32)
    return inverse[difference].astype(jnp.int32)


def draw_exch_kernel(key, part):
    spread = jnp.sqrt(jnp.float32(NOCC) / jnp.float32(NK * NAUX))
    base = jax.random.normal(jax.random.fold_in(key, 3), (NK, NAUX, NAUX), jnp.float32)
    symmetric = (base + jnp.transpose(base, (0, 2, 1))) * 0.7071
    return (symmetric * spread).astype(jnp.bfloat16)


def levels(stream_key, shape, split, smallest, high):
    factor_of = 1.0
    for position, blocks in split:
        draws = jax.random.uniform(jax.random.fold_in(jax.random.fold_in(stream_key, 6), position), (blocks,), jnp.float32, smallest / len(split), high / len(split))
        factor_of = factor_of * jnp.repeat(jnp.exp(draws), shape[position] // blocks).reshape((-1,) + (1,) * (len(shape) - 1 - position))
    return factor_of


def normal_values(key, shape, scale, reach, shards=(), held_as=jnp.bfloat16):
    result = scale * jax.random.normal(key, shape, jnp.float32)
    if shards:
        result = result * levels(key, shape, shards, -0.22, 0.18)
    return jnp.clip(result, -reach, reach).astype(held_as)


def setup_inputs(seed: int = 0) -> dict:
    key_list = jax.random.split(jax.random.key(seed), 9)
    occ_rows = normal_values(key_list[0], (NK, NAUX, NOCC), NOCC ** -0.5, 0.5, ((0, 16), (1, 8)))
    vir_rows = normal_values(key_list[1], (NK, NAUX, NVIR), NVIR ** -0.5, 0.1875, ((0, 16), (1, 8)))
    trial_vectors = normal_values(key_list[2], (NK, NVEC, NOCC, NVIR), 1.0, 6.0, ((0, 16), (3, 8)), jnp.float32)
    occ_energy = jnp.clip(-1.2 + 0.90000004 * jax.random.uniform(key_list[3], (NK, NOCC), jnp.float32) ** levels(key_list[3], (NK, NOCC), ((0, 16),), -0.2, 0.2), -1.2, -0.3)
    vir_energy = jnp.clip(0.1 + 1.4 * jax.random.uniform(key_list[4], (NK, NVIR), jnp.float32) ** levels(key_list[4], (NK, NVIR), ((0, 16), (1, 8)), -0.2, 0.2), 0.1, 1.5)
    coulomb = normal_values(key_list[5], (NAUX, NAUX), (NK * NAUX // 4) ** -0.5, 0.0625, ((0, 8),))
    exch_kernel = draw_exch_kernel(jax.random.fold_in(key_list[8], 71), 0)
    minus_table = draw_minus_table(jax.random.fold_in(key_list[8], 71), 0)
    return dict(occ_rows=occ_rows, vir_rows=vir_rows, trial_vectors=trial_vectors, occ_energy=occ_energy, vir_energy=vir_energy, coulomb=coulomb, exch_kernel=exch_kernel, minus_table=minus_table)


def reference(occ_rows, vir_rows, trial_vectors, occ_energy, vir_energy, coulomb, exch_kernel, minus_table):
    highest = lax.Precision.HIGHEST
    trial_half = trial_vectors.astype(jnp.bfloat16)

    def build_pairs(kpoint):
        occ_here = occ_rows[kpoint].astype(jnp.float32)
        vir_here = vir_rows[kpoint].astype(jnp.float32)
        mixed_rows = jnp.einsum("ri,via->vra", occ_here, trial_half[kpoint].astype(jnp.float32), precision=highest)
        mixed_rows = mixed_rows.astype(jnp.bfloat16)
        pair_block = jnp.einsum("vra,na->vrn", mixed_rows.astype(jnp.float32), vir_here, precision=highest)
        density_here = jnp.sum(mixed_rows.astype(jnp.float32) * vir_here[None], axis=2)
        return pair_block.astype(jnp.bfloat16), density_here

    pair_blocks, densities = lax.map(build_pairs, jnp.arange(NK, dtype=jnp.int32))
    density_half = jnp.sum(densities, axis=0).astype(jnp.bfloat16)
    potential = jnp.einsum("vn,rn->vr", density_half.astype(jnp.float32), coulomb.astype(jnp.float32), precision=highest)

    def build_sigma(kpoint):
        def add_transfer(running, momentum):
            source = minus_table[kpoint, momentum]
            weighted = pair_blocks[source].astype(jnp.float32) * exch_kernel[momentum].astype(jnp.float32)[None]
            return running + weighted, None

        screened, unused = lax.scan(add_transfer, jnp.zeros((NVEC, NAUX, NAUX), jnp.float32), jnp.arange(NK, dtype=jnp.int32))
        screened = screened.astype(jnp.bfloat16)
        vir_here = vir_rows[kpoint].astype(jnp.float32)
        product = jnp.einsum("vrn,na->vra", screened.astype(jnp.float32), vir_here, precision=highest)
        weights = (2.0 * potential[:, :, None] * vir_here[None] - product).astype(jnp.bfloat16)
        coupled = jnp.einsum("ri,vra->via", occ_rows[kpoint].astype(jnp.float32), weights.astype(jnp.float32), precision=highest)
        energy_gaps = vir_energy[kpoint][None, :] - occ_energy[kpoint][:, None]
        return energy_gaps[None] * trial_vectors[kpoint] + coupled

    return lax.map(build_sigma, jnp.arange(NK, dtype=jnp.int32))
```

```python
import jax
import jax.numpy as jnp
from jax import lax
from jax.experimental import pallas as pl
from jax.experimental.pallas import tpu as pltpu
from jax.sharding import PartitionSpec as P

BF = jnp.bfloat16
F32 = jnp.float32
MESH = pl.DeviceIdType.MESH


def each(count, body):
    def step(i, carry):
        body(i)
        return carry

    lax.fori_loop(0, count, step, 0)


def rdma(src, dst, send, recv, ka, band):
    return pltpu.make_async_remote_copy(
        src_ref=src,
        dst_ref=dst,
        send_sem=send,
        recv_sem=recv,
        device_id={"ka": ka, "band": band},
        device_id_type=MESH,
    )


def kernel(
    minus, trial, occ, vir, coulomb, exch, out,
    trial_bf, trial_all, vir_x, occ_x, vir_t, t_all, occ_c, k_bf, k_f, pairs, s_bf, u_send, u_recv,
    dens1, dens2, coul, sig_send, sig_recv,
    tri_s, tri_r, x_s, x_r, o1_s, o1_r, o2_s, o2_r, o3_s, o3_r, t_s, t_r, d1_s, d1_r, d2_s, d2_r,
    u_s, u_r, g_s, g_r, loc,
):
    bands = lax.axis_size("band")
    chips = lax.axis_size("ka") // 2
    ka = lax.axis_index("ka")
    b = lax.axis_index("band")
    j = ka // 2
    c = lax.rem(ka, 2)
    o = 1 - c
    mine = 2 * j + c
    other = 2 * j + o
    rows, nocc = occ.shape
    width = trial.shape[1]
    nk = exch.shape[0]
    slab = rows // bands

    def band_peer(i):
        return lax.rem(b + 1 + i, bands)

    def chip_peer(i):
        return lax.rem(j + 1 + i, chips)

    load_k = pltpu.make_async_copy(
        exch.at[:, :, pl.ds(pl.multiple_of(j * rows, rows), rows)], k_bf, loc.at[0]
    )
    load_k.start()
    load_c = pltpu.make_async_copy(coulomb, coul, loc.at[1])
    load_c.start()

    barrier = pltpu.get_barrier_semaphore()

    def greet(k, band):
        pl.semaphore_signal(barrier, inc=1, device_id={"ka": k, "band": band}, device_id_type=MESH)

    def greet_band(i):
        greet(mine, band_peer(i))
        greet(other, band_peer(i))

    each(bands - 1, greet_band)
    greet(other, b)
    each(chips - 1, lambda i: greet(2 * chip_peer(i) + c, b))
    each(chips - 1, lambda i: greet(2 * chip_peer(i) + c, j))

    @pl.when(j != b)
    def _():
        greet(mine, j)

    trial_bf[...] = trial[...].astype(BF)
    callers = 2 * (bands - 1) + 1 + 2 * (chips - 1)
    pl.semaphore_wait(barrier, jnp.where(j == b, callers, callers + 1))

    own_cols = pl.ds(pl.multiple_of(b * width, 16), width)

    def tri_same(i):
        return rdma(trial_bf.at[c], trial_all.at[0, own_cols], tri_s.at[0, i], tri_r.at[0, b], mine, band_peer(i))

    def tri_cross(i):
        return rdma(trial_bf.at[o], trial_all.at[1, own_cols], tri_s.at[1, i], tri_r.at[1, b], other, lax.rem(b + i, bands))

    each(bands - 1, lambda i: tri_same(i).start())
    each(bands, lambda i: tri_cross(i).start())
    trial_all[0, own_cols, :] = trial_bf[c]

    def occ1(i):
        part = pl.ds(pl.multiple_of(i * slab, slab), slab)
        return rdma(occ.at[part], occ_c.at[c, j, part], o1_s.at[i], o1_r.at[j], 2 * b + c, i)

    def occ1_start(i):
        @pl.when((i != b) | (j != b))
        def _():
            occ1(i).start()

    each(bands, occ1_start)
    own_slab = pl.ds(pl.multiple_of(b * slab, slab), slab)

    @pl.when(j == b)
    def _():
        occ_c[c, j, own_slab, :] = occ[own_slab, :]

    send_vir = rdma(vir, vir_x, x_s.at[0], x_r.at[0], other, b)
    send_occ = rdma(occ, occ_x, x_s.at[1], x_r.at[1], other, b)
    send_vir.start()
    send_occ.start()

    def occ1_wait(i):
        @pl.when((i != j) | (j != b))
        def _():
            rdma(occ.at[own_slab], occ_c.at[c, i, own_slab], o1_s.at[i], o1_r.at[i], mine, i).wait_recv()

    each(chips, occ1_wait)

    def occ2(i):
        return rdma(
            occ_c.at[c, :, own_slab], occ_c.at[c, :, own_slab], o2_s.at[i], o2_r.at[b], mine, band_peer(i)
        )

    each(bands - 1, lambda i: occ2(i).start())

    send_vir.wait_recv()
    send_occ.wait_recv()
    vir_t[0] = vir[...].T
    vir_t[1] = vir_x[...].T

    def tri_wait(i):
        p = band_peer(i)
        cols = pl.ds(pl.multiple_of(p * width, 16), width)
        rdma(trial_bf.at[c], trial_all.at[0, cols], tri_s.at[0, i], tri_r.at[0, p], mine, p).wait_recv()

    def tri_wait_cross(i):
        cols = pl.ds(pl.multiple_of(i * width, 16), width)
        rdma(trial_bf.at[o], trial_all.at[1, cols], tri_s.at[1, i], tri_r.at[1, i], other, i).wait_recv()

    each(bands - 1, tri_wait)
    each(bands, tri_wait_cross)

    t_own = jnp.dot(vir[...], trial_all[0], preferred_element_type=F32)
    t_oth = jnp.dot(vir_x[...], trial_all[1], preferred_element_type=F32)
    t_all[mine] = t_own.astype(BF)
    t_all[other] = t_oth.astype(BF)
    pair_of = pl.ds(2 * j, 2)

    def t_copy(i):
        return rdma(t_all.at[pair_of], t_all.at[pair_of], t_s.at[i], t_r.at[j], 2 * chip_peer(i) + c, b)

    each(chips - 1, lambda i: t_copy(i).start())

    local = occ[...].astype(F32) * t_own + occ_x[...].astype(F32) * t_oth
    high = local.astype(BF)
    low = (local - high.astype(F32)).astype(BF)
    ones = jnp.ones((8, nocc), BF)
    along = (((1,), (1,)), ((), ()))
    dens1[j] = lax.dot_general(ones, high, along, preferred_element_type=F32) + lax.dot_general(
        ones, low, along, preferred_element_type=F32
    )

    def d1_copy(i):
        return rdma(dens1.at[j], dens1.at[j], d1_s.at[i], d1_r.at[j], 2 * chip_peer(i) + c, b)

    each(chips - 1, lambda i: d1_copy(i).start())

    load_k.wait()

    def widen(q):
        k_f[q] = k_bf[q].astype(F32)

    each(nk, widen)

    def occ2_wait(i):
        p = band_peer(i)
        part = pl.ds(pl.multiple_of(p * slab, slab), slab)
        rdma(occ_c.at[c, :, part], occ_c.at[c, :, part], o2_s.at[i], o2_r.at[p], mine, p).wait_recv()

    each(bands - 1, occ2_wait)
    occ3 = rdma(occ_c.at[c], occ_c.at[c], o3_s, o3_r, other, b)
    occ3.start()
    rdma(occ_c.at[c], occ_c.at[o], o3_s, o3_r, other, b).wait_recv()

    def pairs_of(p):
        for s in range(2):
            pairs[2 * p + s] = lax.dot_general(t_all[2 * p + s], occ_c[s, p], along, preferred_element_type=F32)

    pairs_of(j)

    def t_arrived(i):
        p = chip_peer(i)
        part = pl.ds(2 * p, 2)
        rdma(t_all.at[part], t_all.at[part], t_s.at[i], t_r.at[p], 2 * p + c, b).wait_recv()
        pairs_of(p)

    each(chips - 1, t_arrived)

    def d1_wait(i):
        p = chip_peer(i)
        rdma(dens1.at[p], dens1.at[p], d1_s.at[i], d1_r.at[p], 2 * p + c, b).wait_recv()

    each(chips - 1, d1_wait)
    total = dens1[0]
    for p in range(1, chips):
        total = total + dens1[p]
    dens2[b] = total

    def d2_copy(i):
        return rdma(dens2.at[b], dens2.at[b], d2_s.at[i], d2_r.at[b], mine, band_peer(i))

    each(bands - 1, lambda i: d2_copy(i).start())

    tile = 32
    fours = 4

    def screen(g):
        ks = []
        for n in range(fours):
            dest = j ^ (chips - 1 - 2 * g - n // 2)
            ks.append(2 * dest + n % 2)

        def rows_step(r):
            part = pl.ds(pl.multiple_of(r * tile, tile), tile)
            acc = [jnp.zeros((tile, rows), F32) for _ in ks]
            for q in range(nk):
                weight = k_f[q, part, :]
                for n, k in enumerate(ks):
                    acc[n] = acc[n] + pairs[minus[k, q], part, :] * weight
            for n in range(fours):
                s_bf[n, part, :] = acc[n].astype(BF)

        each(rows // tile, rows_step)
        for n, k in enumerate(ks):
            dest = k // 2
            u_send[k] = jnp.dot(s_bf[n], occ_c[n % 2, dest], preferred_element_type=F32).astype(BF)
            if n % 2 == 1:

                @pl.when(dest != j)
                def _():
                    u_copy(dest).start()

    def u_copy(dest):
        return rdma(u_send.at[pl.ds(2 * dest, 2)], u_recv.at[j], u_s.at[dest], u_r.at[j], 2 * dest + c, b)

    each(nk // fours, screen)

    def d2_wait(i):
        p = band_peer(i)
        rdma(dens2.at[p], dens2.at[p], d2_s.at[i], d2_r.at[p], mine, p).wait_recv()

    each(bands - 1, d2_wait)
    load_c.wait()
    pot = jnp.zeros((rows, nocc), F32)
    for p in range(bands):
        row = dens2[p][0:1, :].astype(BF)
        line = jnp.broadcast_to(row, (nocc, rows))
        pot = pot + lax.dot_general(coul[:, p * rows : (p + 1) * rows], line, along, preferred_element_type=F32)
    pot = pot * 2.0
    k_f[0, :, 0:nocc] = pot * occ[...].astype(F32) - u_send[mine].astype(F32)
    k_f[1, :, 0:nocc] = pot * occ_x[...].astype(F32) - u_send[other].astype(F32)

    def u_arrived(i):
        p = chip_peer(i)
        rdma(u_send.at[pl.ds(2 * p, 2)], u_recv.at[p], u_s.at[p], u_r.at[p], 2 * p + c, b).wait_recv()
        k_f[0, :, 0:nocc] = k_f[0, :, 0:nocc] - u_recv[p, c].astype(F32)
        k_f[1, :, 0:nocc] = k_f[1, :, 0:nocc] - u_recv[p, o].astype(F32)

    each(chips - 1, u_arrived)

    for s in range(2):
        sig_send[s] = jnp.dot(vir_t[s], k_f[s, :, 0:nocc].astype(BF), preferred_element_type=F32).astype(BF)

    def sig_same(i):
        p = band_peer(i)
        cols = pl.ds(pl.multiple_of(p * width, 16), width)
        return rdma(sig_send.at[0, cols], sig_recv.at[c, b], g_s.at[0, i], g_r.at[c, b], mine, p)

    def sig_cross(i):
        p = lax.rem(b + i, bands)
        cols = pl.ds(pl.multiple_of(p * width, 16), width)
        return rdma(sig_send.at[1, cols], sig_recv.at[c, b], g_s.at[1, i], g_r.at[c, b], other, p)

    each(bands - 1, lambda i: sig_same(i).start())
    each(bands, lambda i: sig_cross(i).start())
    sig_recv[c, b] = sig_send[0, own_cols, :]

    def sig_wait(i):
        p = band_peer(i)
        rdma(sig_send.at[0, own_cols], sig_recv.at[c, p], g_s.at[0, i], g_r.at[c, p], mine, p).wait_recv()

    def sig_wait_cross(i):
        rdma(sig_send.at[1, own_cols], sig_recv.at[o, i], g_s.at[1, i], g_r.at[o, i], other, i).wait_recv()

    each(bands - 1, sig_wait)
    each(bands, sig_wait_cross)
    for v in range(2):
        sums = sig_recv[v, 0].astype(F32)
        for p in range(1, bands):
            sums = sums + sig_recv[v, p].astype(F32)
        out[v] = sums

    each(bands - 1, lambda i: tri_same(i).wait_send())
    each(bands, lambda i: tri_cross(i).wait_send())

    def occ1_sent(i):
        @pl.when((i != b) | (j != b))
        def _():
            occ1(i).wait_send()

    each(bands, occ1_sent)
    send_vir.wait_send()
    send_occ.wait_send()
    each(bands - 1, lambda i: occ2(i).wait_send())
    occ3.wait_send()
    each(chips - 1, lambda i: t_copy(i).wait_send())
    each(chips - 1, lambda i: d1_copy(i).wait_send())
    each(bands - 1, lambda i: d2_copy(i).wait_send())
    each(chips - 1, lambda i: u_copy(chip_peer(i)).wait_send())
    each(bands - 1, lambda i: sig_same(i).wait_send())
    each(bands, lambda i: sig_cross(i).wait_send())


def solution(mesh):
    bands = mesh.shape["band"]
    chips = mesh.shape["ka"] // 2

    def per_device(occ, vir, trial, occ_energy, vir_energy, coulomb, exch, minus):
        nk, rows, aux = exch.shape
        nocc = occ.shape[2]
        nvir = vir.shape[2]
        width = trial.shape[3]
        turned = jnp.transpose(trial[0], (0, 2, 1))
        vmem = pl.BlockSpec(memory_space=pltpu.VMEM)
        far = pl.BlockSpec(memory_space=pl.ANY)
        dma = pltpu.SemaphoreType.DMA
        coupled = pl.pallas_call(
            kernel,
            out_shape=jax.ShapeDtypeStruct((2, width, nocc), F32),
            in_specs=[pl.BlockSpec(memory_space=pltpu.SMEM), vmem, vmem, vmem, far, far],
            out_specs=vmem,
            scratch_shapes=[
                pltpu.VMEM((2, width, nocc), BF),
                pltpu.VMEM((2, nvir, nocc), BF),
                pltpu.VMEM((rows, nvir), BF),
                pltpu.VMEM((rows, nocc), BF),
                pltpu.VMEM((2, nvir, rows), BF),
                pltpu.VMEM((nk, rows, nocc), BF),
                pltpu.VMEM((2, chips, rows, nocc), BF),
                pltpu.VMEM((nk, rows, rows), BF),
                pltpu.VMEM((nk, rows, rows), F32),
                pltpu.VMEM((nk, rows, rows), F32),
                pltpu.VMEM((4, rows, rows), BF),
                pltpu.VMEM((nk, rows, nocc), BF),
                pltpu.VMEM((chips, 2, rows, nocc), BF),
                pltpu.VMEM((chips, 8, rows), F32),
                pltpu.VMEM((bands, 8, rows), F32),
                pltpu.VMEM((rows, aux), BF),
                pltpu.VMEM((2, nvir, nocc), BF),
                pltpu.VMEM((2, bands, width, nocc), BF),
                dma((2, bands)), dma((2, bands)),
                dma((2,)), dma((2,)),
                dma((bands,)), dma((chips,)),
                dma((bands,)), dma((bands,)),
                dma, dma,
                dma((chips,)), dma((chips,)),
                dma((chips,)), dma((chips,)),
                dma((bands,)), dma((bands,)),
                dma((chips,)), dma((chips,)),
                dma((2, bands)), dma((2, bands)),
                dma((2,)),
            ],
            compiler_params=pltpu.CompilerParams(
                collective_id=0, has_side_effects=True, vmem_limit_bytes=48 * 1024 * 1024
            ),
            name="sigma",
        )(minus, turned, occ[0], vir[0], coulomb, exch)
        gaps = vir_energy[0][None, :] - occ_energy[0][:, None]
        return (gaps[None] * trial[0] + jnp.transpose(coupled, (0, 2, 1)))[None]

    in_specs = (
        P("ka", "band", None),
        P("ka", "band", None),
        P("ka", None, None, "band"),
        P("ka", None),
        P("ka", "band"),
        P("band", None),
        P(None, "band", None),
        P(),
    )
    return jax.shard_map(
        per_device,
        mesh=mesh,
        in_specs=in_specs,
        out_specs=P("ka", None, None, "band"),
        check_vma=False,
    )
```

```python
import jax
import jax.numpy as jnp
from jax import lax
from jax.experimental import pallas as pl
from jax.experimental.pallas import tpu as pltpu
from jax.sharding import PartitionSpec as P

BF = jnp.bfloat16
F32 = jnp.float32
MESH = pl.DeviceIdType.MESH
ALONG = (((1,), (1,)), ((), ()))


def each(count, body):
    def step(i, carry):
        body(i)
        return carry

    lax.fori_loop(0, count, step, 0)


def rdma(src, dst, send, recv, ka, band):
    return pltpu.make_async_remote_copy(
        src_ref=src,
        dst_ref=dst,
        send_sem=send,
        recv_sem=recv,
        device_id={"ka": ka, "band": band},
        device_id_type=MESH,
    )


def kernel(
    minus_h, trial_h, occ_h, vir_h, coulomb, exch, out,
    minus, trial, occ, vir, trial_bf, trial_all, vir_t, t_mine, t_all, occ_c, k_bf, k_f, pairs, s_bf,
    u_send, u_recv, acc_w, dens1, dens2, coul, sig_send, sig_recv,
    tri_s, tri_r, x_s, x_r, o1_s, o1_r, ox_s, ox_r, oy_s, oy_r, o3_s, o3_r, t_s, t_r, d1_s, d1_r, d2_s, d2_r,
    u_s, u_r, g_s, g_r, loc,
):
    bands = lax.axis_size("band")
    chips = lax.axis_size("ka") // 2
    depth = chips // 2
    ka = lax.axis_index("ka")
    b = lax.axis_index("band")
    j = ka // 2
    c = lax.rem(ka, 2)
    o = 1 - c
    h = j // depth
    z = lax.rem(j, depth)
    side = bands // 2
    xl = b // side
    y = lax.rem(b, side)
    quarter = 2 * h + xl
    mine = 2 * j + c
    other = 2 * j + o
    rows, nocc = occ_h.shape
    half = rows // 2
    width = trial.shape[1]
    nk = exch.shape[0]
    slab = rows // bands
    cols = pairs.shape[2]
    home = 2 * z + h
    goal = lax.rem(b, 2) * depth + b // 2

    def band_peer(i):
        return lax.rem(b + 1 + i, bands)

    def chip_peer(i):
        return lax.rem(j + 1 + i, chips)

    def block(start, size, unit=16):
        return pl.ds(pl.multiple_of(start, unit), size)

    loads = [
        pltpu.make_async_copy(occ_h, occ.at[c], loc.at[0]),
        pltpu.make_async_copy(trial_h, trial, loc.at[1]),
        pltpu.make_async_copy(vir_h, vir.at[c], loc.at[2]),
        pltpu.make_async_copy(
            exch.at[:, block(h * half, half), block(z * cols, cols, 128)], k_bf, loc.at[3]
        ),
        pltpu.make_async_copy(minus_h, minus, loc.at[4]),
        pltpu.make_async_copy(coulomb, coul, loc.at[5]),
    ]
    for load in loads:
        load.start()

    barrier = pltpu.get_barrier_semaphore()

    def greet(k, band):
        pl.semaphore_signal(barrier, inc=1, device_id={"ka": k, "band": band}, device_id_type=MESH)

    def greet_band(i):
        greet(mine, band_peer(i))
        greet(other, band_peer(i))

    def greet_chip(i):
        greet(2 * chip_peer(i) + c, b)
        greet(2 * chip_peer(i) + c, home)

    each(bands - 1, greet_band)
    each(chips - 1, greet_chip)
    greet(other, b)
    greet(2 * ((1 - h) * depth + z) + c, (1 - xl) * side + y)

    @pl.when(home != b)
    def _():
        greet(mine, home)

    loads[0].wait()
    loads[1].wait()
    trial_bf[...] = trial[...].astype(BF)
    callers = 2 * (bands - 1) + 2 * (chips - 1) + 2
    pl.semaphore_wait(barrier, jnp.where(home == b, callers, callers + 1))

    def occ1(i):
        return rdma(
            occ.at[c, block(i * slab, slab)],
            occ_c.at[c, j, 2 * lax.rem(b, 2) + i // side, lax.rem(i, side)],
            o1_s.at[i], o1_r.at[j], 2 * goal + c, i,
        )

    def occ1_start(i):
        @pl.when((i != b) | (goal != j))
        def _():
            occ1(i).start()

    each(bands, occ1_start)

    @pl.when(home == b)
    def _():
        occ_c[c, j, quarter, y] = occ[c, block(b * slab, slab), :]

    own_cols = block(b * width, width)

    def tri_same(i):
        return rdma(trial_bf.at[c], trial_all.at[c, own_cols], tri_s.at[0, i], tri_r.at[c, b], mine, band_peer(i))

    def tri_cross(i):
        p = lax.rem(b + i, bands)
        return rdma(trial_bf.at[o], trial_all.at[c, own_cols], tri_s.at[1, i], tri_r.at[c, b], other, p)

    each(bands - 1, lambda i: tri_same(i).start())
    loads[2].wait()
    send_vir = rdma(vir.at[c], vir.at[c], x_s.at[0], x_r.at[0], other, b)
    send_occ = rdma(occ.at[c], occ.at[c], x_s.at[1], x_r.at[1], other, b)
    send_vir.start()
    send_occ.start()
    each(bands, lambda i: tri_cross(i).start())
    trial_all[c, own_cols, :] = trial_bf[c]

    def occ1_wait(i):
        @pl.when((i != j) | (home != b))
        def _():
            rdma(
                occ.at[c, block(b * slab, slab)], occ_c.at[c, i, quarter, y], o1_s.at[i], o1_r.at[i], mine, b
            ).wait_recv()

    each(chips, occ1_wait)

    def piece(q, row):
        return occ_c.at[c, :, q, row]

    def occ_x(i):
        q = quarter ^ (i + 1)
        return rdma(
            piece(quarter, y), piece(quarter, y), ox_s.at[i], ox_r.at[quarter],
            2 * ((q // 2) * depth + z) + c, lax.rem(q, 2) * side + y,
        )

    def occ_y(q, i):
        return rdma(
            piece(q, y), piece(q, y), oy_s.at[q, i], oy_r.at[q, y], mine, xl * side + lax.rem(y + 1 + i, side)
        )

    each(3, lambda i: occ_x(i).start())
    each(side - 1, lambda i: occ_y(quarter, i).start())

    vir_t[c] = vir[c].T

    def tri_wait_same(i):
        p = band_peer(i)
        part = block(p * width, width)
        rdma(trial_bf.at[c], trial_all.at[c, part], tri_s.at[0, i], tri_r.at[c, p], mine, p).wait_recv()

    def tri_wait_cross(i):
        part = block(i * width, width)
        rdma(trial_bf.at[o], trial_all.at[o, part], tri_s.at[1, i], tri_r.at[o, i], other, i).wait_recv()

    def t_copy(s, i):
        p = chip_peer(i)
        return rdma(t_mine.at[p // depth, s], t_all.at[2 * j + s], t_s.at[s, i], t_r.at[s, j], 2 * p + c, b)

    def t_make(s):
        value = jnp.dot(vir[s], trial_all[s], preferred_element_type=F32)
        t_mine[0, s] = value[:half].astype(BF)
        t_mine[1, s] = value[half:].astype(BF)
        each(chips - 1, lambda i: t_copy(s, i).start())
        t_all[2 * j + s] = t_mine[h, s]
        return occ[s].astype(F32) * value

    each(bands - 1, tri_wait_same)
    local = t_make(c)
    rdma(vir.at[c], vir.at[o], x_s.at[0], x_r.at[0], other, b).wait_recv()
    rdma(occ.at[c], occ.at[o], x_s.at[1], x_r.at[1], other, b).wait_recv()
    each(bands, tri_wait_cross)
    local = local + t_make(o)

    def forward(i):
        q = quarter ^ (i + 1)
        rdma(piece(quarter, y), piece(q, y), ox_s.at[i], ox_r.at[q], mine, b).wait_recv()
        each(side - 1, lambda n: occ_y(q, n).start())

    each(3, forward)

    def occ3(row):
        return rdma(occ_c.at[c, :, :, row], occ_c.at[c, :, :, row], o3_s.at[row], o3_r.at[row], other, b)

    occ3(y).start()

    high = local.astype(BF)
    low = (local - high.astype(F32)).astype(BF)
    ones = jnp.ones((8, nocc), BF)
    dens1[j] = lax.dot_general(ones, high, ALONG, preferred_element_type=F32) + lax.dot_general(
        ones, low, ALONG, preferred_element_type=F32
    )

    def d1_copy(i):
        return rdma(dens1.at[j], dens1.at[j], d1_s.at[i], d1_r.at[j], 2 * chip_peer(i) + c, b)

    each(chips - 1, lambda i: d1_copy(i).start())
    vir_t[o] = vir[o].T

    loads[3].wait()

    def widen(q):
        k_f[q] = k_bf[q].astype(F32)

    each(nk, widen)

    def occ_rest(i):
        row = lax.rem(y + 1 + i, side)
        for q in range(4):
            rdma(piece(q, row), piece(q, row), oy_s.at[q, i], oy_r.at[q, row], mine, b).wait_recv()
        occ3(row).start()

    each(side - 1, occ_rest)

    def occ3_wait(row):
        rdma(occ_c.at[c, :, :, row], occ_c.at[o, :, :, row], o3_s.at[row], o3_r.at[row], other, b).wait_recv()

    each(side, occ3_wait)

    def pairs_of(p):
        for s in range(2):
            points = occ_c[s, p].reshape(cols, nocc)
            pairs[2 * p + s] = lax.dot_general(t_all[2 * p + s], points, ALONG, preferred_element_type=F32)

    pairs_of(j)

    def t_arrived(i):
        p = chip_peer(i)
        for s in range(2):
            rdma(t_mine.at[0, s], t_all.at[2 * p + s], t_s.at[s, i], t_r.at[s, p], 2 * p + c, b).wait_recv()
        pairs_of(p)

    each(chips - 1, t_arrived)

    def d1_wait(i):
        p = chip_peer(i)
        rdma(dens1.at[p], dens1.at[p], d1_s.at[i], d1_r.at[p], 2 * p + c, b).wait_recv()

    each(chips - 1, d1_wait)
    total = dens1[0]
    for p in range(1, chips):
        total = total + dens1[p]
    dens2[b] = total

    def d2_copy(i):
        return rdma(dens2.at[b], dens2.at[b], d2_s.at[i], d2_r.at[b], mine, band_peer(i))

    each(bands - 1, lambda i: d2_copy(i).start())
    loads[4].wait()

    tile = 16
    fours = 4

    def u_copy(dest, s):
        return rdma(u_send.at[2 * dest + s], u_recv.at[j, s], u_s.at[s, dest], u_r.at[s, j], 2 * dest + c, b)

    def screen(g, s):
        dests = [j ^ (chips - 1 - fours * g - n) for n in range(fours)]

        def rows_step(r):
            part = block(r * tile, tile)
            acc = [jnp.zeros((tile, cols), F32) for _ in dests]
            for q in range(nk):
                weight = k_f[q, part, :]
                for n, dest in enumerate(dests):
                    acc[n] = acc[n] + pairs[minus[2 * dest + s, q], part, :] * weight
            for n in range(fours):
                s_bf[n, part, :] = acc[n].astype(BF)

        each(half // tile, rows_step)
        for n, dest in enumerate(dests):
            points = occ_c[s, dest].reshape(cols, nocc)
            u_send[2 * dest + s] = jnp.dot(s_bf[n], points, preferred_element_type=F32).astype(BF)

            @pl.when(dest != j)
            def _():
                u_copy(dest, s).start()

    def finish(s):
        mine_rows = block(h * half, half)
        acc_w[s, mine_rows, :] = acc_w[s, mine_rows, :] - u_send[2 * j + s].astype(F32)

        def u_arrived(i):
            p = chip_peer(i)
            rdma(u_send.at[2 * p + s], u_recv.at[p, s], u_s.at[s, p], u_r.at[s, p], 2 * p + c, b).wait_recv()
            part = block((p // depth) * half, half)
            acc_w[s, part, :] = acc_w[s, part, :] - u_recv[p, s].astype(F32)

        each(chips - 1, u_arrived)
        sig_send[s] = jnp.dot(vir_t[s], acc_w[s].astype(BF), preferred_element_type=F32).astype(BF)

        def sig_start(p):
            @pl.when((c != s) | (p != b))
            def _():
                sig_copy(s, p).start()

        each(bands, sig_start)

        @pl.when(c == s)
        def _():
            sig_recv[c, b] = sig_send[s, own_cols, :]

    def sig_copy(s, p):
        return rdma(
            sig_send.at[s, block(p * width, width)], sig_recv.at[c, b], g_s.at[s, p], g_r.at[c, b], 2 * j + s, p
        )

    screen(0, 0)
    screen(1, 0)
    screen(0, 1)

    def d2_wait(i):
        p = band_peer(i)
        rdma(dens2.at[p], dens2.at[p], d2_s.at[i], d2_r.at[p], mine, p).wait_recv()

    each(bands - 1, d2_wait)
    loads[5].wait()
    pot = jnp.zeros((rows, nocc), F32)
    for p in range(bands):
        line = jnp.broadcast_to(dens2[p][0:1, :].astype(BF), (nocc, rows))
        pot = pot + lax.dot_general(coul[:, p * rows : (p + 1) * rows], line, ALONG, preferred_element_type=F32)
    pot = pot * 2.0
    for s in range(2):
        acc_w[s] = pot * occ[s].astype(F32)

    finish(0)
    screen(1, 1)
    finish(1)

    def sig_wait_same(i):
        p = band_peer(i)
        rdma(sig_send.at[0, own_cols], sig_recv.at[c, p], g_s.at[0, i], g_r.at[c, p], mine, p).wait_recv()

    def sig_wait_cross(i):
        rdma(sig_send.at[0, own_cols], sig_recv.at[o, i], g_s.at[1, i], g_r.at[o, i], other, i).wait_recv()

    each(bands - 1, sig_wait_same)
    each(bands, sig_wait_cross)
    for v in range(2):
        sums = sig_recv[v, 0].astype(F32)
        for p in range(1, bands):
            sums = sums + sig_recv[v, p].astype(F32)
        out[v] = sums

    each(bands - 1, lambda i: tri_same(i).wait_send())
    each(bands, lambda i: tri_cross(i).wait_send())

    def occ1_sent(i):
        @pl.when((i != b) | (goal != j))
        def _():
            occ1(i).wait_send()

    each(bands, occ1_sent)
    send_vir.wait_send()
    send_occ.wait_send()
    each(3, lambda i: occ_x(i).wait_send())
    for q in range(4):
        each(side - 1, lambda i: occ_y(q, i).wait_send())
    each(side, lambda row: occ3(row).wait_send())
    each(chips - 1, lambda i: d1_copy(i).wait_send())
    each(bands - 1, lambda i: d2_copy(i).wait_send())
    for s in range(2):
        each(chips - 1, lambda i: t_copy(s, i).wait_send())
        each(chips - 1, lambda i: u_copy(chip_peer(i), s).wait_send())

        def sig_sent(p):
            @pl.when((c != s) | (p != b))
            def _():
                sig_copy(s, p).wait_send()

        each(bands, sig_sent)


def solution(mesh):
    bands = mesh.shape["band"]
    chips = mesh.shape["ka"] // 2

    def per_device(occ, vir, trial, occ_energy, vir_energy, coulomb, exch, minus):
        nk, rows, aux = exch.shape
        nocc = occ.shape[2]
        nvir = vir.shape[2]
        width = trial.shape[3]
        half = rows // 2
        cols = 2 * rows
        turned = jnp.transpose(trial[0], (0, 2, 1))
        far = pl.BlockSpec(memory_space=pltpu.HBM)
        dma = pltpu.SemaphoreType.DMA
        coupled = pl.pallas_call(
            kernel,
            out_shape=jax.ShapeDtypeStruct((2, width, nocc), F32),
            in_specs=[far] * 6,
            out_specs=pl.BlockSpec(memory_space=pltpu.VMEM),
            scratch_shapes=[
                pltpu.SMEM((nk, nk), jnp.int32),
                pltpu.VMEM((2, width, nocc), F32),
                pltpu.VMEM((2, rows, nocc), BF),
                pltpu.VMEM((2, rows, nvir), BF),
                pltpu.VMEM((2, width, nocc), BF),
                pltpu.VMEM((2, nvir, nocc), BF),
                pltpu.VMEM((2, nvir, rows), BF),
                pltpu.VMEM((2, 2, half, nocc), BF),
                pltpu.VMEM((nk, half, nocc), BF),
                pltpu.VMEM((2, chips, 4, bands // 2, rows // bands, nocc), BF),
                pltpu.VMEM((nk, half, cols), BF),
                pltpu.VMEM((nk, half, cols), F32),
                pltpu.VMEM((nk, half, cols), F32),
                pltpu.VMEM((4, half, cols), BF),
                pltpu.VMEM((nk, half, nocc), BF),
                pltpu.VMEM((chips, 2, half, nocc), BF),
                pltpu.VMEM((2, rows, nocc), F32),
                pltpu.VMEM((chips, 8, rows), F32),
                pltpu.VMEM((bands, 8, rows), F32),
                pltpu.VMEM((rows, aux), BF),
                pltpu.VMEM((2, nvir, nocc), BF),
                pltpu.VMEM((2, bands, width, nocc), BF),
                dma((2, bands)), dma((2, bands)),
                dma((2,)), dma((2,)),
                dma((bands,)), dma((chips,)),
                dma((3,)), dma((4,)),
                dma((4, bands // 2)), dma((4, bands // 2)),
                dma((bands // 2,)), dma((bands // 2,)),
                dma((2, chips)), dma((2, chips)),
                dma((chips,)), dma((chips,)),
                dma((bands,)), dma((bands,)),
                dma((2, chips)), dma((2, chips)),
                dma((2, bands)), dma((2, bands)),
                dma((6,)),
            ],
            compiler_params=pltpu.CompilerParams(
                collective_id=0, has_side_effects=True, vmem_limit_bytes=67043328
            ),
            name="sigma",
        )(minus, turned, occ[0], vir[0], coulomb, exch)
        gaps = vir_energy[0][None, :] - occ_energy[0][:, None]
        return (gaps[None] * trial[0] + jnp.transpose(coupled, (0, 2, 1)))[None]

    in_specs = (
        P("ka", "band", None),
        P("ka", "band", None),
        P("ka", None, None, "band"),
        P("ka", None),
        P("ka", "band"),
        P("band", None),
        P(None, "band", None),
        P(),
    )
    return jax.shard_map(
        per_device,
        mesh=mesh,
        in_specs=in_specs,
        out_specs=P("ka", None, None, "band"),
        check_vma=False,
    )
```

```python
import jax
import jax.numpy as jnp
from jax import lax
from jax.experimental import pallas as pl
from jax.experimental.pallas import tpu as pltpu
from jax.sharding import PartitionSpec as P

BF = jnp.bfloat16
F32 = jnp.float32
MESH = pl.DeviceIdType.MESH
ALONG = (((1,), (1,)), ((), ()))


def each(count, body):
    def step(i, carry):
        body(i)
        return carry

    lax.fori_loop(0, count, step, 0)


def rdma(src, dst, send, recv, ka, band):
    return pltpu.make_async_remote_copy(
        src_ref=src,
        dst_ref=dst,
        send_sem=send,
        recv_sem=recv,
        device_id={"ka": ka, "band": band},
        device_id_type=MESH,
    )


def kernel(
    minus_h, trial_h, occ_h, vir_h, coulomb, exch, occ_e_h, vir_e_h, out,
    minus, trial, occ, vir, occ_e, vir_e, turn, trial_bf, trial_all, vir_t, t_mine, t_all, occ_c, k_bf, pairs, s_bf,
    u_send, u_recv, acc_w, dens1, dens2, coul, sig_send, sig_recv,
    tri_s, tri_r, x_s, x_r, o1_s, o1_r, ox_s, ox_r, oy_s, oy_r, o3_s, o3_r, t_s, t_r, d1_s, d1_r, d2_s, d2_r,
    u_s, u_r, g_s, g_r, loc,
):
    bands = lax.axis_size("band")
    chips = lax.axis_size("ka") // 2
    depth = chips // 2
    ka = lax.axis_index("ka")
    b = lax.axis_index("band")
    j = ka // 2
    c = lax.rem(ka, 2)
    o = 1 - c
    h = j // depth
    z = lax.rem(j, depth)
    side = bands // 2
    xl = b // side
    y = lax.rem(b, side)
    quarter = 2 * h + xl
    mine = 2 * j + c
    other = 2 * j + o
    rows, nocc = occ_h.shape
    half = rows // 2
    width = trial.shape[1]
    nk = exch.shape[0]
    slab = rows // bands
    cols = pairs.shape[2]
    home = 2 * z + h
    goal = lax.rem(b, 2) * depth + b // 2

    def band_peer(i):
        return lax.rem(b + 1 + i, bands)

    def chip_peer(i):
        return lax.rem(j + 1 + i, chips)

    def block(start, size, unit=16):
        return pl.ds(pl.multiple_of(start, unit), size)

    loads = [
        pltpu.make_async_copy(occ_h, occ.at[c], loc.at[0]),
        pltpu.make_async_copy(trial_h, trial, loc.at[1]),
        pltpu.make_async_copy(vir_h, vir.at[c], loc.at[2]),
        pltpu.make_async_copy(
            exch.at[:, block(h * half, half), block(z * cols, cols, 128)], k_bf, loc.at[3]
        ),
        pltpu.make_async_copy(minus_h, minus, loc.at[4]),
        pltpu.make_async_copy(coulomb, coul, loc.at[5]),
        pltpu.make_async_copy(occ_e_h, occ_e, loc.at[6]),
        pltpu.make_async_copy(vir_e_h, vir_e, loc.at[7]),
    ]
    for load in loads:
        load.start()

    barrier = pltpu.get_barrier_semaphore()

    def greet(k, band):
        pl.semaphore_signal(barrier, inc=1, device_id={"ka": k, "band": band}, device_id_type=MESH)

    def greet_band(i):
        greet(mine, band_peer(i))
        greet(other, band_peer(i))

    def greet_chip(i):
        greet(2 * chip_peer(i) + c, b)
        greet(2 * chip_peer(i) + c, home)

    each(bands - 1, greet_band)
    each(chips - 1, greet_chip)
    greet(other, b)
    greet(2 * ((1 - h) * depth + z) + c, (1 - xl) * side + y)

    @pl.when(home != b)
    def _():
        greet(mine, home)

    loads[0].wait()
    loads[1].wait()
    trial_bf[...] = trial[...].astype(BF)
    callers = 2 * (bands - 1) + 2 * (chips - 1) + 2
    pl.semaphore_wait(barrier, jnp.where(home == b, callers, callers + 1))

    def occ1(i):
        return rdma(
            occ.at[c, block(i * slab, slab)],
            occ_c.at[c, j, 2 * lax.rem(b, 2) + i // side, lax.rem(i, side)],
            o1_s.at[i], o1_r.at[j], 2 * goal + c, i,
        )

    def occ1_start(i):
        @pl.when((i != b) | (goal != j))
        def _():
            occ1(i).start()

    each(bands, occ1_start)

    @pl.when(home == b)
    def _():
        occ_c[c, j, quarter, y] = occ[c, block(b * slab, slab), :]

    own_cols = block(b * width, width)

    def tri_same(i):
        return rdma(trial_bf.at[c], trial_all.at[c, own_cols], tri_s.at[0, i], tri_r.at[c, b], mine, band_peer(i))

    def tri_cross(i):
        p = lax.rem(b + i, bands)
        return rdma(trial_bf.at[o], trial_all.at[c, own_cols], tri_s.at[1, i], tri_r.at[c, b], other, p)

    each(bands - 1, lambda i: tri_same(i).start())
    loads[2].wait()
    send_vir = rdma(vir.at[c], vir.at[c], x_s.at[0], x_r.at[0], other, b)
    send_occ = rdma(occ.at[c], occ.at[c], x_s.at[1], x_r.at[1], other, b)
    send_vir.start()
    send_occ.start()
    each(bands, lambda i: tri_cross(i).start())
    trial_all[c, own_cols, :] = trial_bf[c]

    def occ1_wait(i):
        @pl.when((i != j) | (home != b))
        def _():
            rdma(
                occ.at[c, block(b * slab, slab)], occ_c.at[c, i, quarter, y], o1_s.at[i], o1_r.at[i], mine, b
            ).wait_recv()

    each(chips, occ1_wait)

    def piece(q, row):
        return occ_c.at[c, :, q, row]

    def occ_x(i):
        q = quarter ^ (i + 1)
        return rdma(
            piece(quarter, y), piece(quarter, y), ox_s.at[i], ox_r.at[quarter],
            2 * ((q // 2) * depth + z) + c, lax.rem(q, 2) * side + y,
        )

    up = lax.rem(y + 1, side)
    down = lax.rem(y + side - 1, side)
    across = lax.rem(y + 2, side)

    def occ_y(q, row, to, n):
        return rdma(piece(q, row), piece(q, row), oy_s.at[q, n], oy_r.at[q, row], mine, xl * side + to)

    def occ_y_start(q):
        occ_y(q, y, up, 0).start()
        occ_y(q, y, down, 1).start()

    def occ_y_wait(q, row):
        rdma(piece(q, row), piece(q, row), oy_s.at[q, 0], oy_r.at[q, row], mine, b).wait_recv()

    each(3, lambda i: occ_x(i).start())
    occ_y_start(quarter)

    vir_t[c] = vir[c].T

    def tri_wait_same(i):
        p = band_peer(i)
        part = block(p * width, width)
        rdma(trial_bf.at[c], trial_all.at[c, part], tri_s.at[0, i], tri_r.at[c, p], mine, p).wait_recv()

    def tri_wait_cross(i):
        part = block(i * width, width)
        rdma(trial_bf.at[o], trial_all.at[o, part], tri_s.at[1, i], tri_r.at[o, i], other, i).wait_recv()

    def t_copy(s, i):
        p = chip_peer(i)
        return rdma(t_mine.at[p // depth, s], t_all.at[2 * j + s], t_s.at[s, i], t_r.at[s, j], 2 * p + c, b)

    def t_make(s):
        value = jnp.dot(vir[s], trial_all[s], preferred_element_type=F32)
        t_mine[0, s] = value[:half].astype(BF)
        t_mine[1, s] = value[half:].astype(BF)
        t_all[2 * j + s] = t_mine[h, s]
        return occ[s].astype(F32) * value

    def t_start(s):
        each(chips - 1, lambda i: t_copy(s, i).start())

    each(bands - 1, tri_wait_same)
    local = t_make(c)
    t_start(c)
    rdma(vir.at[c], vir.at[o], x_s.at[0], x_r.at[0], other, b).wait_recv()
    rdma(occ.at[c], occ.at[o], x_s.at[1], x_r.at[1], other, b).wait_recv()
    each(bands, tri_wait_cross)
    local = local + t_make(o)

    high = local.astype(BF)
    low = (local - high.astype(F32)).astype(BF)
    ones = jnp.ones((8, nocc), BF)
    dens1[j] = lax.dot_general(ones, high, ALONG, preferred_element_type=F32) + lax.dot_general(
        ones, low, ALONG, preferred_element_type=F32
    )

    def d1_copy(i):
        return rdma(dens1.at[j], dens1.at[j], d1_s.at[i], d1_r.at[j], 2 * chip_peer(i) + c, b)

    each(chips - 1, lambda i: d1_copy(i).start())
    t_start(o)

    def forward(i):
        q = quarter ^ (i + 1)
        rdma(piece(quarter, y), piece(q, y), ox_s.at[i], ox_r.at[q], mine, b).wait_recv()
        occ_y_start(q)

    each(3, forward)

    def occ3(row):
        return rdma(occ_c.at[c, :, :, row], occ_c.at[c, :, :, row], o3_s.at[row], o3_r.at[row], other, b)

    occ3(y).start()

    vir_t[o] = vir[o].T
    turn[...] = jnp.zeros_like(turn)
    loads[6].wait()
    loads[7].wait()
    turn[:, 0:width] = jnp.broadcast_to(vir_e[...], (nocc, width))
    gaps = turn[...].T[0:width] - occ_e[...]
    for v in range(2):
        out[v] = gaps * trial[v]

    def occ_near(i):
        q = quarter ^ i
        occ_y_wait(q, down)

        @pl.when(q < 2)
        def _():
            occ_y(q, down, up, 2).start()

        occ_y_wait(q, up)

        @pl.when(q >= 2)
        def _():
            occ_y(q, up, down, 2).start()

    each(4, occ_near)
    occ3(down).start()
    occ3(up).start()

    def d1_wait(i):
        p = chip_peer(i)
        rdma(dens1.at[p], dens1.at[p], d1_s.at[i], d1_r.at[p], 2 * p + c, b).wait_recv()

    each(chips - 1, d1_wait)
    total = dens1[0]
    for p in range(1, chips):
        total = total + dens1[p]
    dens2[b] = total

    def d2_copy(i):
        return rdma(dens2.at[b], dens2.at[b], d2_s.at[i], d2_r.at[b], mine, band_peer(i))

    each(bands - 1, lambda i: d2_copy(i).start())

    each(4, lambda q: occ_y_wait(q, across))
    occ3(across).start()

    def pairs_of(p, s):
        points = occ_c[s, p].reshape(cols, nocc)
        k = 2 * p + s
        pairs[k] = lax.dot_general(t_all[k], points, ALONG, preferred_element_type=F32).astype(BF)

    def t_arrived(i):
        p = chip_peer(i)
        for s in range(2):
            rdma(t_mine.at[0, s], t_all.at[2 * p + s], t_s.at[s, i], t_r.at[s, p], 2 * p + c, b).wait_recv()
        pairs_of(p, c)

    pairs_of(j, c)
    each(chips - 1, t_arrived)

    def d2_wait(i):
        p = band_peer(i)
        rdma(dens2.at[p], dens2.at[p], d2_s.at[i], d2_r.at[p], mine, p).wait_recv()

    each(bands - 1, d2_wait)
    loads[5].wait()
    pot = jnp.zeros((rows, nocc), F32)
    for p in range(bands):
        line = jnp.broadcast_to(dens2[p][0:1, :].astype(BF), (nocc, rows))
        pot = pot + lax.dot_general(coul[:, p * rows : (p + 1) * rows], line, ALONG, preferred_element_type=F32)
    pot = pot * 2.0
    for s in range(2):
        acc_w[s] = pot * occ[s].astype(F32)

    def occ3_wait(row):
        rdma(occ_c.at[c, :, :, row], occ_c.at[o, :, :, row], o3_s.at[row], o3_r.at[row], other, b).wait_recv()

    each(side, occ3_wait)

    each(chips, lambda p: pairs_of(p, o))
    loads[3].wait()
    loads[4].wait()

    tile = 16
    fours = 4

    def u_copy(dest, s):
        return rdma(u_send.at[2 * dest + s], u_recv.at[j, s], u_s.at[s, dest], u_r.at[s, j], 2 * dest + c, b)

    def screen(g, s):
        dests = [j ^ (chips - 1 - fours * g - n) for n in range(fours)]

        def rows_step(r):
            part = block(r * tile, tile)
            for n, dest in enumerate(dests):
                acc = jnp.zeros((tile, cols), F32)
                for q in range(nk):
                    acc = acc + pairs[minus[2 * dest + s, q], part, :].astype(F32) * k_bf[q, part, :].astype(F32)
                s_bf[n, part, :] = acc.astype(BF)

        each(half // tile, rows_step)
        for n, dest in enumerate(dests):
            points = occ_c[s, dest].reshape(cols, nocc)
            u_send[2 * dest + s] = jnp.dot(s_bf[n], points, preferred_element_type=F32).astype(BF)

            @pl.when(dest != j)
            def _():
                u_copy(dest, s).start()

    def finish(s):
        mine_rows = block(h * half, half)
        acc_w[s, mine_rows, :] = acc_w[s, mine_rows, :] - u_send[2 * j + s].astype(F32)

        def u_arrived(i):
            p = chip_peer(i)
            rdma(u_send.at[2 * p + s], u_recv.at[p, s], u_s.at[s, p], u_r.at[s, p], 2 * p + c, b).wait_recv()
            part = block((p // depth) * half, half)
            acc_w[s, part, :] = acc_w[s, part, :] - u_recv[p, s].astype(F32)

        each(chips - 1, u_arrived)
        sig_send[s] = jnp.dot(vir_t[s], acc_w[s].astype(BF), preferred_element_type=F32).astype(BF)

        def sig_start(p):
            @pl.when((c != s) | (p != b))
            def _():
                sig_copy(s, p).start()

        each(bands, sig_start)

        @pl.when(c == s)
        def _():
            sig_recv[c, b] = sig_send[s, own_cols, :]

    def sig_copy(s, p):
        return rdma(
            sig_send.at[s, block(p * width, width)], sig_recv.at[c, b], g_s.at[s, p], g_r.at[c, b], 2 * j + s, p
        )

    screen(0, 0)
    screen(1, 0)
    screen(0, 1)

    finish(0)
    screen(1, 1)
    finish(1)

    def sig_wait_same(i):
        p = band_peer(i)
        rdma(sig_send.at[0, own_cols], sig_recv.at[c, p], g_s.at[0, i], g_r.at[c, p], mine, p).wait_recv()

    def sig_wait_cross(i):
        rdma(sig_send.at[0, own_cols], sig_recv.at[o, i], g_s.at[1, i], g_r.at[o, i], other, i).wait_recv()

    each(bands - 1, sig_wait_same)
    each(bands, sig_wait_cross)
    for v in range(2):
        sums = sig_recv[v, 0].astype(F32)
        for p in range(1, bands):
            sums = sums + sig_recv[v, p].astype(F32)
        out[v] = out[v] + sums

    each(bands - 1, lambda i: tri_same(i).wait_send())
    each(bands, lambda i: tri_cross(i).wait_send())

    def occ1_sent(i):
        @pl.when((i != b) | (goal != j))
        def _():
            occ1(i).wait_send()

    each(bands, occ1_sent)
    send_vir.wait_send()
    send_occ.wait_send()
    each(3, lambda i: occ_x(i).wait_send())
    for q in range(4):
        occ_y(q, y, up, 0).wait_send()
        occ_y(q, y, down, 1).wait_send()
        if q < 2:
            occ_y(q, down, up, 2).wait_send()
        else:
            occ_y(q, up, down, 2).wait_send()
    each(side, lambda row: occ3(row).wait_send())
    each(chips - 1, lambda i: d1_copy(i).wait_send())
    each(bands - 1, lambda i: d2_copy(i).wait_send())
    for s in range(2):
        each(chips - 1, lambda i: t_copy(s, i).wait_send())
        each(chips - 1, lambda i: u_copy(chip_peer(i), s).wait_send())

        def sig_sent(p):
            @pl.when((c != s) | (p != b))
            def _():
                sig_copy(s, p).wait_send()

        each(bands, sig_sent)


def solution(mesh):
    bands = mesh.shape["band"]
    chips = mesh.shape["ka"] // 2

    def per_device(occ, vir, trial, occ_energy, vir_energy, coulomb, exch, minus):
        nk, rows, aux = exch.shape
        nocc = occ.shape[2]
        nvir = vir.shape[2]
        width = trial.shape[3]
        half = rows // 2
        cols = 2 * rows
        turned = jnp.transpose(trial[0], (0, 2, 1))
        far = pl.BlockSpec(memory_space=pltpu.HBM)
        dma = pltpu.SemaphoreType.DMA
        result = pl.pallas_call(
            kernel,
            out_shape=jax.ShapeDtypeStruct((2, width, nocc), F32),
            in_specs=[far] * 8,
            out_specs=pl.BlockSpec(memory_space=pltpu.VMEM),
            scratch_shapes=[
                pltpu.SMEM((nk, nk), jnp.int32),
                pltpu.VMEM((2, width, nocc), F32),
                pltpu.VMEM((2, rows, nocc), BF),
                pltpu.VMEM((2, rows, nvir), BF),
                pltpu.VMEM((1, nocc), F32),
                pltpu.VMEM((1, width), F32),
                pltpu.VMEM((nocc, 128), F32),
                pltpu.VMEM((2, width, nocc), BF),
                pltpu.VMEM((2, nvir, nocc), BF),
                pltpu.VMEM((2, nvir, rows), BF),
                pltpu.VMEM((2, 2, half, nocc), BF),
                pltpu.VMEM((nk, half, nocc), BF),
                pltpu.VMEM((2, chips, 4, bands // 2, rows // bands, nocc), BF),
                pltpu.VMEM((nk, half, cols), BF),
                pltpu.VMEM((nk, half, cols), BF),
                pltpu.VMEM((4, half, cols), BF),
                pltpu.VMEM((nk, half, nocc), BF),
                pltpu.VMEM((chips, 2, half, nocc), BF),
                pltpu.VMEM((2, rows, nocc), F32),
                pltpu.VMEM((chips, 8, rows), F32),
                pltpu.VMEM((bands, 8, rows), F32),
                pltpu.VMEM((rows, aux), BF),
                pltpu.VMEM((2, nvir, nocc), BF),
                pltpu.VMEM((2, bands, width, nocc), BF),
                dma((2, bands)), dma((2, bands)),
                dma((2,)), dma((2,)),
                dma((bands,)), dma((chips,)),
                dma((3,)), dma((4,)),
                dma((4, 3)), dma((4, bands // 2)),
                dma((bands // 2,)), dma((bands // 2,)),
                dma((2, chips)), dma((2, chips)),
                dma((chips,)), dma((chips,)),
                dma((bands,)), dma((bands,)),
                dma((2, chips)), dma((2, chips)),
                dma((2, bands)), dma((2, bands)),
                dma((8,)),
            ],
            compiler_params=pltpu.CompilerParams(
                collective_id=0, has_side_effects=True, vmem_limit_bytes=67043328
            ),
            name="sigma",
        )(minus, turned, occ[0], vir[0], coulomb, exch, occ_energy, vir_energy)
        return jnp.transpose(result, (0, 2, 1))[None]

    in_specs = (
        P("ka", "band", None),
        P("ka", "band", None),
        P("ka", None, None, "band"),
        P("ka", None),
        P("ka", "band"),
        P("band", None),
        P(None, "band", None),
        P(),
    )
    return jax.shard_map(
        per_device,
        mesh=mesh,
        in_specs=in_specs,
        out_specs=P("ka", None, None, "band"),
        check_vma=False,
    )
```

```python
import jax
import jax.numpy as jnp
from jax import lax
from jax.experimental import pallas as pl
from jax.experimental.pallas import tpu as pltpu
from jax.sharding import PartitionSpec as P

BF = jnp.bfloat16
F32 = jnp.float32
MESH = pl.DeviceIdType.MESH
ALONG = (((1,), (1,)), ((), ()))


def each(count, body):
    def step(i, carry):
        body(i)
        return carry

    lax.fori_loop(0, count, step, 0)


def rdma(src, dst, send, recv, ka, band):
    return pltpu.make_async_remote_copy(
        src_ref=src,
        dst_ref=dst,
        send_sem=send,
        recv_sem=recv,
        device_id={"ka": ka, "band": band},
        device_id_type=MESH,
    )


def kernel(
    minus_h, trial_h, occ_h, vir_h, coulomb, exch, occ_e_h, vir_e_h, out,
    minus, trial, occ, vir, occ_e, vir_e, turn, trial_bf, trial_all, vir_t, t_mine, t_all, occ_c, k_bf, pairs, s_bf,
    u_send, u_recv, acc_w, dens1, dens2, coul, sig_send, sig_recv,
    tri_s, tri_r, x_s, x_r, o1_s, o1_r, ox_s, ox_r, oy_s, oy_r, fy_s, fy_r, fx_s, fx_r, o3_s, o3_r, t_s, f_s, t_r, d1_s, d1_r, d2_s, d2_r,
    u_s, u_r, g_s, g_r, loc,
):
    bands = lax.axis_size("band")
    chips = lax.axis_size("ka") // 2
    depth = chips // 2
    ka = lax.axis_index("ka")
    b = lax.axis_index("band")
    j = ka // 2
    c = lax.rem(ka, 2)
    o = 1 - c
    h = j // depth
    z = lax.rem(j, depth)
    side = bands // 2
    xl = b // side
    y = lax.rem(b, side)
    quarter = 2 * h + xl
    mine = 2 * j + c
    other = 2 * j + o
    rows, nocc = occ_h.shape
    half = rows // 2
    width = trial.shape[1]
    nk = exch.shape[0]
    slab = rows // side
    cols = pairs.shape[2]
    home = xl * side + z
    goal = h * depth + y
    partner = (1 - h) * depth + z

    def band_peer(i):
        return lax.rem(b + 1 + i, bands)

    def chip_peer(i):
        return lax.rem(j + 1 + i, chips)

    def block(start, size, unit=16):
        return pl.ds(pl.multiple_of(start, unit), size)

    loads = [
        pltpu.make_async_copy(occ_h, occ.at[c], loc.at[0]),
        pltpu.make_async_copy(trial_h, trial, loc.at[1]),
        pltpu.make_async_copy(vir_h, vir.at[c], loc.at[2]),
        pltpu.make_async_copy(
            exch.at[:, block(h * half, half), block(z * rows, rows, 128)], k_bf.at[:, :, pl.ds(0, rows)], loc.at[3]
        ),
        pltpu.make_async_copy(
            exch.at[:, block(h * half, half), block((z + side) * rows, rows, 128)],
            k_bf.at[:, :, pl.ds(rows, rows)], loc.at[8],
        ),
        pltpu.make_async_copy(minus_h, minus, loc.at[4]),
        pltpu.make_async_copy(coulomb, coul, loc.at[5]),
        pltpu.make_async_copy(occ_e_h, occ_e, loc.at[6]),
        pltpu.make_async_copy(vir_e_h, vir_e, loc.at[7]),
    ]
    for load in loads:
        load.start()

    barrier = pltpu.get_barrier_semaphore()

    def greet(k, band):
        pl.semaphore_signal(barrier, inc=1, device_id={"ka": k, "band": band}, device_id_type=MESH)

    def greet_band(i):
        greet(mine, band_peer(i))
        greet(other, band_peer(i))

    def deep(i):
        return h * depth + lax.rem(z + 1 + i, depth)

    each(bands - 1, greet_band)
    each(chips - 1, lambda i: greet(2 * chip_peer(i) + c, b))
    each(depth - 1, lambda i: greet(2 * deep(i) + c, home))
    greet(other, b)
    greet(2 * ((1 - h) * depth + z) + c, (1 - xl) * side + y)

    loads[0].wait()
    loads[1].wait()
    trial_bf[...] = trial[...].astype(BF)
    callers = 2 * (bands - 1) + (chips - 1) + 2
    pl.semaphore_wait(barrier, jnp.where(y == z, callers, callers + side))

    def occ1(i):
        return rdma(
            occ.at[c, block(i * slab, slab)], occ_c.at[c, quarter, z, i], o1_s.at[i], o1_r.at[z],
            2 * goal + c, xl * side + i,
        )

    def occ1_start(i):
        @pl.when((i != y) | (y != z))
        def _():
            occ1(i).start()

    each(side, occ1_start)

    @pl.when(y == z)
    def _():
        occ_c[c, quarter, z, y] = occ[c, block(y * slab, slab), :]

    own_cols = block(b * width, width)

    def tri_same(i):
        return rdma(trial_bf.at[c], trial_all.at[c, own_cols], tri_s.at[0, i], tri_r.at[c, b], mine, band_peer(i))

    def tri_cross(i):
        p = lax.rem(b + i, bands)
        return rdma(trial_bf.at[o], trial_all.at[c, own_cols], tri_s.at[1, i], tri_r.at[c, b], other, p)

    each(bands - 1, lambda i: tri_same(i).start())
    loads[2].wait()
    send_vir = rdma(vir.at[c], vir.at[c], x_s.at[0], x_r.at[0], other, b)
    send_occ = rdma(occ.at[c], occ.at[c], x_s.at[1], x_r.at[1], other, b)
    send_vir.start()
    send_occ.start()
    each(bands, lambda i: tri_cross(i).start())
    trial_all[c, own_cols, :] = trial_bf[c]

    def occ1_wait(i):
        @pl.when((i != z) | (y != z))
        def _():
            rdma(
                occ.at[c, block(y * slab, slab)], occ_c.at[c, quarter, i, y], o1_s.at[0], o1_r.at[i], mine, b
            ).wait_recv()

    each(depth, occ1_wait)

    def piece(q, row):
        return occ_c.at[c, q, :, row]

    def part_a(q, row):
        return occ_c.at[c, q, pl.ds(0, depth // 2), row]

    def part_b(q, row):
        return occ_c.at[c, q, pl.ds(depth // 2, depth // 2), row]

    def x_send(src, send, recv, i):
        q = quarter ^ (i + 1)
        return rdma(src, src, send, recv, 2 * ((q // 2) * depth + z) + c, lax.rem(q, 2) * side + y)

    def y_send(src, send, recv, i):
        return rdma(src, src, send, recv, mine, xl * side + lax.rem(y + 1 + i, side))

    def occ_x(i):
        return x_send(piece(quarter, y), ox_s.at[i], ox_r.at[quarter], i)

    def occ_y(i):
        return y_send(piece(quarter, y), oy_s.at[i], oy_r.at[y], i)

    def occ_xy(q, i):
        return y_send(part_a(q, y), fy_s.at[q, i], fy_r.at[q, y], i)

    def occ_yx(row, i):
        return x_send(part_b(quarter, row), fx_s.at[row, i], fx_r.at[quarter, row], i)

    def landed(dst, recv):
        rdma(dst, dst, x_s.at[0], recv, mine, b).wait_recv()

    each(3, lambda i: occ_x(i).start())
    each(side - 1, lambda i: occ_y(i).start())

    vir_t[c] = vir[c].T

    def tri_wait_same(i):
        p = band_peer(i)
        part = block(p * width, width)
        rdma(trial_bf.at[c], trial_all.at[c, part], tri_s.at[0, i], tri_r.at[c, p], mine, p).wait_recv()

    def tri_wait_cross(i):
        part = block(i * width, width)
        rdma(trial_bf.at[o], trial_all.at[o, part], tri_s.at[1, i], tri_r.at[o, i], other, i).wait_recv()

    def t_copy(s, i):
        return rdma(t_mine.at[h, s], t_all.at[2 * j + s], t_s.at[s, i], t_r.at[s, j], 2 * deep(i) + c, b)

    def t_cross(s):
        return rdma(
            t_mine.at[1 - h, s], t_all.at[2 * j + s], t_s.at[s, depth - 1], t_r.at[s, j], 2 * partner + c, b
        )

    def t_forward(s, i):
        there = t_all.at[2 * partner + s]
        return rdma(there, there, f_s.at[s, i], t_r.at[s, partner], 2 * deep(i) + c, b)

    def t_landed(s, p):
        landed(t_all.at[2 * p + s], t_r.at[s, p])

    def t_make(s):
        value = jnp.dot(vir[s], trial_all[s], preferred_element_type=F32)
        t_mine[0, s] = value[:half].astype(BF)
        t_mine[1, s] = value[half:].astype(BF)
        t_all[2 * j + s] = t_mine[h, s]
        return occ[s].astype(F32) * value

    def t_start(s):
        t_cross(s).start()
        each(depth - 1, lambda i: t_copy(s, i).start())

    each(bands - 1, tri_wait_same)
    local = t_make(c)
    t_start(c)
    rdma(vir.at[c], vir.at[o], x_s.at[0], x_r.at[0], other, b).wait_recv()
    rdma(occ.at[c], occ.at[o], x_s.at[1], x_r.at[1], other, b).wait_recv()
    each(bands, tri_wait_cross)
    local = local + t_make(o)

    high = local.astype(BF)
    low = (local - high.astype(F32)).astype(BF)
    ones = jnp.ones((8, nocc), BF)
    dens1[j] = lax.dot_general(ones, high, ALONG, preferred_element_type=F32) + lax.dot_general(
        ones, low, ALONG, preferred_element_type=F32
    )

    def d1_copy(i):
        return rdma(dens1.at[j], dens1.at[j], d1_s.at[i], d1_r.at[j], 2 * chip_peer(i) + c, b)

    each(chips - 1, lambda i: d1_copy(i).start())
    t_start(o)

    def x_arrived(i):
        q = quarter ^ (i + 1)
        landed(piece(q, y), ox_r.at[q])
        each(side - 1, lambda n: occ_xy(q, n).start())

    def y_arrived(i):
        row = lax.rem(y + 1 + i, side)
        landed(piece(quarter, row), oy_r.at[row])
        each(3, lambda n: occ_yx(row, n).start())

    each(3, x_arrived)
    each(side - 1, y_arrived)

    def t_pass(s):
        t_landed(s, partner)
        each(depth - 1, lambda i: t_forward(s, i).start())

    t_pass(c)
    t_pass(o)

    def occ3(n):
        q = quarter ^ (n // 2)
        there = occ_c.at[c, q, pl.ds(lax.rem(n, 2) * (depth // 2), depth // 2)]
        return rdma(there, there, o3_s.at[n], o3_r.at[n], other, b)

    occ3(0).start()
    occ3(1).start()

    vir_t[o] = vir[o].T
    turn[...] = jnp.zeros_like(turn)
    loads[7].wait()
    loads[8].wait()
    turn[:, 0:width] = jnp.broadcast_to(vir_e[...], (nocc, width))
    gaps = turn[...].T[0:width] - occ_e[...]
    for v in range(2):
        out[v] = gaps * trial[v]

    def occ_rest(i):
        q = quarter ^ (i + 1)

        def from_y(n):
            row = lax.rem(y + 1 + n, side)
            landed(part_a(q, row), fy_r.at[q, row])

        def from_x(n):
            row = lax.rem(y + 1 + n, side)
            landed(part_b(q, row), fx_r.at[q, row])

        each(side - 1, from_y)
        occ3(2 * i + 2).start()
        each(side - 1, from_x)
        occ3(2 * i + 3).start()

    each(3, occ_rest)

    def d1_wait(i):
        p = chip_peer(i)
        rdma(dens1.at[p], dens1.at[p], d1_s.at[i], d1_r.at[p], 2 * p + c, b).wait_recv()

    each(chips - 1, d1_wait)
    total = dens1[0]
    for p in range(1, chips):
        total = total + dens1[p]
    dens2[b] = total

    def d2_copy(i):
        return rdma(dens2.at[b], dens2.at[b], d2_s.at[i], d2_r.at[b], mine, band_peer(i))

    each(bands - 1, lambda i: d2_copy(i).start())

    def t_rest(i):
        near = deep(i)
        far = lax.rem(near + depth, chips)
        for s in range(2):
            t_landed(s, near)
            t_landed(s, far)

    each(depth - 1, t_rest)

    def points_of(p, s, e):
        return occ_c[s, 2 * (p // depth) + e, lax.rem(p, depth)].reshape(rows, nocc)

    def pairs_of(s):
        for p in range(chips):
            for e in range(2):
                pairs[2 * p + s, :, e * rows : (e + 1) * rows] = lax.dot_general(
                    t_all[2 * p + s], points_of(p, s, e), ALONG, preferred_element_type=F32
                ).astype(BF)

    pairs_of(c)

    def d2_wait(i):
        p = band_peer(i)
        rdma(dens2.at[p], dens2.at[p], d2_s.at[i], d2_r.at[p], mine, p).wait_recv()

    each(bands - 1, d2_wait)
    loads[6].wait()
    pot = jnp.zeros((rows, nocc), F32)
    for p in range(bands):
        line = jnp.broadcast_to(dens2[p][0:1, :].astype(BF), (nocc, rows))
        pot = pot + lax.dot_general(coul[:, p * rows : (p + 1) * rows], line, ALONG, preferred_element_type=F32)
    pot = pot * 2.0
    for s in range(2):
        acc_w[s] = pot * occ[s].astype(F32)

    def occ3_wait(n):
        q = quarter ^ (n // 2)
        landed(occ_c.at[o, q, pl.ds(lax.rem(n, 2) * (depth // 2), depth // 2)], o3_r.at[n])

    each(8, occ3_wait)

    pairs_of(o)
    loads[3].wait()
    loads[4].wait()
    loads[5].wait()

    tile = 16
    fours = 4

    def u_copy(dest, s):
        return rdma(u_send.at[2 * dest + s], u_recv.at[j, s], u_s.at[s, dest], u_r.at[s, j], 2 * dest + c, b)

    def screen(g, s):
        dests = [j ^ (chips - 1 - fours * g - n) for n in range(fours)]

        def rows_step(r):
            part = block(r * tile, tile)
            for n, dest in enumerate(dests):
                acc = jnp.zeros((tile, cols), F32)
                for q in range(nk):
                    acc = acc + pairs[minus[2 * dest + s, q], part, :].astype(F32) * k_bf[q, part, :].astype(F32)
                s_bf[n, part, :] = acc.astype(BF)

        each(half // tile, rows_step)
        for n, dest in enumerate(dests):
            part_sum = jnp.dot(s_bf[n, :, :rows], points_of(dest, s, 0), preferred_element_type=F32)
            part_sum = part_sum + jnp.dot(s_bf[n, :, rows:], points_of(dest, s, 1), preferred_element_type=F32)
            u_send[2 * dest + s] = part_sum.astype(BF)

            @pl.when(dest != j)
            def _():
                u_copy(dest, s).start()

    def finish(s):
        mine_rows = block(h * half, half)
        acc_w[s, mine_rows, :] = acc_w[s, mine_rows, :] - u_send[2 * j + s].astype(F32)

        def u_arrived(i):
            p = chip_peer(i)
            rdma(u_send.at[2 * p + s], u_recv.at[p, s], u_s.at[s, p], u_r.at[s, p], 2 * p + c, b).wait_recv()
            part = block((p // depth) * half, half)
            acc_w[s, part, :] = acc_w[s, part, :] - u_recv[p, s].astype(F32)

        each(chips - 1, u_arrived)
        sig_send[s] = jnp.dot(vir_t[s], acc_w[s].astype(BF), preferred_element_type=F32).astype(BF)

        def sig_start(p):
            @pl.when((c != s) | (p != b))
            def _():
                sig_copy(s, p).start()

        each(bands, sig_start)

        @pl.when(c == s)
        def _():
            sig_recv[c, b] = sig_send[s, own_cols, :]

    def sig_copy(s, p):
        return rdma(
            sig_send.at[s, block(p * width, width)], sig_recv.at[c, b], g_s.at[s, p], g_r.at[c, b], 2 * j + s, p
        )

    screen(0, 0)
    screen(1, 0)
    screen(0, 1)

    screen(1, 1)
    finish(0)
    finish(1)

    def sig_wait_same(i):
        p = band_peer(i)
        rdma(sig_send.at[0, own_cols], sig_recv.at[c, p], g_s.at[0, i], g_r.at[c, p], mine, p).wait_recv()

    def sig_wait_cross(i):
        rdma(sig_send.at[0, own_cols], sig_recv.at[o, i], g_s.at[1, i], g_r.at[o, i], other, i).wait_recv()

    each(bands - 1, sig_wait_same)
    each(bands, sig_wait_cross)
    for v in range(2):
        sums = sig_recv[v, 0].astype(F32)
        for p in range(1, bands):
            sums = sums + sig_recv[v, p].astype(F32)
        out[v] = out[v] + sums

    each(bands - 1, lambda i: tri_same(i).wait_send())
    each(bands, lambda i: tri_cross(i).wait_send())

    def occ1_sent(i):
        @pl.when((i != y) | (y != z))
        def _():
            occ1(i).wait_send()

    each(side, occ1_sent)
    send_vir.wait_send()
    send_occ.wait_send()
    each(3, lambda i: occ_x(i).wait_send())
    each(side - 1, lambda i: occ_y(i).wait_send())

    def forwarded(i):
        each(side - 1, lambda n: occ_xy(quarter ^ (i + 1), n).wait_send())
        each(3, lambda n: occ_yx(lax.rem(y + 1 + i, side), n).wait_send())

    each(3, forwarded)
    each(8, lambda n: occ3(n).wait_send())
    each(chips - 1, lambda i: d1_copy(i).wait_send())
    each(bands - 1, lambda i: d2_copy(i).wait_send())
    for s in range(2):
        each(depth - 1, lambda i: t_copy(s, i).wait_send())
        t_cross(s).wait_send()
        each(depth - 1, lambda i: t_forward(s, i).wait_send())
        each(chips - 1, lambda i: u_copy(chip_peer(i), s).wait_send())

        def sig_sent(p):
            @pl.when((c != s) | (p != b))
            def _():
                sig_copy(s, p).wait_send()

        each(bands, sig_sent)


def solution(mesh):
    bands = mesh.shape["band"]
    chips = mesh.shape["ka"] // 2

    def per_device(occ, vir, trial, occ_energy, vir_energy, coulomb, exch, minus):
        nk, rows, aux = exch.shape
        nocc = occ.shape[2]
        nvir = vir.shape[2]
        width = trial.shape[3]
        half = rows // 2
        cols = 2 * rows
        turned = jnp.transpose(trial[0], (0, 2, 1))
        far = pl.BlockSpec(memory_space=pltpu.HBM)
        dma = pltpu.SemaphoreType.DMA
        result = pl.pallas_call(
            kernel,
            out_shape=jax.ShapeDtypeStruct((2, width, nocc), F32),
            in_specs=[far] * 8,
            out_specs=pl.BlockSpec(memory_space=pltpu.VMEM),
            scratch_shapes=[
                pltpu.SMEM((nk, nk), jnp.int32),
                pltpu.VMEM((2, width, nocc), F32),
                pltpu.VMEM((2, rows, nocc), BF),
                pltpu.VMEM((2, rows, nvir), BF),
                pltpu.VMEM((1, nocc), F32),
                pltpu.VMEM((1, width), F32),
                pltpu.VMEM((nocc, 128), F32),
                pltpu.VMEM((2, width, nocc), BF),
                pltpu.VMEM((2, nvir, nocc), BF),
                pltpu.VMEM((2, nvir, rows), BF),
                pltpu.VMEM((2, 2, half, nocc), BF),
                pltpu.VMEM((nk, half, nocc), BF),
                pltpu.VMEM((2, 4, chips // 2, bands // 2, 2 * rows // bands, nocc), BF),
                pltpu.VMEM((nk, half, cols), BF),
                pltpu.VMEM((nk, half, cols), BF),
                pltpu.VMEM((4, half, cols), BF),
                pltpu.VMEM((nk, half, nocc), BF),
                pltpu.VMEM((chips, 2, half, nocc), BF),
                pltpu.VMEM((2, rows, nocc), F32),
                pltpu.VMEM((chips, 8, rows), F32),
                pltpu.VMEM((bands, 8, rows), F32),
                pltpu.VMEM((rows, aux), BF),
                pltpu.VMEM((2, nvir, nocc), BF),
                pltpu.VMEM((2, bands, width, nocc), BF),
                dma((2, bands)), dma((2, bands)),
                dma((2,)), dma((2,)),
                dma((bands // 2,)), dma((chips // 2,)),
                dma((3,)), dma((4,)),
                dma((3,)), dma((bands // 2,)),
                dma((4, 3)), dma((4, bands // 2)),
                dma((bands // 2, 3)), dma((4, bands // 2)),
                dma((8,)), dma((8,)),
                dma((2, 4)), dma((2, 4)), dma((2, chips)),
                dma((chips,)), dma((chips,)),
                dma((bands,)), dma((bands,)),
                dma((2, chips)), dma((2, chips)),
                dma((2, bands)), dma((2, bands)),
                dma((9,)),
            ],
            compiler_params=pltpu.CompilerParams(
                collective_id=0, has_side_effects=True, vmem_limit_bytes=67043328
            ),
            name="sigma",
        )(minus, turned, occ[0], vir[0], coulomb, exch, occ_energy, vir_energy)
        return jnp.transpose(result, (0, 2, 1))[None]

    in_specs = (
        P("ka", "band", None),
        P("ka", "band", None),
        P("ka", None, None, "band"),
        P("ka", None),
        P("ka", "band"),
        P("band", None),
        P(None, "band", None),
        P(),
    )
    return jax.shard_map(
        per_device,
        mesh=mesh,
        in_specs=in_specs,
        out_specs=P("ka", None, None, "band"),
        check_vma=False,
    )
```

```python
import jax
import jax.numpy as jnp
from jax import lax
from jax.experimental import pallas as pl
from jax.experimental.pallas import tpu as pltpu
from jax.sharding import PartitionSpec as P

BF = jnp.bfloat16
F32 = jnp.float32
MESH = pl.DeviceIdType.MESH
ALONG = (((1,), (1,)), ((), ()))


def each(count, body):
    def step(i, carry):
        body(i)
        return carry

    lax.fori_loop(0, count, step, 0)


def rdma(src, dst, send, recv, ka, band):
    return pltpu.make_async_remote_copy(
        src_ref=src,
        dst_ref=dst,
        send_sem=send,
        recv_sem=recv,
        device_id={"ka": ka, "band": band},
        device_id_type=MESH,
    )


def kernel(
    minus_h, trial_h, occ_h, vir_h, coulomb, exch, occ_e_h, vir_e_h, out,
    minus, trial, occ, vir, occ_e, vir_e, turn, trial_bf, trial_all, vir_t, t_mine, t_all, occ_c, k_bf, pairs, s_bf,
    u_send, u_recv, acc_w, dens1, dens2, coul, sig_send, sig_recv,
    tri_s, tri_r, x_s, x_r, o1_s, o1_r, ox_s, ox_r, oy_s, oy_r, fy_s, fy_r, fx_s, fx_r, o3_s, o3_r, t_s, f_s, t_r, d1_s, d1_r, d2_s, d2_r,
    u_s, u_r, g_s, g_r, loc,
):
    bands = lax.axis_size("band")
    chips = lax.axis_size("ka") // 2
    depth = chips // 2
    ka = lax.axis_index("ka")
    b = lax.axis_index("band")
    j = ka // 2
    c = lax.rem(ka, 2)
    o = 1 - c
    h = j // depth
    z = lax.rem(j, depth)
    side = bands // 2
    xl = b // side
    y = lax.rem(b, side)
    quarter = 2 * h + xl
    mine = 2 * j + c
    other = 2 * j + o
    rows, nocc = occ_h.shape
    half = rows // 2
    width = trial.shape[1]
    nk = exch.shape[0]
    slab = rows // side
    cols = pairs.shape[2]
    home = xl * side + z
    goal = h * depth + y
    partner = (1 - h) * depth + z

    def band_peer(i):
        return lax.rem(b + 1 + i, bands)

    def chip_peer(i):
        return lax.rem(j + 1 + i, chips)

    def block(start, size, unit=16):
        return pl.ds(pl.multiple_of(start, unit), size)

    loads = [
        pltpu.make_async_copy(occ_h, occ.at[c], loc.at[0]),
        pltpu.make_async_copy(trial_h, trial, loc.at[1]),
        pltpu.make_async_copy(vir_h, vir.at[c], loc.at[2]),
        pltpu.make_async_copy(
            exch.at[:, block(h * half, half), block(z * rows, rows, 128)], k_bf.at[:, :, pl.ds(0, rows)], loc.at[3]
        ),
        pltpu.make_async_copy(
            exch.at[:, block(h * half, half), block((z + side) * rows, rows, 128)],
            k_bf.at[:, :, pl.ds(rows, rows)], loc.at[8],
        ),
        pltpu.make_async_copy(minus_h, minus, loc.at[4]),
        pltpu.make_async_copy(coulomb, coul, loc.at[5]),
        pltpu.make_async_copy(occ_e_h, occ_e, loc.at[6]),
        pltpu.make_async_copy(vir_e_h, vir_e, loc.at[7]),
    ]
    for load in loads:
        load.start()

    barrier = pltpu.get_barrier_semaphore()

    def greet(k, band):
        pl.semaphore_signal(barrier, inc=1, device_id={"ka": k, "band": band}, device_id_type=MESH)

    def greet_band(i):
        greet(mine, band_peer(i))
        greet(other, band_peer(i))

    def deep(i):
        return h * depth + lax.rem(z + 1 + i, depth)

    each(bands - 1, greet_band)
    each(chips - 1, lambda i: greet(2 * chip_peer(i) + c, b))
    each(depth - 1, lambda i: greet(2 * deep(i) + c, home))
    greet(other, b)
    greet(2 * ((1 - h) * depth + z) + c, (1 - xl) * side + y)

    loads[0].wait()
    loads[1].wait()
    trial_bf[...] = trial[...].astype(BF)
    callers = 2 * (bands - 1) + (chips - 1) + 2
    pl.semaphore_wait(barrier, jnp.where(y == z, callers, callers + side))

    def occ1(i):
        return rdma(
            occ.at[c, block(i * slab, slab)], occ_c.at[c, quarter, z, i], o1_s.at[i], o1_r.at[z],
            2 * goal + c, xl * side + i,
        )

    def occ1_start(i):
        @pl.when((i != y) | (y != z))
        def _():
            occ1(i).start()

    each(side, occ1_start)

    @pl.when(y == z)
    def _():
        occ_c[c, quarter, z, y] = occ[c, block(y * slab, slab), :]

    own_cols = block(b * width, width)

    def tri_same(i):
        return rdma(trial_bf.at[c], trial_all.at[c, own_cols], tri_s.at[0, i], tri_r.at[c, b], mine, band_peer(i))

    def tri_cross(i):
        p = lax.rem(b + i, bands)
        return rdma(trial_bf.at[o], trial_all.at[c, own_cols], tri_s.at[1, i], tri_r.at[c, b], other, p)

    each(bands - 1, lambda i: tri_same(i).start())
    loads[2].wait()
    send_vir = rdma(vir.at[c], vir.at[c], x_s.at[0], x_r.at[0], other, b)
    send_occ = rdma(occ.at[c], occ.at[c], x_s.at[1], x_r.at[1], other, b)
    send_vir.start()
    send_occ.start()
    each(bands, lambda i: tri_cross(i).start())
    trial_all[c, own_cols, :] = trial_bf[c]

    def occ1_wait(i):
        @pl.when((i != z) | (y != z))
        def _():
            rdma(
                occ.at[c, block(y * slab, slab)], occ_c.at[c, quarter, i, y], o1_s.at[0], o1_r.at[i], mine, b
            ).wait_recv()

    each(depth, occ1_wait)

    def piece(q, row):
        return occ_c.at[c, q, :, row]

    def part_a(q, row):
        return occ_c.at[c, q, pl.ds(0, depth // 2), row]

    def part_b(q, row):
        return occ_c.at[c, q, pl.ds(depth // 2, depth // 2), row]

    def x_send(src, send, recv, i):
        q = quarter ^ (i + 1)
        return rdma(src, src, send, recv, 2 * ((q // 2) * depth + z) + c, lax.rem(q, 2) * side + y)

    def y_send(src, send, recv, i):
        return rdma(src, src, send, recv, mine, xl * side + lax.rem(y + 1 + i, side))

    def occ_x(i):
        return x_send(piece(quarter, y), ox_s.at[i], ox_r.at[quarter], i)

    def occ_y(i):
        return y_send(piece(quarter, y), oy_s.at[i], oy_r.at[y], i)

    def occ_xy(q, i):
        return y_send(part_a(q, y), fy_s.at[q, i], fy_r.at[q, y], i)

    def occ_yx(row, i):
        return x_send(part_b(quarter, row), fx_s.at[row, i], fx_r.at[quarter, row], i)

    def landed(dst, recv):
        rdma(dst, dst, x_s.at[0], recv, mine, b).wait_recv()

    each(3, lambda i: occ_x(i).start())
    each(side - 1, lambda i: occ_y(i).start())

    vir_t[c] = vir[c].T

    def tri_wait_same(i):
        p = band_peer(i)
        part = block(p * width, width)
        rdma(trial_bf.at[c], trial_all.at[c, part], tri_s.at[0, i], tri_r.at[c, p], mine, p).wait_recv()

    def tri_wait_cross(i):
        part = block(i * width, width)
        rdma(trial_bf.at[o], trial_all.at[o, part], tri_s.at[1, i], tri_r.at[o, i], other, i).wait_recv()

    def t_copy(s, i):
        return rdma(t_mine.at[h, s], t_all.at[2 * j + s], t_s.at[s, i], t_r.at[s, j], 2 * deep(i) + c, b)

    def t_cross(s):
        return rdma(
            t_mine.at[1 - h, s], t_all.at[2 * j + s], t_s.at[s, depth - 1], t_r.at[s, j], 2 * partner + c, b
        )

    def t_forward(s, i):
        there = t_all.at[2 * partner + s]
        return rdma(there, there, f_s.at[s, i], t_r.at[s, partner], 2 * deep(i) + c, b)

    def t_landed(s, p):
        landed(t_all.at[2 * p + s], t_r.at[s, p])

    def t_make(s):
        value = jnp.dot(vir[s], trial_all[s], preferred_element_type=F32)
        t_mine[0, s] = value[:half].astype(BF)
        t_mine[1, s] = value[half:].astype(BF)
        t_all[2 * j + s] = t_mine[h, s]
        return occ[s].astype(F32) * value

    def t_start(s):
        t_cross(s).start()
        each(depth - 1, lambda i: t_copy(s, i).start())

    each(bands - 1, tri_wait_same)
    local = t_make(c)
    t_start(c)
    rdma(vir.at[c], vir.at[o], x_s.at[0], x_r.at[0], other, b).wait_recv()
    rdma(occ.at[c], occ.at[o], x_s.at[1], x_r.at[1], other, b).wait_recv()
    each(bands, tri_wait_cross)
    local = local + t_make(o)

    high = local.astype(BF)
    low = (local - high.astype(F32)).astype(BF)
    ones = jnp.ones((8, nocc), BF)
    dens1[j] = lax.dot_general(ones, high, ALONG, preferred_element_type=F32) + lax.dot_general(
        ones, low, ALONG, preferred_element_type=F32
    )

    def d1_copy(i):
        return rdma(dens1.at[j], dens1.at[j], d1_s.at[i], d1_r.at[j], 2 * chip_peer(i) + c, b)

    each(chips - 1, lambda i: d1_copy(i).start())
    t_start(o)

    def x_arrived(i):
        q = quarter ^ (i + 1)
        landed(piece(q, y), ox_r.at[q])
        each(side - 1, lambda n: occ_xy(q, n).start())

    def y_arrived(i):
        row = lax.rem(y + 1 + i, side)
        landed(piece(quarter, row), oy_r.at[row])
        each(3, lambda n: occ_yx(row, n).start())

    each(3, x_arrived)
    each(side - 1, y_arrived)

    def t_pass(s):
        t_landed(s, partner)
        each(depth - 1, lambda i: t_forward(s, i).start())

    t_pass(c)
    t_pass(o)

    def occ3(n):
        q = quarter ^ (n // 2)
        there = occ_c.at[c, q, pl.ds(lax.rem(n, 2) * (depth // 2), depth // 2)]
        return rdma(there, there, o3_s.at[n], o3_r.at[n], other, b)

    occ3(0).start()
    occ3(1).start()

    vir_t[o] = vir[o].T
    turn[...] = jnp.zeros_like(turn)
    loads[7].wait()
    loads[8].wait()
    turn[:, 0:width] = jnp.broadcast_to(vir_e[...], (nocc, width))
    gaps = turn[...].T[0:width] - occ_e[...]
    for v in range(2):
        out[v] = gaps * trial[v]

    def occ_rest(i):
        q = quarter ^ (i + 1)

        def from_y(n):
            row = lax.rem(y + 1 + n, side)
            landed(part_a(q, row), fy_r.at[q, row])

        def from_x(n):
            row = lax.rem(y + 1 + n, side)
            landed(part_b(q, row), fx_r.at[q, row])

        each(side - 1, from_y)
        occ3(2 * i + 2).start()
        each(side - 1, from_x)
        occ3(2 * i + 3).start()

    each(3, occ_rest)

    def d1_wait(i):
        p = chip_peer(i)
        rdma(dens1.at[p], dens1.at[p], d1_s.at[i], d1_r.at[p], 2 * p + c, b).wait_recv()

    each(chips - 1, d1_wait)
    total = dens1[0]
    for p in range(1, chips):
        total = total + dens1[p]
    dens2[b] = total

    def d2_copy(i):
        return rdma(dens2.at[b], dens2.at[b], d2_s.at[i], d2_r.at[b], mine, band_peer(i))

    each(bands - 1, lambda i: d2_copy(i).start())

    def t_rest(i):
        near = deep(i)
        far = lax.rem(near + depth, chips)
        for s in range(2):
            t_landed(s, near)
            t_landed(s, far)

    each(depth - 1, t_rest)

    def points_of(p, s, e):
        return occ_c[s, 2 * (p // depth) + e, lax.rem(p, depth)].reshape(rows, nocc)

    def pairs_of(s):
        for p in range(chips):
            for e in range(2):
                pairs[2 * p + s, :, e * rows : (e + 1) * rows] = lax.dot_general(
                    t_all[2 * p + s], points_of(p, s, e), ALONG, preferred_element_type=F32
                ).astype(BF)

    pairs_of(c)

    def occ3_wait(n):
        q = quarter ^ (n // 2)
        landed(occ_c.at[o, q, pl.ds(lax.rem(n, 2) * (depth // 2), depth // 2)], o3_r.at[n])

    each(8, occ3_wait)

    pairs_of(o)
    loads[3].wait()
    loads[4].wait()
    loads[5].wait()

    tile = 16
    fours = 4

    def u_copy(dest, s):
        return rdma(u_send.at[2 * dest + s], u_recv.at[j, s], u_s.at[s, dest], u_r.at[s, j], 2 * dest + c, b)

    def screen(g, s):
        dests = [j ^ (chips - 1 - fours * g - n) for n in range(fours)]

        def rows_step(r):
            part = block(r * tile, tile)
            for n, dest in enumerate(dests):
                acc = jnp.zeros((tile, cols), F32)
                for q in range(nk):
                    acc = acc + pairs[minus[2 * dest + s, q], part, :].astype(F32) * k_bf[q, part, :].astype(F32)
                s_bf[n, part, :] = acc.astype(BF)

        each(half // tile, rows_step)
        sums = []
        for n, dest in enumerate(dests):
            left = jnp.dot(s_bf[n, :, :rows], points_of(dest, s, 0), preferred_element_type=F32)
            sums.append(left + jnp.dot(s_bf[n, :, rows:], points_of(dest, s, 1), preferred_element_type=F32))
        for n, dest in enumerate(dests):
            u_send[2 * dest + s] = sums[n].astype(BF)
        for n, dest in enumerate(dests):
            if chips - 1 - fours * g - n:
                u_copy(dest, s).start()

    def finish(s):
        mine_rows = block(h * half, half)
        acc_w[s, mine_rows, :] = acc_w[s, mine_rows, :] - u_send[2 * j + s].astype(F32)

        def u_arrived(i):
            p = chip_peer(i)
            rdma(u_send.at[2 * p + s], u_recv.at[p, s], u_s.at[s, p], u_r.at[s, p], 2 * p + c, b).wait_recv()
            part = block((p // depth) * half, half)
            acc_w[s, part, :] = acc_w[s, part, :] - u_recv[p, s].astype(F32)

        each(chips - 1, u_arrived)
        sig_send[s] = jnp.dot(vir_t[s], acc_w[s].astype(BF), preferred_element_type=F32).astype(BF)

        def sig_start(p):
            @pl.when((c != s) | (p != b))
            def _():
                sig_copy(s, p).start()

        each(bands, sig_start)

        @pl.when(c == s)
        def _():
            sig_recv[c, b] = sig_send[s, own_cols, :]

    def sig_copy(s, p):
        return rdma(
            sig_send.at[s, block(p * width, width)], sig_recv.at[c, b], g_s.at[s, p], g_r.at[c, b], 2 * j + s, p
        )

    screen(0, 0)
    screen(1, 0)
    screen(0, 1)

    screen(1, 1)
    def d2_wait(i):
        p = band_peer(i)
        rdma(dens2.at[p], dens2.at[p], d2_s.at[i], d2_r.at[p], mine, p).wait_recv()

    each(bands - 1, d2_wait)
    loads[6].wait()
    pot = jnp.zeros((rows, nocc), F32)
    for p in range(bands):
        line = jnp.broadcast_to(dens2[p][0:1, :].astype(BF), (nocc, rows))
        pot = pot + lax.dot_general(coul[:, p * rows : (p + 1) * rows], line, ALONG, preferred_element_type=F32)
    pot = pot * 2.0
    for s in range(2):
        acc_w[s] = pot * occ[s].astype(F32)

    finish(0)
    each(bands - 1, lambda i: tri_same(i).wait_send())
    each(bands, lambda i: tri_cross(i).wait_send())

    def occ1_sent(i):
        @pl.when((i != y) | (y != z))
        def _():
            occ1(i).wait_send()

    each(side, occ1_sent)
    send_vir.wait_send()
    send_occ.wait_send()
    each(3, lambda i: occ_x(i).wait_send())
    each(side - 1, lambda i: occ_y(i).wait_send())

    def forwarded(i):
        each(side - 1, lambda n: occ_xy(quarter ^ (i + 1), n).wait_send())
        each(3, lambda n: occ_yx(lax.rem(y + 1 + i, side), n).wait_send())

    each(3, forwarded)
    each(8, lambda n: occ3(n).wait_send())
    each(chips - 1, lambda i: d1_copy(i).wait_send())
    each(bands - 1, lambda i: d2_copy(i).wait_send())
    for s in range(2):
        each(depth - 1, lambda i: t_copy(s, i).wait_send())
        t_cross(s).wait_send()
        each(depth - 1, lambda i: t_forward(s, i).wait_send())

    finish(1)

    def sig_wait_same(i):
        p = band_peer(i)
        rdma(sig_send.at[0, own_cols], sig_recv.at[c, p], g_s.at[0, i], g_r.at[c, p], mine, p).wait_recv()

    def sig_wait_cross(i):
        rdma(sig_send.at[0, own_cols], sig_recv.at[o, i], g_s.at[1, i], g_r.at[o, i], other, i).wait_recv()

    each(bands - 1, sig_wait_same)
    each(bands, sig_wait_cross)
    for v in range(2):
        sums = sig_recv[v, 0].astype(F32)
        for p in range(1, bands):
            sums = sums + sig_recv[v, p].astype(F32)
        out[v] = out[v] + sums

    for s in range(2):
        each(chips - 1, lambda i: u_copy(chip_peer(i), s).wait_send())

        def sig_sent(p):
            @pl.when((c != s) | (p != b))
            def _():
                sig_copy(s, p).wait_send()

        each(bands, sig_sent)


def solution(mesh):
    bands = mesh.shape["band"]
    chips = mesh.shape["ka"] // 2

    def per_device(occ, vir, trial, occ_energy, vir_energy, coulomb, exch, minus):
        nk, rows, aux = exch.shape
        nocc = occ.shape[2]
        nvir = vir.shape[2]
        width = trial.shape[3]
        half = rows // 2
        cols = 2 * rows
        turned = jnp.transpose(trial[0], (0, 2, 1))
        far = pl.BlockSpec(memory_space=pltpu.HBM)
        dma = pltpu.SemaphoreType.DMA
        result = pl.pallas_call(
            kernel,
            out_shape=jax.ShapeDtypeStruct((2, width, nocc), F32),
            in_specs=[far] * 8,
            out_specs=pl.BlockSpec(memory_space=pltpu.VMEM),
            scratch_shapes=[
                pltpu.SMEM((nk, nk), jnp.int32),
                pltpu.VMEM((2, width, nocc), F32),
                pltpu.VMEM((2, rows, nocc), BF),
                pltpu.VMEM((2, rows, nvir), BF),
                pltpu.VMEM((1, nocc), F32),
                pltpu.VMEM((1, width), F32),
                pltpu.VMEM((nocc, 128), F32),
                pltpu.VMEM((2, width, nocc), BF),
                pltpu.VMEM((2, nvir, nocc), BF),
                pltpu.VMEM((2, nvir, rows), BF),
                pltpu.VMEM((2, 2, half, nocc), BF),
                pltpu.VMEM((nk, half, nocc), BF),
                pltpu.VMEM((2, 4, chips // 2, bands // 2, 2 * rows // bands, nocc), BF),
                pltpu.VMEM((nk, half, cols), BF),
                pltpu.VMEM((nk, half, cols), BF),
                pltpu.VMEM((4, half, cols), BF),
                pltpu.VMEM((nk, half, nocc), BF),
                pltpu.VMEM((chips, 2, half, nocc), BF),
                pltpu.VMEM((2, rows, nocc), F32),
                pltpu.VMEM((chips, 8, rows), F32),
                pltpu.VMEM((bands, 8, rows), F32),
                pltpu.VMEM((rows, aux), BF),
                pltpu.VMEM((2, nvir, nocc), BF),
                pltpu.VMEM((2, bands, width, nocc), BF),
                dma((2, bands)), dma((2, bands)),
                dma((2,)), dma((2,)),
                dma((bands // 2,)), dma((chips // 2,)),
                dma((3,)), dma((4,)),
                dma((3,)), dma((bands // 2,)),
                dma((4, 3)), dma((4, bands // 2)),
                dma((bands // 2, 3)), dma((4, bands // 2)),
                dma((8,)), dma((8,)),
                dma((2, 4)), dma((2, 4)), dma((2, chips)),
                dma((chips,)), dma((chips,)),
                dma((bands,)), dma((bands,)),
                dma((2, chips)), dma((2, chips)),
                dma((2, bands)), dma((2, bands)),
                dma((9,)),
            ],
            compiler_params=pltpu.CompilerParams(
                collective_id=0, has_side_effects=True, vmem_limit_bytes=67043328
            ),
            name="sigma",
        )(minus, turned, occ[0], vir[0], coulomb, exch, occ_energy, vir_energy)
        return jnp.transpose(result, (0, 2, 1))[None]

    in_specs = (
        P("ka", "band", None),
        P("ka", "band", None),
        P("ka", None, None, "band"),
        P("ka", None),
        P("ka", "band"),
        P("band", None),
        P(None, "band", None),
        P(),
    )
    return jax.shard_map(
        per_device,
        mesh=mesh,
        in_specs=in_specs,
        out_specs=P("ka", None, None, "band"),
        check_vma=False,
    )
```

```python
import jax
import jax.numpy as jnp
from jax import lax
from jax.experimental import pallas as pl
from jax.experimental.pallas import tpu as pltpu
from jax.sharding import PartitionSpec as P

BF = jnp.bfloat16
F32 = jnp.float32
MESH = pl.DeviceIdType.MESH
ALONG = (((1,), (1,)), ((), ()))


def each(count, body):
    def step(i, carry):
        body(i)
        return carry

    lax.fori_loop(0, count, step, 0)


def rdma(src, dst, send, recv, ka, band):
    return pltpu.make_async_remote_copy(
        src_ref=src,
        dst_ref=dst,
        send_sem=send,
        recv_sem=recv,
        device_id={"ka": ka, "band": band},
        device_id_type=MESH,
    )


def kernel(
    minus_h, trial_h, occ_h, vir_h, coulomb, exch, occ_e_h, vir_e_h, out,
    minus, trial, occ, vir, occ_e, vir_e, turn, trial_bf, trial_all, vir_t, t_mine, t_all, occ_c, k_bf, pairs, s_bf,
    u_send, u_recv, acc_w, dens1, dens2, coul, sig_send, sig_recv,
    tri_s, tri_r, tri_f, x_s, x_r, o1_s, o1_r, ox_s, ox_r, oy_s, oy_r, fy_s, fy_r, fx_s, fx_r, o3_s, o3_r, t_s, f_s, t_r, d1_s, d1_r, d2_s, d2_r,
    u_s, u_r, g_s, g_r, loc,
):
    bands = lax.axis_size("band")
    chips = lax.axis_size("ka") // 2
    depth = chips // 2
    ka = lax.axis_index("ka")
    b = lax.axis_index("band")
    j = ka // 2
    c = lax.rem(ka, 2)
    o = 1 - c
    h = j // depth
    z = lax.rem(j, depth)
    side = bands // 2
    xl = b // side
    y = lax.rem(b, side)
    quarter = 2 * h + xl
    mine = 2 * j + c
    other = 2 * j + o
    rows, nocc = occ_h.shape
    half = rows // 2
    width = trial.shape[1]
    nk = exch.shape[0]
    slab = rows // side
    cols = pairs.shape[2]
    home = xl * side + z
    goal = h * depth + y
    partner = (1 - h) * depth + z

    def band_peer(i):
        return lax.rem(b + 1 + i, bands)

    def chip_peer(i):
        return lax.rem(j + 1 + i, chips)

    def block(start, size, unit=16):
        return pl.ds(pl.multiple_of(start, unit), size)

    loads = [
        pltpu.make_async_copy(occ_h, occ.at[c], loc.at[0]),
        pltpu.make_async_copy(trial_h, trial, loc.at[1]),
        pltpu.make_async_copy(vir_h, vir.at[c], loc.at[2]),
        pltpu.make_async_copy(
            exch.at[:, block(h * half, half), block(z * rows, rows, 128)], k_bf.at[:, :, pl.ds(0, rows)], loc.at[3]
        ),
        pltpu.make_async_copy(
            exch.at[:, block(h * half, half), block((z + side) * rows, rows, 128)],
            k_bf.at[:, :, pl.ds(rows, rows)], loc.at[8],
        ),
        pltpu.make_async_copy(minus_h, minus, loc.at[4]),
        pltpu.make_async_copy(coulomb, coul, loc.at[5]),
        pltpu.make_async_copy(occ_e_h, occ_e, loc.at[6]),
        pltpu.make_async_copy(vir_e_h, vir_e, loc.at[7]),
    ]
    for load in loads:
        load.start()

    barrier = pltpu.get_barrier_semaphore()

    def greet(k, band):
        pl.semaphore_signal(barrier, inc=1, device_id={"ka": k, "band": band}, device_id_type=MESH)

    def greet_band(i):
        greet(mine, band_peer(i))
        greet(other, band_peer(i))

    def deep(i):
        return h * depth + lax.rem(z + 1 + i, depth)

    each(bands - 1, greet_band)
    each(chips - 1, lambda i: greet(2 * chip_peer(i) + c, b))
    each(depth - 1, lambda i: greet(2 * deep(i) + c, home))
    greet(other, b)
    greet(2 * ((1 - h) * depth + z) + c, (1 - xl) * side + y)

    loads[0].wait()
    loads[1].wait()
    trial_bf[...] = trial[...].astype(BF)
    callers = 2 * (bands - 1) + (chips - 1) + 2
    pl.semaphore_wait(barrier, jnp.where(y == z, callers, callers + side))

    def occ1(i):
        return rdma(
            occ.at[c, block(i * slab, slab)], occ_c.at[c, quarter, z, i], o1_s.at[i], o1_r.at[z],
            2 * goal + c, xl * side + i,
        )

    def occ1_start(i):
        @pl.when((i != y) | (y != z))
        def _():
            occ1(i).start()

    each(side, occ1_start)

    @pl.when(y == z)
    def _():
        occ_c[c, quarter, z, y] = occ[c, block(y * slab, slab), :]

    own_cols = block(b * width, width)

    facing = (1 - xl) * side + y

    def beside(i):
        return xl * side + lax.rem(y + 1 + i, side)

    def behind(i):
        return (1 - xl) * side + lax.rem(y + 1 + i, side)

    def tri_copy(w, n, p):
        vector, chip_core = ((c, mine), (o, other))[w]
        return rdma(trial_bf.at[vector], trial_all.at[c, own_cols], tri_s.at[w, n], tri_r.at[c, b], chip_core, p)

    def tri_out(w, n):
        return tri_copy(w, n, (facing, beside(0), beside(1), beside(2), b)[n])

    tri_order = [(0, 0), (1, 0), (0, 1), (0, 2), (0, 3), (1, 1), (1, 2), (1, 3), (1, 4)]
    for w, n in tri_order[:5]:
        tri_out(w, n).start()
    loads[2].wait()
    send_vir = rdma(vir.at[c], vir.at[c], x_s.at[0], x_r.at[0], other, b)
    send_occ = rdma(occ.at[c], occ.at[c], x_s.at[1], x_r.at[1], other, b)
    send_vir.start()
    send_occ.start()
    for w, n in tri_order[5:]:
        tri_out(w, n).start()
    trial_all[c, own_cols, :] = trial_bf[c]

    def landed(dst, recv):
        rdma(dst, dst, x_s.at[0], recv, mine, b).wait_recv()

    def tri_piece(s, p):
        return trial_all.at[s, block(p * width, width)]

    def tri_landed(s, p):
        landed(tri_piece(s, p), tri_r.at[s, p])

    def tri_pass(s, i):
        return rdma(
            tri_piece(s, facing), tri_piece(s, facing), tri_f.at[s, i], tri_r.at[s, facing], mine, beside(i)
        )

    for s in (c, o):
        tri_landed(s, facing)
        for i in range(side - 1):
            tri_pass(s, i).start()

    def occ1_wait(i):
        @pl.when((i != z) | (y != z))
        def _():
            rdma(
                occ.at[c, block(y * slab, slab)], occ_c.at[c, quarter, i, y], o1_s.at[0], o1_r.at[i], mine, b
            ).wait_recv()

    each(depth, occ1_wait)

    def piece(q, row):
        return occ_c.at[c, q, :, row]

    def part_a(q, row):
        return occ_c.at[c, q, pl.ds(0, depth // 2), row]

    def part_b(q, row):
        return occ_c.at[c, q, pl.ds(depth // 2, depth // 2), row]

    def x_send(src, send, recv, i):
        q = quarter ^ (i + 1)
        return rdma(src, src, send, recv, 2 * ((q // 2) * depth + z) + c, lax.rem(q, 2) * side + y)

    def y_send(src, send, recv, i):
        return rdma(src, src, send, recv, mine, xl * side + lax.rem(y + 1 + i, side))

    def occ_x(i):
        return x_send(piece(quarter, y), ox_s.at[i], ox_r.at[quarter], i)

    def occ_y(i):
        return y_send(piece(quarter, y), oy_s.at[i], oy_r.at[y], i)

    def occ_xy(q, i):
        return y_send(part_a(q, y), fy_s.at[q, i], fy_r.at[q, y], i)

    def occ_yx(row, i):
        return x_send(part_b(quarter, row), fx_s.at[row, i], fx_r.at[quarter, row], i)

    each(3, lambda i: occ_x(i).start())
    each(side - 1, lambda i: occ_y(i).start())

    vir_t[c] = vir[c].T

    def t_copy(s, i):
        return rdma(t_mine.at[h, s], t_all.at[2 * j + s], t_s.at[s, i], t_r.at[s, j], 2 * deep(i) + c, b)

    def t_cross(s):
        return rdma(
            t_mine.at[1 - h, s], t_all.at[2 * j + s], t_s.at[s, depth - 1], t_r.at[s, j], 2 * partner + c, b
        )

    def t_forward(s, i):
        there = t_all.at[2 * partner + s]
        return rdma(there, there, f_s.at[s, i], t_r.at[s, partner], 2 * deep(i) + c, b)

    def t_landed(s, p):
        landed(t_all.at[2 * p + s], t_r.at[s, p])

    def t_make(s):
        value = jnp.dot(vir[s], trial_all[s], preferred_element_type=F32)
        t_mine[0, s] = value[:half].astype(BF)
        t_mine[1, s] = value[half:].astype(BF)
        t_all[2 * j + s] = t_mine[h, s]
        return occ[s].astype(F32) * value

    def t_start(s):
        t_cross(s).start()
        each(depth - 1, lambda i: t_copy(s, i).start())

    def tri_rest(s):
        for i in range(side - 1):
            tri_landed(s, beside(i))
            tri_landed(s, behind(i))

    tri_rest(c)
    local = t_make(c)
    t_start(c)
    rdma(vir.at[c], vir.at[o], x_s.at[0], x_r.at[0], other, b).wait_recv()
    rdma(occ.at[c], occ.at[o], x_s.at[1], x_r.at[1], other, b).wait_recv()
    tri_rest(o)
    tri_landed(o, b)
    local = local + t_make(o)

    high = local.astype(BF)
    low = (local - high.astype(F32)).astype(BF)
    ones = jnp.ones((8, nocc), BF)
    dens1[j] = lax.dot_general(ones, high, ALONG, preferred_element_type=F32) + lax.dot_general(
        ones, low, ALONG, preferred_element_type=F32
    )

    def d1_copy(i):
        return rdma(dens1.at[j], dens1.at[j], d1_s.at[i], d1_r.at[j], 2 * chip_peer(i) + c, b)

    each(chips - 1, lambda i: d1_copy(i).start())
    t_start(o)

    def x_arrived(i):
        q = quarter ^ (i + 1)
        landed(piece(q, y), ox_r.at[q])
        each(side - 1, lambda n: occ_xy(q, n).start())

    def y_arrived(i):
        row = lax.rem(y + 1 + i, side)
        landed(piece(quarter, row), oy_r.at[row])
        each(3, lambda n: occ_yx(row, n).start())

    each(3, x_arrived)
    each(side - 1, y_arrived)

    def t_pass(s):
        t_landed(s, partner)
        each(depth - 1, lambda i: t_forward(s, i).start())

    t_pass(c)
    t_pass(o)

    def occ3(n):
        q = quarter ^ (n // 2)
        there = occ_c.at[c, q, pl.ds(lax.rem(n, 2) * (depth // 2), depth // 2)]
        return rdma(there, there, o3_s.at[n], o3_r.at[n], other, b)

    occ3(0).start()
    occ3(1).start()

    vir_t[o] = vir[o].T
    turn[...] = jnp.zeros_like(turn)
    loads[7].wait()
    loads[8].wait()
    turn[:, 0:width] = jnp.broadcast_to(vir_e[...], (nocc, width))
    gaps = turn[...].T[0:width] - occ_e[...]
    for v in range(2):
        out[v] = gaps * trial[v]

    def occ_rest(i):
        q = quarter ^ (i + 1)

        def from_y(n):
            row = lax.rem(y + 1 + n, side)
            landed(part_a(q, row), fy_r.at[q, row])

        def from_x(n):
            row = lax.rem(y + 1 + n, side)
            landed(part_b(q, row), fx_r.at[q, row])

        each(side - 1, from_y)
        occ3(2 * i + 2).start()
        each(side - 1, from_x)
        occ3(2 * i + 3).start()

    each(3, occ_rest)

    def d1_wait(i):
        p = chip_peer(i)
        rdma(dens1.at[p], dens1.at[p], d1_s.at[i], d1_r.at[p], 2 * p + c, b).wait_recv()

    each(chips - 1, d1_wait)
    total = dens1[0]
    for p in range(1, chips):
        total = total + dens1[p]
    dens2[b] = total

    def d2_copy(i):
        return rdma(dens2.at[b], dens2.at[b], d2_s.at[i], d2_r.at[b], mine, band_peer(i))

    each(bands - 1, lambda i: d2_copy(i).start())

    def t_rest(i):
        near = deep(i)
        far = lax.rem(near + depth, chips)
        for s in range(2):
            t_landed(s, near)
            t_landed(s, far)

    each(depth - 1, t_rest)

    def points_of(p, s, e):
        return occ_c[s, 2 * (p // depth) + e, lax.rem(p, depth)].reshape(rows, nocc)

    def pairs_of(s):
        for p in range(chips):
            for e in range(2):
                pairs[2 * p + s, :, e * rows : (e + 1) * rows] = lax.dot_general(
                    t_all[2 * p + s], points_of(p, s, e), ALONG, preferred_element_type=F32
                ).astype(BF)

    pairs_of(c)

    def occ3_wait(n):
        q = quarter ^ (n // 2)
        landed(occ_c.at[o, q, pl.ds(lax.rem(n, 2) * (depth // 2), depth // 2)], o3_r.at[n])

    each(8, occ3_wait)

    pairs_of(o)
    loads[3].wait()
    loads[4].wait()
    loads[5].wait()

    tile = 16
    group = 2

    def u_copy(dest, s):
        return rdma(u_send.at[2 * dest + s], u_recv.at[j, s], u_s.at[s, dest], u_r.at[s, j], 2 * dest + c, b)

    def screen(g, s):
        dests = [j ^ (chips - 1 - group * g - n) for n in range(group)]

        def rows_step(r):
            part = block(r * tile, tile)
            for n, dest in enumerate(dests):
                acc = jnp.zeros((tile, cols), F32)
                for q in range(nk):
                    acc = acc + pairs[minus[2 * dest + s, q], part, :].astype(F32) * k_bf[q, part, :].astype(F32)
                s_bf[n, part, :] = acc.astype(BF)

        each(half // tile, rows_step)
        sums = []
        for n, dest in enumerate(dests):
            left = jnp.dot(s_bf[n, :, :rows], points_of(dest, s, 0), preferred_element_type=F32)
            sums.append(left + jnp.dot(s_bf[n, :, rows:], points_of(dest, s, 1), preferred_element_type=F32))
        for n, dest in enumerate(dests):
            if chips - 1 - group * g - n:
                u_send[2 * dest + s] = sums[n].astype(BF)
                u_copy(dest, s).start()
            else:
                u_recv[j, s] = sums[n].astype(BF)

    def finish(s):
        def u_landed(i):
            p = chip_peer(i)
            landed(u_recv.at[p, s], u_r.at[s, p])

        each(chips - 1, u_landed)
        sides = []
        for e in range(2):
            total = u_recv[e * depth, s].astype(F32)
            for p in range(1, depth):
                total = total + u_recv[e * depth + p, s].astype(F32)
            sides.append((acc_w[s, e * half : (e + 1) * half, :] - total).astype(BF))
        sig_send[s] = jnp.dot(vir_t[s], jnp.concatenate(sides, axis=0), preferred_element_type=F32).astype(BF)

        def sig_start(p):
            @pl.when((c != s) | (p != b))
            def _():
                sig_copy(s, p).start()

        each(bands, sig_start)

        @pl.when(c == s)
        def _():
            sig_recv[c, b] = sig_send[s, own_cols, :]

    def sig_copy(s, p):
        return rdma(
            sig_send.at[s, block(p * width, width)], sig_recv.at[c, b], g_s.at[s, p], g_r.at[c, b], 2 * j + s, p
        )

    for s in range(2):
        for g in range(chips // group):
            screen(g, s)

    def d2_wait(i):
        p = band_peer(i)
        rdma(dens2.at[p], dens2.at[p], d2_s.at[i], d2_r.at[p], mine, p).wait_recv()

    each(bands - 1, d2_wait)
    loads[6].wait()
    pot = jnp.zeros((rows, nocc), F32)
    for p in range(bands):
        line = jnp.broadcast_to(dens2[p][0:1, :].astype(BF), (nocc, rows))
        pot = pot + lax.dot_general(coul[:, p * rows : (p + 1) * rows], line, ALONG, preferred_element_type=F32)
    pot = pot * 2.0
    for s in range(2):
        acc_w[s] = pot * occ[s].astype(F32)

    finish(0)
    for w, n in tri_order:
        tri_out(w, n).wait_send()
    for s in range(2):
        for i in range(side - 1):
            tri_pass(s, i).wait_send()

    def occ1_sent(i):
        @pl.when((i != y) | (y != z))
        def _():
            occ1(i).wait_send()

    each(side, occ1_sent)
    send_vir.wait_send()
    send_occ.wait_send()
    each(3, lambda i: occ_x(i).wait_send())
    each(side - 1, lambda i: occ_y(i).wait_send())

    def forwarded(i):
        each(side - 1, lambda n: occ_xy(quarter ^ (i + 1), n).wait_send())
        each(3, lambda n: occ_yx(lax.rem(y + 1 + i, side), n).wait_send())

    each(3, forwarded)
    each(8, lambda n: occ3(n).wait_send())
    each(chips - 1, lambda i: d1_copy(i).wait_send())
    each(bands - 1, lambda i: d2_copy(i).wait_send())
    for s in range(2):
        each(depth - 1, lambda i: t_copy(s, i).wait_send())
        t_cross(s).wait_send()
        each(depth - 1, lambda i: t_forward(s, i).wait_send())

    finish(1)

    def sig_wait_same(i):
        p = band_peer(i)
        rdma(sig_send.at[0, own_cols], sig_recv.at[c, p], g_s.at[0, i], g_r.at[c, p], mine, p).wait_recv()

    def sig_wait_cross(i):
        rdma(sig_send.at[0, own_cols], sig_recv.at[o, i], g_s.at[1, i], g_r.at[o, i], other, i).wait_recv()

    each(bands - 1, sig_wait_same)
    each(bands, sig_wait_cross)
    for v in range(2):
        sums = sig_recv[v, 0].astype(F32)
        for p in range(1, bands):
            sums = sums + sig_recv[v, p].astype(F32)
        out[v] = out[v] + sums

    for s in range(2):
        each(chips - 1, lambda i: u_copy(chip_peer(i), s).wait_send())

        def sig_sent(p):
            @pl.when((c != s) | (p != b))
            def _():
                sig_copy(s, p).wait_send()

        each(bands, sig_sent)


def solution(mesh):
    bands = mesh.shape["band"]
    chips = mesh.shape["ka"] // 2

    def per_device(occ, vir, trial, occ_energy, vir_energy, coulomb, exch, minus):
        nk, rows, aux = exch.shape
        nocc = occ.shape[2]
        nvir = vir.shape[2]
        width = trial.shape[3]
        half = rows // 2
        cols = 2 * rows
        turned = jnp.transpose(trial[0], (0, 2, 1))
        far = pl.BlockSpec(memory_space=pltpu.HBM)
        dma = pltpu.SemaphoreType.DMA
        operands = (minus, turned, occ[0], vir[0], coulomb, exch, occ_energy, vir_energy)
        result = pl.pallas_call(
            kernel,
            out_shape=jax.ShapeDtypeStruct((2, width, nocc), F32),
            in_specs=[far] * 8,
            out_specs=pl.BlockSpec(memory_space=pltpu.VMEM),
            scratch_shapes=[
                pltpu.SMEM((nk, nk), jnp.int32),
                pltpu.VMEM((2, width, nocc), F32),
                pltpu.VMEM((2, rows, nocc), BF),
                pltpu.VMEM((2, rows, nvir), BF),
                pltpu.VMEM((1, nocc), F32),
                pltpu.VMEM((1, width), F32),
                pltpu.VMEM((nocc, 128), F32),
                pltpu.VMEM((2, width, nocc), BF),
                pltpu.VMEM((2, nvir, nocc), BF),
                pltpu.VMEM((2, nvir, rows), BF),
                pltpu.VMEM((2, 2, half, nocc), BF),
                pltpu.VMEM((nk, half, nocc), BF),
                pltpu.VMEM((2, 4, chips // 2, bands // 2, 2 * rows // bands, nocc), BF),
                pltpu.VMEM((nk, half, cols), BF),
                pltpu.VMEM((nk, half, cols), BF),
                pltpu.VMEM((2, half, cols), BF),
                pltpu.VMEM((nk, half, nocc), BF),
                pltpu.VMEM((chips, 2, half, nocc), BF),
                pltpu.VMEM((2, rows, nocc), F32),
                pltpu.VMEM((chips, 8, rows), F32),
                pltpu.VMEM((bands, 8, rows), F32),
                pltpu.VMEM((rows, aux), BF),
                pltpu.VMEM((2, nvir, nocc), BF),
                pltpu.VMEM((2, bands, width, nocc), BF),
                dma((2, 5)), dma((2, bands)), dma((2, 3)),
                dma((2,)), dma((2,)),
                dma((bands // 2,)), dma((chips // 2,)),
                dma((3,)), dma((4,)),
                dma((3,)), dma((bands // 2,)),
                dma((4, 3)), dma((4, bands // 2)),
                dma((bands // 2, 3)), dma((4, bands // 2)),
                dma((8,)), dma((8,)),
                dma((2, 4)), dma((2, 4)), dma((2, chips)),
                dma((chips,)), dma((chips,)),
                dma((bands,)), dma((bands,)),
                dma((2, chips)), dma((2, chips)),
                dma((2, bands)), dma((2, bands)),
                dma((9,)),
            ],
            compiler_params=pltpu.CompilerParams(
                collective_id=0, has_side_effects=True, vmem_limit_bytes=48 * 1024 * 1024
            ),
            name="sigma",
        )(*[pltpu.with_memory_space_constraint(a, pltpu.HBM) for a in operands])
        return jnp.transpose(result, (0, 2, 1))[None]

    in_specs = (
        P("ka", "band", None),
        P("ka", "band", None),
        P("ka", None, None, "band"),
        P("ka", None),
        P("ka", "band"),
        P("band", None),
        P(None, "band", None),
        P(),
    )
    return jax.shard_map(
        per_device,
        mesh=mesh,
        in_specs=in_specs,
        out_specs=P("ka", None, None, "band"),
        check_vma=False,
    )
```

```python
import jax
import jax.numpy as jnp
from jax import lax
from jax.experimental import pallas as pl
from jax.experimental.pallas import tpu as pltpu
from jax.sharding import PartitionSpec as P

BF = jnp.bfloat16
F32 = jnp.float32
MESH = pl.DeviceIdType.MESH
ALONG = (((1,), (1,)), ((), ()))


def each(count, body):
    def step(i, carry):
        body(i)
        return carry

    lax.fori_loop(0, count, step, 0)


def rdma(src, dst, send, recv, ka, band):
    return pltpu.make_async_remote_copy(
        src_ref=src,
        dst_ref=dst,
        send_sem=send,
        recv_sem=recv,
        device_id={"ka": ka, "band": band},
        device_id_type=MESH,
    )


def kernel(
    minus_h, trial_h, occ_h, vir_h, coulomb, exch, occ_e_h, vir_e_h, out,
    minus, trial, occ, vir, occ_e, vir_e, turn, trial_bf, trial_all, vir_t, t_mine, t_all, occ_c, k_bf, pairs, s_bf,
    u_send, u_recv, acc_w, dens1, dens2, coul, sig_send, sig_recv,
    tri_s, tri_r, tri_f, x_s, x_r, o1_s, o1_r, ox_s, ox_r, oy_s, oy_r, fy_s, fy_r, fx_s, fx_r, o3_s, o3_r, t_s, f_s, t_r, d1_s, d1_r, d2_s, d2_r,
    u_s, u_r, g_s, g_r, loc,
):
    bands = lax.axis_size("band")
    chips = lax.axis_size("ka") // 2
    depth = chips // 2
    ka = lax.axis_index("ka")
    b = lax.axis_index("band")
    j = ka // 2
    c = lax.rem(ka, 2)
    o = 1 - c
    h = j // depth
    z = lax.rem(j, depth)
    side = bands // 2
    xl = b // side
    y = lax.rem(b, side)
    quarter = 2 * h + xl
    mine = 2 * j + c
    other = 2 * j + o
    rows, nocc = occ_h.shape
    half = rows // 2
    width = trial.shape[1]
    nk = exch.shape[0]
    slab = rows // side
    cols = pairs.shape[2]
    home = xl * side + z
    goal = h * depth + y
    partner = (1 - h) * depth + z

    def band_peer(i):
        return lax.rem(b + 1 + i, bands)

    def chip_peer(i):
        return lax.rem(j + 1 + i, chips)

    def block(start, size, unit=16):
        return pl.ds(pl.multiple_of(start, unit), size)

    loads = [
        pltpu.make_async_copy(occ_h, occ.at[c], loc.at[0]),
        pltpu.make_async_copy(trial_h, trial, loc.at[1]),
        pltpu.make_async_copy(vir_h, vir.at[c], loc.at[2]),
        pltpu.make_async_copy(
            exch.at[:, block(h * half, half), block(z * rows, rows, 128)], k_bf.at[:, :, pl.ds(0, rows)], loc.at[3]
        ),
        pltpu.make_async_copy(
            exch.at[:, block(h * half, half), block((z + side) * rows, rows, 128)],
            k_bf.at[:, :, pl.ds(rows, rows)], loc.at[8],
        ),
        pltpu.make_async_copy(minus_h, minus, loc.at[4]),
        pltpu.make_async_copy(coulomb, coul, loc.at[5]),
        pltpu.make_async_copy(occ_e_h, occ_e, loc.at[6]),
        pltpu.make_async_copy(vir_e_h, vir_e, loc.at[7]),
    ]
    for load in loads:
        load.start()

    barrier = pltpu.get_barrier_semaphore()

    def greet(k, band):
        pl.semaphore_signal(barrier, inc=1, device_id={"ka": k, "band": band}, device_id_type=MESH)

    def greet_band(i):
        greet(mine, band_peer(i))
        greet(other, band_peer(i))

    def deep(i):
        return h * depth + lax.rem(z + 1 + i, depth)

    each(bands - 1, greet_band)
    each(chips - 1, lambda i: greet(2 * chip_peer(i) + c, b))
    each(depth - 1, lambda i: greet(2 * deep(i) + c, home))
    greet(other, b)
    greet(2 * ((1 - h) * depth + z) + c, (1 - xl) * side + y)

    loads[0].wait()
    loads[1].wait()
    trial_bf[...] = trial[...].astype(BF)
    callers = 2 * (bands - 1) + (chips - 1) + 2
    pl.semaphore_wait(barrier, jnp.where(y == z, callers, callers + side))

    def occ1(i):
        return rdma(
            occ.at[c, block(i * slab, slab)], occ_c.at[c, quarter, z, i], o1_s.at[i], o1_r.at[z],
            2 * goal + c, xl * side + i,
        )

    def occ1_start(i):
        @pl.when((i != y) | (y != z))
        def _():
            occ1(i).start()

    each(side, occ1_start)

    @pl.when(y == z)
    def _():
        occ_c[c, quarter, z, y] = occ[c, block(y * slab, slab), :]

    own_cols = block(b * width, width)

    facing = (1 - xl) * side + y

    def beside(i):
        return xl * side + lax.rem(y + 1 + i, side)

    def behind(i):
        return (1 - xl) * side + lax.rem(y + 1 + i, side)

    def tri_copy(w, n, p):
        vector, chip_core = ((c, mine), (o, other))[w]
        return rdma(trial_bf.at[vector], trial_all.at[c, own_cols], tri_s.at[w, n], tri_r.at[c, b], chip_core, p)

    def tri_out(w, n):
        return tri_copy(w, n, (facing, beside(0), beside(1), beside(2), b)[n])

    tri_order = [(0, 0), (1, 0), (0, 1), (0, 2), (0, 3), (1, 1), (1, 2), (1, 3), (1, 4)]
    for w, n in tri_order[:5]:
        tri_out(w, n).start()
    loads[2].wait()
    send_vir = rdma(vir.at[c], vir.at[c], x_s.at[0], x_r.at[0], other, b)
    send_occ = rdma(occ.at[c], occ.at[c], x_s.at[1], x_r.at[1], other, b)
    send_vir.start()
    send_occ.start()
    for w, n in tri_order[5:]:
        tri_out(w, n).start()
    trial_all[c, own_cols, :] = trial_bf[c]

    def landed(dst, recv):
        rdma(dst, dst, x_s.at[0], recv, mine, b).wait_recv()

    def tri_piece(s, p):
        return trial_all.at[s, block(p * width, width)]

    def tri_landed(s, p):
        landed(tri_piece(s, p), tri_r.at[s, p])

    def tri_pass(s, i):
        return rdma(
            tri_piece(s, facing), tri_piece(s, facing), tri_f.at[s, i], tri_r.at[s, facing], mine, beside(i)
        )

    for s in (c, o):
        tri_landed(s, facing)
        for i in range(side - 1):
            tri_pass(s, i).start()

    def occ1_wait(i):
        @pl.when((i != z) | (y != z))
        def _():
            rdma(
                occ.at[c, block(y * slab, slab)], occ_c.at[c, quarter, i, y], o1_s.at[0], o1_r.at[i], mine, b
            ).wait_recv()

    each(depth, occ1_wait)

    def piece(q, row):
        return occ_c.at[c, q, :, row]

    def part_a(q, row):
        return occ_c.at[c, q, pl.ds(0, depth // 2), row]

    def part_b(q, row):
        return occ_c.at[c, q, pl.ds(depth // 2, depth // 2), row]

    def x_send(src, send, recv, i):
        q = quarter ^ (i + 1)
        return rdma(src, src, send, recv, 2 * ((q // 2) * depth + z) + c, lax.rem(q, 2) * side + y)

    def y_send(src, send, recv, i):
        return rdma(src, src, send, recv, mine, xl * side + lax.rem(y + 1 + i, side))

    def occ_x(i):
        return x_send(piece(quarter, y), ox_s.at[i], ox_r.at[quarter], i)

    def occ_y(i):
        return y_send(piece(quarter, y), oy_s.at[i], oy_r.at[y], i)

    def occ_xy(q, i):
        return y_send(part_a(q, y), fy_s.at[q, i], fy_r.at[q, y], i)

    def occ_yx(row, i):
        return x_send(part_b(quarter, row), fx_s.at[row, i], fx_r.at[quarter, row], i)

    each(3, lambda i: occ_x(i).start())
    each(side - 1, lambda i: occ_y(i).start())

    vir_t[c] = vir[c].T

    def t_copy(s, i):
        return rdma(t_mine.at[h, s], t_all.at[2 * j + s], t_s.at[s, i], t_r.at[s, j], 2 * deep(i) + c, b)

    def t_cross(s):
        return rdma(
            t_mine.at[1 - h, s], t_all.at[2 * j + s], t_s.at[s, depth - 1], t_r.at[s, j], 2 * partner + c, b
        )

    def t_forward(s, i):
        there = t_all.at[2 * partner + s]
        return rdma(there, there, f_s.at[s, i], t_r.at[s, partner], 2 * deep(i) + c, b)

    def t_landed(s, p):
        landed(t_all.at[2 * p + s], t_r.at[s, p])

    def t_make(s):
        value = jnp.dot(vir[s], trial_all[s], preferred_element_type=F32)
        t_mine[0, s] = value[:half].astype(BF)
        t_mine[1, s] = value[half:].astype(BF)
        t_all[2 * j + s] = t_mine[h, s]
        return occ[s].astype(F32) * value

    def t_start(s):
        t_cross(s).start()
        each(depth - 1, lambda i: t_copy(s, i).start())

    def tri_rest(s):
        for i in range(side - 1):
            tri_landed(s, beside(i))
            tri_landed(s, behind(i))

    tri_rest(c)
    local = t_make(c)
    t_start(c)
    rdma(vir.at[c], vir.at[o], x_s.at[0], x_r.at[0], other, b).wait_recv()
    rdma(occ.at[c], occ.at[o], x_s.at[1], x_r.at[1], other, b).wait_recv()
    tri_rest(o)
    tri_landed(o, b)
    local = local + t_make(o)

    high = local.astype(BF)
    low = (local - high.astype(F32)).astype(BF)
    ones = jnp.ones((8, nocc), BF)
    dens1[j] = lax.dot_general(ones, high, ALONG, preferred_element_type=F32) + lax.dot_general(
        ones, low, ALONG, preferred_element_type=F32
    )

    def d1_copy(i):
        return rdma(dens1.at[j], dens1.at[j], d1_s.at[i], d1_r.at[j], 2 * chip_peer(i) + c, b)

    each(chips - 1, lambda i: d1_copy(i).start())
    t_start(o)

    def x_arrived(i):
        q = quarter ^ (i + 1)
        landed(piece(q, y), ox_r.at[q])
        each(side - 1, lambda n: occ_xy(q, n).start())

    def y_arrived(i):
        row = lax.rem(y + 1 + i, side)
        landed(piece(quarter, row), oy_r.at[row])
        each(3, lambda n: occ_yx(row, n).start())

    each(3, x_arrived)
    each(side - 1, y_arrived)

    def t_pass(s):
        t_landed(s, partner)
        each(depth - 1, lambda i: t_forward(s, i).start())

    t_pass(c)
    t_pass(o)

    def occ3(n):
        q = quarter ^ (n // 2)
        there = occ_c.at[c, q, pl.ds(lax.rem(n, 2) * (depth // 2), depth // 2)]
        return rdma(there, there, o3_s.at[n], o3_r.at[n], other, b)

    occ3(0).start()
    occ3(1).start()

    vir_t[o] = vir[o].T
    turn[...] = jnp.zeros_like(turn)
    loads[7].wait()
    loads[8].wait()
    turn[:, 0:width] = jnp.broadcast_to(vir_e[...], (nocc, width))
    gaps = turn[...].T[0:width] - occ_e[...]
    for v in range(2):
        out[v] = gaps * trial[v]

    def occ_rest(i):
        q = quarter ^ (i + 1)

        def from_y(n):
            row = lax.rem(y + 1 + n, side)
            landed(part_a(q, row), fy_r.at[q, row])

        def from_x(n):
            row = lax.rem(y + 1 + n, side)
            landed(part_b(q, row), fx_r.at[q, row])

        each(side - 1, from_y)
        occ3(2 * i + 2).start()
        each(side - 1, from_x)
        occ3(2 * i + 3).start()

    each(3, occ_rest)

    def d1_wait(i):
        p = chip_peer(i)
        rdma(dens1.at[p], dens1.at[p], d1_s.at[i], d1_r.at[p], 2 * p + c, b).wait_recv()

    each(chips - 1, d1_wait)
    total = dens1[0]
    for p in range(1, chips):
        total = total + dens1[p]
    dens2[b] = total

    def d2_copy(i):
        return rdma(dens2.at[b], dens2.at[b], d2_s.at[i], d2_r.at[b], mine, band_peer(i))

    each(bands - 1, lambda i: d2_copy(i).start())

    def t_rest(i):
        near = deep(i)
        far = lax.rem(near + depth, chips)
        for s in range(2):
            t_landed(s, near)
            t_landed(s, far)

    each(depth - 1, t_rest)

    def points_of(p, s, e):
        return occ_c[s, 2 * (p // depth) + e, lax.rem(p, depth)].reshape(rows, nocc)

    def pairs_of(s, column):
        for n in range(depth):
            p = column * depth + n
            for e in range(2):
                pairs[2 * p + s, :, e * rows : (e + 1) * rows] = lax.dot_general(
                    t_all[2 * p + s], points_of(p, s, e), ALONG, preferred_element_type=F32
                ).astype(BF)

    pairs_of(c, h)
    pairs_of(c, 1 - h)

    def occ3_wait(n):
        q = quarter ^ (n // 2)
        landed(occ_c.at[o, q, pl.ds(lax.rem(n, 2) * (depth // 2), depth // 2)], o3_r.at[n])

    each(4, occ3_wait)
    pairs_of(o, h)
    each(4, lambda n: occ3_wait(n + 4))

    pairs_of(o, 1 - h)
    loads[3].wait()
    loads[4].wait()
    loads[5].wait()

    tile = 16

    def u_copy(dest, s):
        return rdma(u_send.at[2 * dest + s], u_recv.at[j, s], u_s.at[s, dest], u_r.at[s, j], 2 * dest + c, b)

    def screen(offsets, s):
        dests = [j ^ m for m in offsets]

        def rows_step(r):
            part = block(r * tile, tile)
            for n, dest in enumerate(dests):
                acc = jnp.zeros((tile, cols), F32)
                for q in range(nk):
                    acc = acc + pairs[minus[2 * dest + s, q], part, :].astype(F32) * k_bf[q, part, :].astype(F32)
                s_bf[n, part, :] = acc.astype(BF)

        each(half // tile, rows_step)
        sums = []
        for n, dest in enumerate(dests):
            left = jnp.dot(s_bf[n, :, :rows], points_of(dest, s, 0), preferred_element_type=F32)
            sums.append(left + jnp.dot(s_bf[n, :, rows:], points_of(dest, s, 1), preferred_element_type=F32))
        for n, dest in enumerate(dests):
            if offsets[n]:
                u_send[2 * dest + s] = sums[n].astype(BF)
                u_copy(dest, s).start()
            else:
                u_recv[j, s] = sums[n].astype(BF)

    def finish(s):
        def u_landed(i):
            p = chip_peer(i)
            landed(u_recv.at[p, s], u_r.at[s, p])

        each(chips - 1, u_landed)
        sides = []
        for e in range(2):
            total = u_recv[e * depth, s].astype(F32)
            for p in range(1, depth):
                total = total + u_recv[e * depth + p, s].astype(F32)
            sides.append((acc_w[s, e * half : (e + 1) * half, :] - total).astype(BF))
        sig_send[s] = jnp.dot(vir_t[s], jnp.concatenate(sides, axis=0), preferred_element_type=F32).astype(BF)

        for n in range(bands - 1, 0, -1):
            sig_copy(s, b ^ n).start()

        @pl.when(c == s)
        def _():
            sig_recv[c, b] = sig_send[s, own_cols, :]

        @pl.when(c != s)
        def _():
            sig_copy(s, b).start()

    def sig_copy(s, p):
        return rdma(
            sig_send.at[s, block(p * width, width)], sig_recv.at[c, b], g_s.at[s, p], g_r.at[c, b], 2 * j + s, p
        )

    for s in range(2):
        for m in range(depth - 1, -1, -1):
            screen((depth + m, m), s)

    def d2_wait(i):
        p = band_peer(i)
        rdma(dens2.at[p], dens2.at[p], d2_s.at[i], d2_r.at[p], mine, p).wait_recv()

    each(bands - 1, d2_wait)
    loads[6].wait()
    pot = jnp.zeros((rows, nocc), F32)
    for p in range(bands):
        line = jnp.broadcast_to(dens2[p][0:1, :].astype(BF), (nocc, rows))
        pot = pot + lax.dot_general(coul[:, p * rows : (p + 1) * rows], line, ALONG, preferred_element_type=F32)
    pot = pot * 2.0
    for s in range(2):
        acc_w[s] = pot * occ[s].astype(F32)

    finish(0)
    for w, n in tri_order:
        tri_out(w, n).wait_send()
    for s in range(2):
        for i in range(side - 1):
            tri_pass(s, i).wait_send()

    def occ1_sent(i):
        @pl.when((i != y) | (y != z))
        def _():
            occ1(i).wait_send()

    each(side, occ1_sent)
    send_vir.wait_send()
    send_occ.wait_send()
    each(3, lambda i: occ_x(i).wait_send())
    each(side - 1, lambda i: occ_y(i).wait_send())

    def forwarded(i):
        each(side - 1, lambda n: occ_xy(quarter ^ (i + 1), n).wait_send())
        each(3, lambda n: occ_yx(lax.rem(y + 1 + i, side), n).wait_send())

    each(3, forwarded)
    each(8, lambda n: occ3(n).wait_send())
    each(chips - 1, lambda i: d1_copy(i).wait_send())
    each(bands - 1, lambda i: d2_copy(i).wait_send())
    for s in range(2):
        each(depth - 1, lambda i: t_copy(s, i).wait_send())
        t_cross(s).wait_send()
        each(depth - 1, lambda i: t_forward(s, i).wait_send())

    finish(1)

    def sig_wait_same(i):
        p = band_peer(i)
        rdma(sig_send.at[0, own_cols], sig_recv.at[c, p], g_s.at[0, i], g_r.at[c, p], mine, p).wait_recv()

    def sig_wait_cross(i):
        rdma(sig_send.at[0, own_cols], sig_recv.at[o, i], g_s.at[1, i], g_r.at[o, i], other, i).wait_recv()

    each(bands - 1, sig_wait_same)
    each(bands, sig_wait_cross)
    for v in range(2):
        sums = sig_recv[v, 0].astype(F32)
        for p in range(1, bands):
            sums = sums + sig_recv[v, p].astype(F32)
        out[v] = out[v] + sums

    for s in range(2):
        each(chips - 1, lambda i: u_copy(chip_peer(i), s).wait_send())

        def sig_sent(p):
            @pl.when((c != s) | (p != b))
            def _():
                sig_copy(s, p).wait_send()

        each(bands, sig_sent)


def solution(mesh):
    bands = mesh.shape["band"]
    chips = mesh.shape["ka"] // 2

    def per_device(occ, vir, trial, occ_energy, vir_energy, coulomb, exch, minus):
        nk, rows, aux = exch.shape
        nocc = occ.shape[2]
        nvir = vir.shape[2]
        width = trial.shape[3]
        half = rows // 2
        cols = 2 * rows
        turned = jnp.transpose(trial[0], (0, 2, 1))
        far = pl.BlockSpec(memory_space=pltpu.HBM)
        dma = pltpu.SemaphoreType.DMA
        operands = (minus, turned, occ[0], vir[0], coulomb, exch, occ_energy, vir_energy)
        result = pl.pallas_call(
            kernel,
            out_shape=jax.ShapeDtypeStruct((2, width, nocc), F32),
            in_specs=[far] * 8,
            out_specs=pl.BlockSpec(memory_space=pltpu.VMEM),
            scratch_shapes=[
                pltpu.SMEM((nk, nk), jnp.int32),
                pltpu.VMEM((2, width, nocc), F32),
                pltpu.VMEM((2, rows, nocc), BF),
                pltpu.VMEM((2, rows, nvir), BF),
                pltpu.VMEM((1, nocc), F32),
                pltpu.VMEM((1, width), F32),
                pltpu.VMEM((nocc, 128), F32),
                pltpu.VMEM((2, width, nocc), BF),
                pltpu.VMEM((2, nvir, nocc), BF),
                pltpu.VMEM((2, nvir, rows), BF),
                pltpu.VMEM((2, 2, half, nocc), BF),
                pltpu.VMEM((nk, half, nocc), BF),
                pltpu.VMEM((2, 4, chips // 2, bands // 2, 2 * rows // bands, nocc), BF),
                pltpu.VMEM((nk, half, cols), BF),
                pltpu.VMEM((nk, half, cols), BF),
                pltpu.VMEM((4, half, cols), BF),
                pltpu.VMEM((nk, half, nocc), BF),
                pltpu.VMEM((chips, 2, half, nocc), BF),
                pltpu.VMEM((2, rows, nocc), F32),
                pltpu.VMEM((chips, 8, rows), F32),
                pltpu.VMEM((bands, 8, rows), F32),
                pltpu.VMEM((rows, aux), BF),
                pltpu.VMEM((2, nvir, nocc), BF),
                pltpu.VMEM((2, bands, width, nocc), BF),
                dma((2, 5)), dma((2, bands)), dma((2, 3)),
                dma((2,)), dma((2,)),
                dma((bands // 2,)), dma((chips // 2,)),
                dma((3,)), dma((4,)),
                dma((3,)), dma((bands // 2,)),
                dma((4, 3)), dma((4, bands // 2)),
                dma((bands // 2, 3)), dma((4, bands // 2)),
                dma((8,)), dma((8,)),
                dma((2, 4)), dma((2, 4)), dma((2, chips)),
                dma((chips,)), dma((chips,)),
                dma((bands,)), dma((bands,)),
                dma((2, chips)), dma((2, chips)),
                dma((2, bands)), dma((2, bands)),
                dma((9,)),
            ],
            compiler_params=pltpu.CompilerParams(
                collective_id=0, has_side_effects=True, vmem_limit_bytes=48 * 1024 * 1024
            ),
            name="sigma",
        )(*[pltpu.with_memory_space_constraint(a, pltpu.HBM) for a in operands])
        return jnp.transpose(result, (0, 2, 1))[None]

    in_specs = (
        P("ka", "band", None),
        P("ka", "band", None),
        P("ka", None, None, "band"),
        P("ka", None),
        P("ka", "band"),
        P("band", None),
        P(None, "band", None),
        P(),
    )
    return jax.shard_map(
        per_device,
        mesh=mesh,
        in_specs=in_specs,
        out_specs=P("ka", None, None, "band"),
        check_vma=False,
    )
```

```python
import jax
import jax.numpy as jnp
from jax import lax
from jax.experimental import pallas as pl
from jax.experimental.pallas import tpu as pltpu
from jax.sharding import PartitionSpec as P

BF = jnp.bfloat16
F32 = jnp.float32
MESH = pl.DeviceIdType.MESH
ALONG = (((1,), (1,)), ((), ()))


def each(count, body):
    def step(i, carry):
        body(i)
        return carry

    lax.fori_loop(0, count, step, 0)


def rdma(src, dst, send, recv, ka, band):
    return pltpu.make_async_remote_copy(
        src_ref=src,
        dst_ref=dst,
        send_sem=send,
        recv_sem=recv,
        device_id={"ka": ka, "band": band},
        device_id_type=MESH,
    )


def kernel(
    minus_h, trial_h, occ_h, vir_h, coulomb, exch, occ_e_h, vir_e_h, out,
    minus, trial, occ, vir, occ_e, vir_e, turn, trial_bf, trial_all, vir_t, t_mine, t_all, occ_c, k_bf, pairs, s_bf,
    u_send, u_recv, acc_w, dens1, dens2, coul, sig_send, sig_recv,
    tri_s, tri_r, tri_f, x_s, x_r, o1_s, o1_r, ox_s, ox_r, oy_s, oy_r, fy_s, fy_r, fx_s, fx_r, o3_s, o3_r, t_s, f_s, t_r, d1_s, d1_r, d2_s, d2_r,
    u_s, u_r, g_s, g_r, loc,
):
    bands = lax.axis_size("band")
    chips = lax.axis_size("ka") // 2
    depth = chips // 2
    ka = lax.axis_index("ka")
    b = lax.axis_index("band")
    j = ka // 2
    c = lax.rem(ka, 2)
    o = 1 - c
    h = j // depth
    z = lax.rem(j, depth)
    side = bands // 2
    xl = b // side
    y = lax.rem(b, side)
    quarter = 2 * h + xl
    mine = 2 * j + c
    other = 2 * j + o
    rows, nocc = occ_h.shape
    half = rows // 2
    width = trial.shape[1]
    nk = exch.shape[0]
    slab = rows // side
    cols = pairs.shape[2]
    home = xl * side + z
    goal = h * depth + y
    partner = (1 - h) * depth + z

    def band_peer(i):
        return lax.rem(b + 1 + i, bands)

    def chip_peer(i):
        return lax.rem(j + 1 + i, chips)

    def block(start, size, unit=16):
        return pl.ds(pl.multiple_of(start, unit), size)

    loads = [
        pltpu.make_async_copy(occ_h, occ.at[c], loc.at[0]),
        pltpu.make_async_copy(trial_h, trial, loc.at[1]),
        pltpu.make_async_copy(vir_h, vir.at[c], loc.at[2]),
        pltpu.make_async_copy(
            exch.at[:, block(h * half, half), block(z * rows, rows, 128)], k_bf.at[:, :, pl.ds(0, rows)], loc.at[3]
        ),
        pltpu.make_async_copy(
            exch.at[:, block(h * half, half), block((z + side) * rows, rows, 128)],
            k_bf.at[:, :, pl.ds(rows, rows)], loc.at[8],
        ),
        pltpu.make_async_copy(minus_h, minus, loc.at[4]),
        pltpu.make_async_copy(coulomb, coul, loc.at[5]),
        pltpu.make_async_copy(occ_e_h, occ_e, loc.at[6]),
        pltpu.make_async_copy(vir_e_h, vir_e, loc.at[7]),
    ]
    for load in loads:
        load.start()

    barrier = pltpu.get_barrier_semaphore()

    def greet(k, band):
        pl.semaphore_signal(barrier, inc=1, device_id={"ka": k, "band": band}, device_id_type=MESH)

    def greet_band(i):
        greet(mine, band_peer(i))
        greet(other, band_peer(i))

    def deep(i):
        return h * depth + lax.rem(z + 1 + i, depth)

    each(bands - 1, greet_band)
    each(chips - 1, lambda i: greet(2 * chip_peer(i) + c, b))
    each(depth - 1, lambda i: greet(2 * deep(i) + c, home))
    greet(other, b)
    greet(2 * ((1 - h) * depth + z) + c, (1 - xl) * side + y)

    loads[0].wait()
    loads[1].wait()
    trial_bf[...] = trial[...].astype(BF)
    callers = 2 * (bands - 1) + (chips - 1) + 2
    pl.semaphore_wait(barrier, jnp.where(y == z, callers, callers + side))

    def occ1(i):
        return rdma(
            occ.at[c, block(i * slab, slab)], occ_c.at[c, quarter, z, i], o1_s.at[i], o1_r.at[z],
            2 * goal + c, xl * side + i,
        )

    def occ1_start(i):
        @pl.when((i != y) | (y != z))
        def _():
            occ1(i).start()

    each(side, occ1_start)

    @pl.when(y == z)
    def _():
        occ_c[c, quarter, z, y] = occ[c, block(y * slab, slab), :]

    own_cols = block(b * width, width)

    facing = (1 - xl) * side + y

    def beside(i):
        return xl * side + lax.rem(y + 1 + i, side)

    def behind(i):
        return (1 - xl) * side + lax.rem(y + 1 + i, side)

    def tri_copy(w, n, p):
        vector, chip_core = ((c, mine), (o, other))[w]
        return rdma(trial_bf.at[vector], trial_all.at[c, own_cols], tri_s.at[w, n], tri_r.at[c, b], chip_core, p)

    def tri_out(w, n):
        return tri_copy(w, n, (facing, beside(0), beside(1), beside(2), b)[n])

    tri_order = [(0, 0), (1, 0), (0, 1), (0, 2), (0, 3), (1, 1), (1, 2), (1, 3), (1, 4)]
    for w, n in tri_order[:5]:
        tri_out(w, n).start()
    loads[2].wait()
    send_vir = rdma(vir.at[c], vir.at[c], x_s.at[0], x_r.at[0], other, b)
    send_occ = rdma(occ.at[c], occ.at[c], x_s.at[1], x_r.at[1], other, b)
    send_vir.start()
    send_occ.start()
    for w, n in tri_order[5:]:
        tri_out(w, n).start()
    trial_all[c, own_cols, :] = trial_bf[c]

    def landed(dst, recv):
        rdma(dst, dst, x_s.at[0], recv, mine, b).wait_recv()

    def tri_piece(s, p):
        return trial_all.at[s, block(p * width, width)]

    def tri_landed(s, p):
        landed(tri_piece(s, p), tri_r.at[s, p])

    def tri_pass(s, i):
        return rdma(
            tri_piece(s, facing), tri_piece(s, facing), tri_f.at[s, i], tri_r.at[s, facing], mine, beside(i)
        )

    for s in (c, o):
        tri_landed(s, facing)
        for i in range(side - 1):
            tri_pass(s, i).start()

    def occ1_wait(i):
        @pl.when((i != z) | (y != z))
        def _():
            rdma(
                occ.at[c, block(y * slab, slab)], occ_c.at[c, quarter, i, y], o1_s.at[0], o1_r.at[i], mine, b
            ).wait_recv()

    each(depth, occ1_wait)

    def part_a(q, row):
        return occ_c.at[c, q, pl.ds(0, depth // 2), row]

    def part_b(q, row):
        return occ_c.at[c, q, pl.ds(depth // 2, depth // 2), row]

    def x_send(src, send, recv, i):
        q = quarter ^ (i + 1)
        return rdma(src, src, send, recv, 2 * ((q // 2) * depth + z) + c, lax.rem(q, 2) * side + y)

    def y_send(src, send, recv, i):
        return rdma(src, src, send, recv, mine, xl * side + lax.rem(y + 1 + i, side))

    parts = (part_a, part_b)

    def occ_x(n, i):
        return x_send(parts[n](quarter, y), ox_s.at[n, i], ox_r.at[n, quarter], i)

    def occ_y(n, i):
        return y_send(parts[n](quarter, y), oy_s.at[n, i], oy_r.at[n, y], i)

    def occ_xy(q, i):
        return y_send(part_a(q, y), fy_s.at[q, i], fy_r.at[q, y], i)

    def occ_yx(row, i):
        return x_send(part_b(quarter, row), fx_s.at[row, i], fx_r.at[quarter, row], i)

    for n in range(2):
        each(3, lambda i: occ_x(n, i).start())
        each(side - 1, lambda i: occ_y(1 - n, i).start())

    vir_t[c] = vir[c].T

    def t_copy(s, i):
        return rdma(t_mine.at[h, s], t_all.at[2 * j + s], t_s.at[s, i], t_r.at[s, j], 2 * deep(i) + c, b)

    def t_cross(s):
        return rdma(
            t_mine.at[1 - h, s], t_all.at[2 * j + s], t_s.at[s, depth - 1], t_r.at[s, j], 2 * partner + c, b
        )

    def t_forward(s, i):
        there = t_all.at[2 * partner + s]
        return rdma(there, there, f_s.at[s, i], t_r.at[s, partner], 2 * deep(i) + c, b)

    def t_landed(s, p):
        landed(t_all.at[2 * p + s], t_r.at[s, p])

    def t_make(s):
        value = jnp.dot(vir[s], trial_all[s], preferred_element_type=F32)
        t_mine[0, s] = value[:half].astype(BF)
        t_mine[1, s] = value[half:].astype(BF)
        t_all[2 * j + s] = t_mine[h, s]
        return occ[s].astype(F32) * value

    def t_start(s):
        t_cross(s).start()
        each(depth - 1, lambda i: t_copy(s, i).start())

    def tri_rest(s):
        for i in range(side - 1):
            tri_landed(s, beside(i))
            tri_landed(s, behind(i))

    tri_rest(c)
    local = t_make(c)
    t_start(c)
    rdma(vir.at[c], vir.at[o], x_s.at[0], x_r.at[0], other, b).wait_recv()
    rdma(occ.at[c], occ.at[o], x_s.at[1], x_r.at[1], other, b).wait_recv()
    tri_rest(o)
    tri_landed(o, b)
    local = local + t_make(o)

    high = local.astype(BF)
    low = (local - high.astype(F32)).astype(BF)
    ones = jnp.ones((8, nocc), BF)
    dens1[j] = lax.dot_general(ones, high, ALONG, preferred_element_type=F32) + lax.dot_general(
        ones, low, ALONG, preferred_element_type=F32
    )

    def d1_copy(i):
        return rdma(dens1.at[j], dens1.at[j], d1_s.at[i], d1_r.at[j], 2 * chip_peer(i) + c, b)

    each(chips - 1, lambda i: d1_copy(i).start())
    t_start(o)

    def x_arrived(i):
        q = quarter ^ (i + 1)
        landed(part_a(q, y), ox_r.at[0, q])
        each(side - 1, lambda n: occ_xy(q, n).start())

    def y_arrived(i):
        row = lax.rem(y + 1 + i, side)
        landed(part_b(quarter, row), oy_r.at[1, row])
        each(3, lambda n: occ_yx(row, n).start())

    each(3, x_arrived)
    each(side - 1, y_arrived)

    def second_halves(i):
        row = lax.rem(y + 1 + i, side)
        landed(part_a(quarter, row), oy_r.at[0, row])

    def t_pass(s):
        t_landed(s, partner)
        each(depth - 1, lambda i: t_forward(s, i).start())

    t_pass(c)
    t_pass(o)

    def occ3(n):
        q = quarter ^ (n // 2)
        there = occ_c.at[c, q, pl.ds(lax.rem(n, 2) * (depth // 2), depth // 2)]
        return rdma(there, there, o3_s.at[n], o3_r.at[n], other, b)

    each(side - 1, second_halves)
    occ3(0).start()
    occ3(1).start()

    vir_t[o] = vir[o].T
    turn[...] = jnp.zeros_like(turn)
    loads[7].wait()
    loads[8].wait()
    turn[:, 0:width] = jnp.broadcast_to(vir_e[...], (nocc, width))
    gaps = turn[...].T[0:width] - occ_e[...]
    for v in range(2):
        out[v] = gaps * trial[v]

    def occ_rest(i):
        q = quarter ^ (i + 1)

        def from_y(n):
            row = lax.rem(y + 1 + n, side)
            landed(part_a(q, row), fy_r.at[q, row])

        def from_x(n):
            row = lax.rem(y + 1 + n, side)
            landed(part_b(q, row), fx_r.at[q, row])

        each(side - 1, from_y)
        occ3(2 * i + 2).start()
        each(side - 1, from_x)
        landed(part_b(q, y), ox_r.at[1, q])
        occ3(2 * i + 3).start()

    each(3, occ_rest)

    def d1_wait(i):
        p = chip_peer(i)
        rdma(dens1.at[p], dens1.at[p], d1_s.at[i], d1_r.at[p], 2 * p + c, b).wait_recv()

    each(chips - 1, d1_wait)
    total = dens1[0]
    for p in range(1, chips):
        total = total + dens1[p]
    dens2[b] = total

    def d2_copy(i):
        return rdma(dens2.at[b], dens2.at[b], d2_s.at[i], d2_r.at[b], mine, band_peer(i))

    each(bands - 1, lambda i: d2_copy(i).start())

    def t_rest(i):
        near = deep(i)
        far = lax.rem(near + depth, chips)
        for s in range(2):
            t_landed(s, near)
            t_landed(s, far)

    each(depth - 1, t_rest)

    def points_of(p, s, e):
        return occ_c[s, 2 * (p // depth) + e, lax.rem(p, depth)].reshape(rows, nocc)

    def pairs_of(s, column):
        for n in range(depth):
            p = column * depth + n
            for e in range(2):
                pairs[2 * p + s, :, e * rows : (e + 1) * rows] = lax.dot_general(
                    t_all[2 * p + s], points_of(p, s, e), ALONG, preferred_element_type=F32
                ).astype(BF)

    pairs_of(c, h)
    pairs_of(c, 1 - h)

    def occ3_wait(n):
        q = quarter ^ (n // 2)
        landed(occ_c.at[o, q, pl.ds(lax.rem(n, 2) * (depth // 2), depth // 2)], o3_r.at[n])

    each(4, occ3_wait)
    pairs_of(o, h)
    each(4, lambda n: occ3_wait(n + 4))

    pairs_of(o, 1 - h)
    loads[3].wait()
    loads[4].wait()
    loads[5].wait()

    tile = 16

    def u_copy(dest, s):
        return rdma(u_send.at[2 * dest + s], u_recv.at[j, s], u_s.at[s, dest], u_r.at[s, j], 2 * dest + c, b)

    def screen(offsets, s):
        dests = [j ^ m for m in offsets]

        def rows_step(r):
            part = block(r * tile, tile)
            for n, dest in enumerate(dests):
                acc = jnp.zeros((tile, cols), F32)
                for q in range(nk):
                    acc = acc + pairs[minus[2 * dest + s, q], part, :].astype(F32) * k_bf[q, part, :].astype(F32)
                s_bf[n, part, :] = acc.astype(BF)

        each(half // tile, rows_step)
        sums = []
        for n, dest in enumerate(dests):
            left = jnp.dot(s_bf[n, :, :rows], points_of(dest, s, 0), preferred_element_type=F32)
            sums.append(left + jnp.dot(s_bf[n, :, rows:], points_of(dest, s, 1), preferred_element_type=F32))
        for n, dest in enumerate(dests):
            if offsets[n]:
                u_send[2 * dest + s] = sums[n].astype(BF)
                u_copy(dest, s).start()
            else:
                u_recv[j, s] = sums[n].astype(BF)

    def finish(s):
        def u_landed(i):
            p = chip_peer(i)
            landed(u_recv.at[p, s], u_r.at[s, p])

        each(chips - 1, u_landed)
        sides = []
        for e in range(2):
            total = u_recv[e * depth, s].astype(F32)
            for p in range(1, depth):
                total = total + u_recv[e * depth + p, s].astype(F32)
            sides.append((acc_w[s, e * half : (e + 1) * half, :] - total).astype(BF))
        sig_send[s] = jnp.dot(vir_t[s], jnp.concatenate(sides, axis=0), preferred_element_type=F32).astype(BF)

        for n in range(bands - 1, 0, -1):
            sig_copy(s, b ^ n).start()

        @pl.when(c == s)
        def _():
            sig_recv[c, b] = sig_send[s, own_cols, :]

        @pl.when(c != s)
        def _():
            sig_copy(s, b).start()

    def sig_copy(s, p):
        return rdma(
            sig_send.at[s, block(p * width, width)], sig_recv.at[c, b], g_s.at[s, p], g_r.at[c, b], 2 * j + s, p
        )

    for s in range(2):
        for m in range(depth - 1, -1, -1):
            screen((depth + m, m), s)

    def d2_wait(i):
        p = band_peer(i)
        rdma(dens2.at[p], dens2.at[p], d2_s.at[i], d2_r.at[p], mine, p).wait_recv()

    each(bands - 1, d2_wait)
    loads[6].wait()
    pot = jnp.zeros((rows, nocc), F32)
    for p in range(bands):
        line = jnp.broadcast_to(dens2[p][0:1, :].astype(BF), (nocc, rows))
        pot = pot + lax.dot_general(coul[:, p * rows : (p + 1) * rows], line, ALONG, preferred_element_type=F32)
    pot = pot * 2.0
    for s in range(2):
        acc_w[s] = pot * occ[s].astype(F32)

    finish(0)
    for w, n in tri_order:
        tri_out(w, n).wait_send()
    for s in range(2):
        for i in range(side - 1):
            tri_pass(s, i).wait_send()

    def occ1_sent(i):
        @pl.when((i != y) | (y != z))
        def _():
            occ1(i).wait_send()

    each(side, occ1_sent)
    send_vir.wait_send()
    send_occ.wait_send()
    for n in range(2):
        each(3, lambda i: occ_x(n, i).wait_send())
        each(side - 1, lambda i: occ_y(n, i).wait_send())

    def forwarded(i):
        each(side - 1, lambda n: occ_xy(quarter ^ (i + 1), n).wait_send())
        each(3, lambda n: occ_yx(lax.rem(y + 1 + i, side), n).wait_send())

    each(3, forwarded)
    each(8, lambda n: occ3(n).wait_send())
    each(chips - 1, lambda i: d1_copy(i).wait_send())
    each(bands - 1, lambda i: d2_copy(i).wait_send())
    for s in range(2):
        each(depth - 1, lambda i: t_copy(s, i).wait_send())
        t_cross(s).wait_send()
        each(depth - 1, lambda i: t_forward(s, i).wait_send())

    finish(1)

    def sig_sent(s):
        for n in range(1, bands):
            sig_copy(s, b ^ n).wait_send()

        @pl.when(c != s)
        def _():
            sig_copy(s, b).wait_send()

    for s in range(2):
        each(chips - 1, lambda i: u_copy(chip_peer(i), s).wait_send())
    sig_sent(0)

    def sig_wait_same(i):
        p = band_peer(i)
        rdma(sig_send.at[0, own_cols], sig_recv.at[c, p], g_s.at[0, i], g_r.at[c, p], mine, p).wait_recv()

    def sig_wait_cross(i):
        rdma(sig_send.at[0, own_cols], sig_recv.at[o, i], g_s.at[1, i], g_r.at[o, i], other, i).wait_recv()

    each(bands - 1, sig_wait_same)
    each(bands, sig_wait_cross)
    for v in range(2):
        sums = sig_recv[v, 0].astype(F32)
        for p in range(1, bands):
            sums = sums + sig_recv[v, p].astype(F32)
        out[v] = out[v] + sums

    sig_sent(1)


def solution(mesh):
    bands = mesh.shape["band"]
    chips = mesh.shape["ka"] // 2

    def per_device(occ, vir, trial, occ_energy, vir_energy, coulomb, exch, minus):
        nk, rows, aux = exch.shape
        nocc = occ.shape[2]
        nvir = vir.shape[2]
        width = trial.shape[3]
        half = rows // 2
        cols = 2 * rows
        turned = jnp.transpose(trial[0], (0, 2, 1))
        far = pl.BlockSpec(memory_space=pltpu.HBM)
        dma = pltpu.SemaphoreType.DMA
        operands = (minus, turned, occ[0], vir[0], coulomb, exch, occ_energy, vir_energy)
        result = pl.pallas_call(
            kernel,
            out_shape=jax.ShapeDtypeStruct((2, width, nocc), F32),
            in_specs=[far] * 8,
            out_specs=pl.BlockSpec(memory_space=pltpu.VMEM),
            scratch_shapes=[
                pltpu.SMEM((nk, nk), jnp.int32),
                pltpu.VMEM((2, width, nocc), F32),
                pltpu.VMEM((2, rows, nocc), BF),
                pltpu.VMEM((2, rows, nvir), BF),
                pltpu.VMEM((1, nocc), F32),
                pltpu.VMEM((1, width), F32),
                pltpu.VMEM((nocc, 128), F32),
                pltpu.VMEM((2, width, nocc), BF),
                pltpu.VMEM((2, nvir, nocc), BF),
                pltpu.VMEM((2, nvir, rows), BF),
                pltpu.VMEM((2, 2, half, nocc), BF),
                pltpu.VMEM((nk, half, nocc), BF),
                pltpu.VMEM((2, 4, chips // 2, bands // 2, 2 * rows // bands, nocc), BF),
                pltpu.VMEM((nk, half, cols), BF),
                pltpu.VMEM((nk, half, cols), BF),
                pltpu.VMEM((4, half, cols), BF),
                pltpu.VMEM((nk, half, nocc), BF),
                pltpu.VMEM((chips, 2, half, nocc), BF),
                pltpu.VMEM((2, rows, nocc), F32),
                pltpu.VMEM((chips, 8, rows), F32),
                pltpu.VMEM((bands, 8, rows), F32),
                pltpu.VMEM((rows, aux), BF),
                pltpu.VMEM((2, nvir, nocc), BF),
                pltpu.VMEM((2, bands, width, nocc), BF),
                dma((2, 5)), dma((2, bands)), dma((2, 3)),
                dma((2,)), dma((2,)),
                dma((bands // 2,)), dma((chips // 2,)),
                dma((2, 3)), dma((2, 4)),
                dma((2, 3)), dma((2, bands // 2)),
                dma((4, 3)), dma((4, bands // 2)),
                dma((bands // 2, 3)), dma((4, bands // 2)),
                dma((8,)), dma((8,)),
                dma((2, 4)), dma((2, 4)), dma((2, chips)),
                dma((chips,)), dma((chips,)),
                dma((bands,)), dma((bands,)),
                dma((2, chips)), dma((2, chips)),
                dma((2, bands)), dma((2, bands)),
                dma((9,)),
            ],
            compiler_params=pltpu.CompilerParams(
                collective_id=0, has_side_effects=True, vmem_limit_bytes=48 * 1024 * 1024
            ),
            name="sigma",
        )(*[pltpu.with_memory_space_constraint(a, pltpu.HBM) for a in operands])
        return jnp.transpose(result, (0, 2, 1))[None]

    in_specs = (
        P("ka", "band", None),
        P("ka", "band", None),
        P("ka", None, None, "band"),
        P("ka", None),
        P("ka", "band"),
        P("band", None),
        P(None, "band", None),
        P(),
    )
    return jax.shard_map(
        per_device,
        mesh=mesh,
        in_specs=in_specs,
        out_specs=P("ka", None, None, "band"),
        check_vma=False,
    )
```

```python
import jax
import jax.numpy as jnp
from jax import lax
from jax.experimental import pallas as pl
from jax.experimental.pallas import tpu as pltpu
from jax.sharding import PartitionSpec as P

BF = jnp.bfloat16
F32 = jnp.float32
MESH = pl.DeviceIdType.MESH
ALONG = (((1,), (1,)), ((), ()))


def each(count, body):
    def step(i, carry):
        body(i)
        return carry

    lax.fori_loop(0, count, step, 0)


def rdma(src, dst, send, recv, ka, band):
    return pltpu.make_async_remote_copy(
        src_ref=src,
        dst_ref=dst,
        send_sem=send,
        recv_sem=recv,
        device_id={"ka": ka, "band": band},
        device_id_type=MESH,
    )


def kernel(
    minus_h, trial_h, occ_h, vir_h, coulomb, exch, occ_e_h, vir_e_h, out,
    minus, trial, occ, vir, occ_e, vir_e, turn, trial_bf, trial_all, vir_t, t_mine, t_all, occ_c, k_bf, pairs, s_bf,
    u_send, u_recv, acc_w, dens1, dens2, coul, sig_send, sig_recv,
    tri_s, tri_r, tri_f, x_s, x_r, o1_s, o1_r, ox_s, ox_r, oy_s, oy_r, fy_s, fy_r, fx_s, fx_r, o3_s, o3_r, t_s, f_s, t_r, d1_s, d1_r, d2_s, d2_r,
    u_s, u_r, g_s, g_r, loc,
):
    bands = lax.axis_size("band")
    chips = lax.axis_size("ka") // 2
    depth = chips // 2
    ka = lax.axis_index("ka")
    b = lax.axis_index("band")
    j = ka // 2
    c = lax.rem(ka, 2)
    o = 1 - c
    h = j // depth
    z = lax.rem(j, depth)
    side = bands // 2
    xl = b // side
    y = lax.rem(b, side)
    quarter = 2 * h + xl
    mine = 2 * j + c
    other = 2 * j + o
    rows, nocc = occ_h.shape
    half = rows // 2
    width = trial.shape[1]
    nk = exch.shape[0]
    slab = rows // side
    cols = pairs.shape[2]
    home = xl * side + z
    goal = h * depth + y
    partner = (1 - h) * depth + z

    def band_peer(i):
        return lax.rem(b + 1 + i, bands)

    def chip_peer(i):
        return lax.rem(j + 1 + i, chips)

    def block(start, size, unit=16):
        return pl.ds(pl.multiple_of(start, unit), size)

    loads = [
        pltpu.make_async_copy(occ_h, occ.at[c], loc.at[0]),
        pltpu.make_async_copy(trial_h, trial, loc.at[1]),
        pltpu.make_async_copy(vir_h, vir.at[c], loc.at[2]),
        pltpu.make_async_copy(
            exch.at[:, block(h * half, half), block(z * rows, rows, 128)], k_bf.at[:, :, pl.ds(0, rows)], loc.at[3]
        ),
        pltpu.make_async_copy(
            exch.at[:, block(h * half, half), block((z + side) * rows, rows, 128)],
            k_bf.at[:, :, pl.ds(rows, rows)], loc.at[8],
        ),
        pltpu.make_async_copy(minus_h, minus, loc.at[4]),
        pltpu.make_async_copy(coulomb, coul, loc.at[5]),
        pltpu.make_async_copy(occ_e_h, occ_e, loc.at[6]),
        pltpu.make_async_copy(vir_e_h, vir_e, loc.at[7]),
    ]
    for load in loads:
        load.start()

    barrier = pltpu.get_barrier_semaphore()

    def greet(k, band):
        pl.semaphore_signal(barrier, inc=1, device_id={"ka": k, "band": band}, device_id_type=MESH)

    def greet_band(i):
        greet(mine, band_peer(i))
        greet(other, band_peer(i))

    def deep(i):
        return h * depth + lax.rem(z + 1 + i, depth)

    each(bands - 1, greet_band)
    each(chips - 1, lambda i: greet(2 * chip_peer(i) + c, b))
    each(depth - 1, lambda i: greet(2 * deep(i) + c, home))
    greet(other, b)
    greet(2 * ((1 - h) * depth + z) + c, (1 - xl) * side + y)

    loads[0].wait()
    loads[1].wait()
    trial_bf[...] = trial[...].astype(BF)
    callers = 2 * (bands - 1) + (chips - 1) + 2
    pl.semaphore_wait(barrier, jnp.where(y == z, callers, callers + side))

    def occ1(i):
        return rdma(
            occ.at[c, block(i * slab, slab)], occ_c.at[c, quarter, z, i], o1_s.at[i], o1_r.at[z],
            2 * goal + c, xl * side + i,
        )

    def occ1_start(i):
        @pl.when((i != y) | (y != z))
        def _():
            occ1(i).start()

    each(side, occ1_start)

    @pl.when(y == z)
    def _():
        occ_c[c, quarter, z, y] = occ[c, block(y * slab, slab), :]

    own_cols = block(b * width, width)

    facing = (1 - xl) * side + y

    def beside(i):
        return xl * side + lax.rem(y + 1 + i, side)

    def behind(i):
        return (1 - xl) * side + lax.rem(y + 1 + i, side)

    def tri_copy(w, n, p):
        vector, chip_core = ((c, mine), (o, other))[w]
        return rdma(trial_bf.at[vector], trial_all.at[c, own_cols], tri_s.at[w, n], tri_r.at[c, b], chip_core, p)

    def tri_out(w, n):
        return tri_copy(w, n, (facing, beside(0), beside(1), beside(2), b)[n])

    tri_order = [(0, 0), (1, 0), (0, 1), (0, 2), (0, 3), (1, 1), (1, 2), (1, 3), (1, 4)]
    for w, n in tri_order[:5]:
        tri_out(w, n).start()
    loads[2].wait()
    send_vir = rdma(vir.at[c], vir.at[c], x_s.at[0], x_r.at[0], other, b)
    send_occ = rdma(occ.at[c], occ.at[c], x_s.at[1], x_r.at[1], other, b)
    send_vir.start()
    send_occ.start()
    for w, n in tri_order[5:]:
        tri_out(w, n).start()
    trial_all[c, own_cols, :] = trial_bf[c]

    def landed(dst, recv):
        rdma(dst, dst, x_s.at[0], recv, mine, b).wait_recv()

    def tri_piece(s, p):
        return trial_all.at[s, block(p * width, width)]

    def tri_landed(s, p):
        landed(tri_piece(s, p), tri_r.at[s, p])

    def tri_pass(s, i):
        return rdma(
            tri_piece(s, facing), tri_piece(s, facing), tri_f.at[s, i], tri_r.at[s, facing], mine, beside(i)
        )

    for s in (c, o):
        tri_landed(s, facing)
        for i in range(side - 1):
            tri_pass(s, i).start()

    def occ1_wait(i):
        @pl.when((i != z) | (y != z))
        def _():
            rdma(
                occ.at[c, block(y * slab, slab)], occ_c.at[c, quarter, i, y], o1_s.at[0], o1_r.at[i], mine, b
            ).wait_recv()

    each(depth, occ1_wait)

    def part_a(q, row):
        return occ_c.at[c, q, pl.ds(0, depth // 2), row]

    def part_b(q, row):
        return occ_c.at[c, q, pl.ds(depth // 2, depth // 2), row]

    def x_send(src, send, recv, i):
        q = quarter ^ (i + 1)
        return rdma(src, src, send, recv, 2 * ((q // 2) * depth + z) + c, lax.rem(q, 2) * side + y)

    def y_send(src, send, recv, i):
        return rdma(src, src, send, recv, mine, xl * side + lax.rem(y + 1 + i, side))

    parts = (part_a, part_b)

    def occ_x(n, i):
        return x_send(parts[n](quarter, y), ox_s.at[n, i], ox_r.at[n, quarter], i)

    def occ_y(n, i):
        return y_send(parts[n](quarter, y), oy_s.at[n, i], oy_r.at[n, y], i)

    def occ_xy(q, i):
        return y_send(part_a(q, y), fy_s.at[q, i], fy_r.at[q, y], i)

    def occ_yx(row, i):
        return x_send(part_b(quarter, row), fx_s.at[row, i], fx_r.at[quarter, row], i)

    for n in range(2):
        each(3, lambda i: occ_x(n, i).start())
        each(side - 1, lambda i: occ_y(1 - n, i).start())

    vir_t[c] = vir[c].T

    def t_copy(s, i):
        return rdma(t_mine.at[h, s], t_all.at[2 * j + s], t_s.at[s, i], t_r.at[s, j], 2 * deep(i) + c, b)

    def t_cross(s):
        return rdma(
            t_mine.at[1 - h, s], t_all.at[2 * j + s], t_s.at[s, depth - 1], t_r.at[s, j], 2 * partner + c, b
        )

    def t_forward(s, i):
        there = t_all.at[2 * partner + s]
        return rdma(there, there, f_s.at[s, i], t_r.at[s, partner], 2 * deep(i) + c, b)

    def t_landed(s, p):
        landed(t_all.at[2 * p + s], t_r.at[s, p])

    def t_make(s):
        value = jnp.dot(vir[s], trial_all[s], preferred_element_type=F32)
        t_mine[0, s] = value[:half].astype(BF)
        t_mine[1, s] = value[half:].astype(BF)
        t_all[2 * j + s] = t_mine[h, s]
        return occ[s].astype(F32) * value

    def t_start(s):
        t_cross(s).start()
        each(depth - 1, lambda i: t_copy(s, i).start())

    def tri_rest(s):
        for i in range(side - 1):
            tri_landed(s, beside(i))
            tri_landed(s, behind(i))

    tri_rest(c)
    local = t_make(c)
    t_start(c)
    rdma(vir.at[c], vir.at[o], x_s.at[0], x_r.at[0], other, b).wait_recv()
    rdma(occ.at[c], occ.at[o], x_s.at[1], x_r.at[1], other, b).wait_recv()
    tri_rest(o)
    tri_landed(o, b)
    local = local + t_make(o)

    high = local.astype(BF)
    low = (local - high.astype(F32)).astype(BF)
    ones = jnp.ones((8, nocc), BF)
    dens1[j] = lax.dot_general(ones, high, ALONG, preferred_element_type=F32) + lax.dot_general(
        ones, low, ALONG, preferred_element_type=F32
    )

    def d1_copy(i):
        return rdma(dens1.at[j], dens1.at[j], d1_s.at[i], d1_r.at[j], 2 * chip_peer(i) + c, b)

    each(chips - 1, lambda i: d1_copy(i).start())
    t_start(o)

    def x_arrived(i):
        q = quarter ^ (i + 1)
        landed(part_a(q, y), ox_r.at[0, q])
        each(side - 1, lambda n: occ_xy(q, n).start())

    def y_arrived(i):
        row = lax.rem(y + 1 + i, side)
        landed(part_b(quarter, row), oy_r.at[1, row])
        each(3, lambda n: occ_yx(row, n).start())

    each(3, x_arrived)
    each(side - 1, y_arrived)

    def second_halves(i):
        row = lax.rem(y + 1 + i, side)
        landed(part_a(quarter, row), oy_r.at[0, row])

    def t_pass(s):
        t_landed(s, partner)
        each(depth - 1, lambda i: t_forward(s, i).start())

    t_pass(c)
    t_pass(o)

    def occ3(n):
        q = quarter ^ (n // 2)
        there = occ_c.at[c, q, pl.ds(lax.rem(n, 2) * (depth // 2), depth // 2)]
        return rdma(there, there, o3_s.at[n], o3_r.at[n], other, b)

    each(side - 1, second_halves)
    occ3(0).start()
    occ3(1).start()

    vir_t[o] = vir[o].T
    turn[...] = jnp.zeros_like(turn)
    loads[7].wait()
    loads[8].wait()
    turn[:, 0:width] = jnp.broadcast_to(vir_e[...], (nocc, width))
    gaps = turn[...].T[0:width] - occ_e[...]
    for v in range(2):
        out[v] = gaps * trial[v]

    def occ_rest(i):
        q = quarter ^ (i + 1)

        def from_y(n):
            row = lax.rem(y + 1 + n, side)
            landed(part_a(q, row), fy_r.at[q, row])

        def from_x(n):
            row = lax.rem(y + 1 + n, side)
            landed(part_b(q, row), fx_r.at[q, row])

        each(side - 1, from_y)
        occ3(2 * i + 2).start()
        each(side - 1, from_x)
        landed(part_b(q, y), ox_r.at[1, q])
        occ3(2 * i + 3).start()

    each(3, occ_rest)

    def d1_wait(i):
        p = chip_peer(i)
        rdma(dens1.at[p], dens1.at[p], d1_s.at[i], d1_r.at[p], 2 * p + c, b).wait_recv()

    each(chips - 1, d1_wait)
    total = dens1[0]
    for p in range(1, chips):
        total = total + dens1[p]
    dens2[b] = total

    def d2_copy(i):
        return rdma(dens2.at[b], dens2.at[b], d2_s.at[i], d2_r.at[b], mine, band_peer(i))

    each(bands - 1, lambda i: d2_copy(i).start())

    def t_rest(i):
        near = deep(i)
        far = lax.rem(near + depth, chips)
        for s in range(2):
            t_landed(s, near)
            t_landed(s, far)

    each(depth - 1, t_rest)

    def points_of(p, s, e):
        return occ_c[s, 2 * (p // depth) + e, lax.rem(p, depth)].reshape(rows, nocc)

    def pairs_of(s, column):
        for n in range(depth):
            p = column * depth + n
            for e in range(2):
                pairs[2 * p + s, :, e * rows : (e + 1) * rows] = lax.dot_general(
                    t_all[2 * p + s], points_of(p, s, e), ALONG, preferred_element_type=F32
                ).astype(BF)

    pairs_of(c, h)
    pairs_of(c, 1 - h)

    def occ3_wait(n):
        q = quarter ^ (n // 2)
        landed(occ_c.at[o, q, pl.ds(lax.rem(n, 2) * (depth // 2), depth // 2)], o3_r.at[n])

    each(4, occ3_wait)
    pairs_of(o, h)
    each(4, lambda n: occ3_wait(n + 4))

    pairs_of(o, 1 - h)
    loads[3].wait()
    loads[4].wait()
    loads[5].wait()

    tile = 16

    def u_copy(dest, s):
        return rdma(u_send.at[2 * dest + s], u_recv.at[j, s], u_s.at[s, dest], u_r.at[s, j], 2 * dest + c, b)

    def screen(offsets, s):
        dests = [j ^ m for m in offsets]

        def rows_step(r):
            for t in range(2):
                part = block((r * 2 + t) * tile, tile)
                for n, dest in enumerate(dests):
                    acc = jnp.zeros((tile, cols), F32)
                    for q in range(nk):
                        source = minus[2 * dest + s, q]
                        acc = acc + pairs[source, part, :].astype(F32) * k_bf[q, part, :].astype(F32)
                    s_bf[n, part, :] = acc.astype(BF)

        each(half // tile // 2, rows_step)
        sums = []
        for n, dest in enumerate(dests):
            left = jnp.dot(s_bf[n, :, :rows], points_of(dest, s, 0), preferred_element_type=F32)
            sums.append(left + jnp.dot(s_bf[n, :, rows:], points_of(dest, s, 1), preferred_element_type=F32))
        for n, dest in enumerate(dests):
            if offsets[n]:
                u_send[2 * dest + s] = sums[n].astype(BF)
                u_copy(dest, s).start()
            else:
                u_recv[j, s] = sums[n].astype(BF)

    def finish(s):
        def u_landed(i):
            p = chip_peer(i)
            landed(u_recv.at[p, s], u_r.at[s, p])

        each(chips - 1, u_landed)
        sides = []
        for e in range(2):
            total = u_recv[e * depth, s].astype(F32)
            for p in range(1, depth):
                total = total + u_recv[e * depth + p, s].astype(F32)
            sides.append((acc_w[s, e * half : (e + 1) * half, :] - total).astype(BF))
        weight = jnp.concatenate(sides, axis=0)
        for column in (1 - xl, xl):
            part = block(column * side * width, side * width)
            sig_send[s, part, :] = jnp.dot(vir_t[s, part, :], weight, preferred_element_type=F32).astype(BF)
            for n in range(side - 1, -1, -1):
                if column is xl and n == 0:
                    continue
                sig_copy(s, column * side + (y ^ n)).start()

        @pl.when(c == s)
        def _():
            sig_recv[c, b] = sig_send[s, own_cols, :]

        @pl.when(c != s)
        def _():
            sig_copy(s, b).start()

    def sig_copy(s, p):
        return rdma(
            sig_send.at[s, block(p * width, width)], sig_recv.at[c, b], g_s.at[s, p], g_r.at[c, b], 2 * j + s, p
        )

    for s in range(2):
        for m in range(depth - 1, -1, -1):
            screen((depth + m, m), s)

    def d2_wait(i):
        p = band_peer(i)
        rdma(dens2.at[p], dens2.at[p], d2_s.at[i], d2_r.at[p], mine, p).wait_recv()

    each(bands - 1, d2_wait)
    loads[6].wait()
    pot = jnp.zeros((rows, nocc), F32)
    for p in range(bands):
        line = jnp.broadcast_to(dens2[p][0:1, :].astype(BF), (nocc, rows))
        pot = pot + lax.dot_general(coul[:, p * rows : (p + 1) * rows], line, ALONG, preferred_element_type=F32)
    pot = pot * 2.0
    for s in range(2):
        acc_w[s] = pot * occ[s].astype(F32)

    finish(0)
    for w, n in tri_order:
        tri_out(w, n).wait_send()
    for s in range(2):
        for i in range(side - 1):
            tri_pass(s, i).wait_send()

    def occ1_sent(i):
        @pl.when((i != y) | (y != z))
        def _():
            occ1(i).wait_send()

    each(side, occ1_sent)
    send_vir.wait_send()
    send_occ.wait_send()
    for n in range(2):
        each(3, lambda i: occ_x(n, i).wait_send())
        each(side - 1, lambda i: occ_y(n, i).wait_send())

    def forwarded(i):
        each(side - 1, lambda n: occ_xy(quarter ^ (i + 1), n).wait_send())
        each(3, lambda n: occ_yx(lax.rem(y + 1 + i, side), n).wait_send())

    each(3, forwarded)
    each(8, lambda n: occ3(n).wait_send())
    each(chips - 1, lambda i: d1_copy(i).wait_send())
    each(bands - 1, lambda i: d2_copy(i).wait_send())
    for s in range(2):
        each(depth - 1, lambda i: t_copy(s, i).wait_send())
        t_cross(s).wait_send()
        each(depth - 1, lambda i: t_forward(s, i).wait_send())

    finish(1)

    def sig_sent(s):
        for n in range(1, bands):
            sig_copy(s, b ^ n).wait_send()

        @pl.when(c != s)
        def _():
            sig_copy(s, b).wait_send()

    for s in range(2):
        each(chips - 1, lambda i: u_copy(chip_peer(i), s).wait_send())
    sig_sent(0)

    def sig_wait_same(i):
        p = band_peer(i)
        rdma(sig_send.at[0, own_cols], sig_recv.at[c, p], g_s.at[0, i], g_r.at[c, p], mine, p).wait_recv()

    def sig_wait_cross(i):
        rdma(sig_send.at[0, own_cols], sig_recv.at[o, i], g_s.at[1, i], g_r.at[o, i], other, i).wait_recv()

    each(bands - 1, sig_wait_same)
    each(bands, sig_wait_cross)
    for v in range(2):
        sums = sig_recv[v, 0].astype(F32)
        for p in range(1, bands):
            sums = sums + sig_recv[v, p].astype(F32)
        out[v] = out[v] + sums

    sig_sent(1)


def solution(mesh):
    bands = mesh.shape["band"]
    chips = mesh.shape["ka"] // 2

    def per_device(occ, vir, trial, occ_energy, vir_energy, coulomb, exch, minus):
        nk, rows, aux = exch.shape
        nocc = occ.shape[2]
        nvir = vir.shape[2]
        width = trial.shape[3]
        half = rows // 2
        cols = 2 * rows
        turned = jnp.transpose(trial[0], (0, 2, 1))
        far = pl.BlockSpec(memory_space=pltpu.HBM)
        dma = pltpu.SemaphoreType.DMA
        operands = (minus, turned, occ[0], vir[0], coulomb, exch, occ_energy, vir_energy)
        result = pl.pallas_call(
            kernel,
            out_shape=jax.ShapeDtypeStruct((2, width, nocc), F32),
            in_specs=[far] * 8,
            out_specs=pl.BlockSpec(memory_space=pltpu.VMEM),
            scratch_shapes=[
                pltpu.SMEM((nk, nk), jnp.int32),
                pltpu.VMEM((2, width, nocc), F32),
                pltpu.VMEM((2, rows, nocc), BF),
                pltpu.VMEM((2, rows, nvir), BF),
                pltpu.VMEM((1, nocc), F32),
                pltpu.VMEM((1, width), F32),
                pltpu.VMEM((nocc, 128), F32),
                pltpu.VMEM((2, width, nocc), BF),
                pltpu.VMEM((2, nvir, nocc), BF),
                pltpu.VMEM((2, nvir, rows), BF),
                pltpu.VMEM((2, 2, half, nocc), BF),
                pltpu.VMEM((nk, half, nocc), BF),
                pltpu.VMEM((2, 4, chips // 2, bands // 2, 2 * rows // bands, nocc), BF),
                pltpu.VMEM((nk, half, cols), BF),
                pltpu.VMEM((nk, half, cols), BF),
                pltpu.VMEM((4, half, cols), BF),
                pltpu.VMEM((nk, half, nocc), BF),
                pltpu.VMEM((chips, 2, half, nocc), BF),
                pltpu.VMEM((2, rows, nocc), F32),
                pltpu.VMEM((chips, 8, rows), F32),
                pltpu.VMEM((bands, 8, rows), F32),
                pltpu.VMEM((rows, aux), BF),
                pltpu.VMEM((2, nvir, nocc), BF),
                pltpu.VMEM((2, bands, width, nocc), BF),
                dma((2, 5)), dma((2, bands)), dma((2, 3)),
                dma((2,)), dma((2,)),
                dma((bands // 2,)), dma((chips // 2,)),
                dma((2, 3)), dma((2, 4)),
                dma((2, 3)), dma((2, bands // 2)),
                dma((4, 3)), dma((4, bands // 2)),
                dma((bands // 2, 3)), dma((4, bands // 2)),
                dma((8,)), dma((8,)),
                dma((2, 4)), dma((2, 4)), dma((2, chips)),
                dma((chips,)), dma((chips,)),
                dma((bands,)), dma((bands,)),
                dma((2, chips)), dma((2, chips)),
                dma((2, bands)), dma((2, bands)),
                dma((9,)),
            ],
            compiler_params=pltpu.CompilerParams(
                collective_id=0, has_side_effects=True, vmem_limit_bytes=48 * 1024 * 1024
            ),
            name="sigma",
        )(*[pltpu.with_memory_space_constraint(a, pltpu.HBM) for a in operands])
        return jnp.transpose(result, (0, 2, 1))[None]

    in_specs = (
        P("ka", "band", None),
        P("ka", "band", None),
        P("ka", None, None, "band"),
        P("ka", None),
        P("ka", "band"),
        P("band", None),
        P(None, "band", None),
        P(),
    )
    return jax.shard_map(
        per_device,
        mesh=mesh,
        in_specs=in_specs,
        out_specs=P("ka", None, None, "band"),
        check_vma=False,
    )
```

```python
import jax
import jax.numpy as jnp
from jax import lax
from jax.experimental import pallas as pl
from jax.experimental.pallas import tpu as pltpu
from jax.sharding import PartitionSpec as P

BF = jnp.bfloat16
F32 = jnp.float32
MESH = pl.DeviceIdType.MESH
ALONG = (((1,), (1,)), ((), ()))


def each(count, body):
    def step(i, carry):
        body(i)
        return carry

    lax.fori_loop(0, count, step, 0)


def rdma(src, dst, send, recv, ka, band):
    return pltpu.make_async_remote_copy(
        src_ref=src,
        dst_ref=dst,
        send_sem=send,
        recv_sem=recv,
        device_id={"ka": ka, "band": band},
        device_id_type=MESH,
    )


def kernel(
    minus_h, trial_h, occ_h, vir_h, coulomb, exch, occ_e_h, vir_e_h, out,
    minus, trial, occ, vir, occ_e, vir_e, turn, trial_bf, trial_all, vir_t, t_mine, t_all, occ_c, k_bf, pairs, s_bf,
    u_send, u_recv, acc_w, dens1, dens2, coul, sig_send, sig_recv,
    tri_s, tri_r, tri_f, x_s, x_r, o1_s, o1_r, ox_s, ox_r, oy_s, oy_r, fy_s, fy_r, fx_s, fx_r, o3_s, o3_r, t_s, f_s, t_r, d1_s, d1_r, d2_s, d2_r,
    u_s, u_r, g_s, g_r, loc,
):
    bands = lax.axis_size("band")
    chips = lax.axis_size("ka") // 2
    depth = chips // 2
    ka = lax.axis_index("ka")
    b = lax.axis_index("band")
    j = ka // 2
    c = lax.rem(ka, 2)
    o = 1 - c
    h = j // depth
    z = lax.rem(j, depth)
    side = bands // 2
    xl = b // side
    y = lax.rem(b, side)
    quarter = 2 * h + xl
    mine = 2 * j + c
    other = 2 * j + o
    rows, nocc = occ_h.shape
    half = rows // 2
    width = trial.shape[1]
    nk = exch.shape[0]
    slab = rows // side
    cols = pairs.shape[2]
    home = xl * side + z
    goal = h * depth + y
    partner = (1 - h) * depth + z

    def band_peer(i):
        return lax.rem(b + 1 + i, bands)

    def chip_peer(i):
        return lax.rem(j + 1 + i, chips)

    def block(start, size, unit=16):
        return pl.ds(pl.multiple_of(start, unit), size)

    loads = [
        pltpu.make_async_copy(occ_h, occ.at[c], loc.at[0]),
        pltpu.make_async_copy(trial_h, trial, loc.at[1]),
        pltpu.make_async_copy(vir_h, vir.at[c], loc.at[2]),
        pltpu.make_async_copy(
            exch.at[:, block(h * half, half), block(z * rows, rows, 128)], k_bf.at[:, :, pl.ds(0, rows)], loc.at[3]
        ),
        pltpu.make_async_copy(
            exch.at[:, block(h * half, half), block((z + side) * rows, rows, 128)],
            k_bf.at[:, :, pl.ds(rows, rows)], loc.at[8],
        ),
        pltpu.make_async_copy(minus_h, minus, loc.at[4]),
        pltpu.make_async_copy(coulomb, coul, loc.at[5]),
        pltpu.make_async_copy(occ_e_h, occ_e, loc.at[6]),
        pltpu.make_async_copy(vir_e_h, vir_e, loc.at[7]),
    ]
    for load in loads:
        load.start()

    barrier = pltpu.get_barrier_semaphore()

    def greet(k, band):
        pl.semaphore_signal(barrier, inc=1, device_id={"ka": k, "band": band}, device_id_type=MESH)

    def greet_band(i):
        greet(mine, band_peer(i))
        greet(other, band_peer(i))

    def deep(i):
        return h * depth + lax.rem(z + 1 + i, depth)

    each(bands - 1, greet_band)
    each(chips - 1, lambda i: greet(2 * chip_peer(i) + c, b))
    each(depth - 1, lambda i: greet(2 * deep(i) + c, home))
    greet(other, b)
    greet(2 * ((1 - h) * depth + z) + c, (1 - xl) * side + y)

    loads[0].wait()
    loads[1].wait()
    trial_bf[...] = trial[...].astype(BF)
    callers = 2 * (bands - 1) + (chips - 1) + 2
    pl.semaphore_wait(barrier, jnp.where(y == z, callers, callers + side))

    def occ1(i):
        return rdma(
            occ.at[c, block(i * slab, slab)], occ_c.at[c, quarter, z, i], o1_s.at[i], o1_r.at[z],
            2 * goal + c, xl * side + i,
        )

    def occ1_start(i):
        @pl.when((i != y) | (y != z))
        def _():
            occ1(i).start()

    each(side, occ1_start)

    @pl.when(y == z)
    def _():
        occ_c[c, quarter, z, y] = occ[c, block(y * slab, slab), :]

    own_cols = block(b * width, width)

    facing = (1 - xl) * side + y

    def beside(i):
        return xl * side + lax.rem(y + 1 + i, side)

    def behind(i):
        return (1 - xl) * side + lax.rem(y + 1 + i, side)

    def tri_copy(w, n, p):
        vector, chip_core = ((c, mine), (o, other))[w]
        return rdma(trial_bf.at[vector], trial_all.at[c, own_cols], tri_s.at[w, n], tri_r.at[c, b], chip_core, p)

    def tri_out(w, n):
        return tri_copy(w, n, (facing, beside(0), beside(1), beside(2), b)[n])

    tri_order = [(0, 0), (1, 0), (0, 1), (0, 2), (0, 3), (1, 1), (1, 2), (1, 3), (1, 4)]
    for w, n in tri_order[:5]:
        tri_out(w, n).start()
    loads[2].wait()
    send_vir = rdma(vir.at[c], vir.at[c], x_s.at[0], x_r.at[0], other, b)
    send_occ = rdma(occ.at[c], occ.at[c], x_s.at[1], x_r.at[1], other, b)
    send_vir.start()
    send_occ.start()
    for w, n in tri_order[5:]:
        tri_out(w, n).start()
    trial_all[c, own_cols, :] = trial_bf[c]

    def landed(dst, recv):
        rdma(dst, dst, x_s.at[0], recv, mine, b).wait_recv()

    def tri_piece(s, p):
        return trial_all.at[s, block(p * width, width)]

    def tri_landed(s, p):
        landed(tri_piece(s, p), tri_r.at[s, p])

    def tri_pass(s, i):
        return rdma(
            tri_piece(s, facing), tri_piece(s, facing), tri_f.at[s, i], tri_r.at[s, facing], mine, beside(i)
        )

    for s in (c, o):
        tri_landed(s, facing)
        for i in range(side - 1):
            tri_pass(s, i).start()

    def occ1_wait(i):
        @pl.when((i != z) | (y != z))
        def _():
            rdma(
                occ.at[c, block(y * slab, slab)], occ_c.at[c, quarter, i, y], o1_s.at[0], o1_r.at[i], mine, b
            ).wait_recv()

    each(depth, occ1_wait)

    def part_a(q, row):
        return occ_c.at[c, q, pl.ds(0, depth // 2), row]

    def part_b(q, row):
        return occ_c.at[c, q, pl.ds(depth // 2, depth // 2), row]

    def x_send(src, send, recv, i):
        q = quarter ^ (i + 1)
        return rdma(src, src, send, recv, 2 * ((q // 2) * depth + z) + c, lax.rem(q, 2) * side + y)

    def y_send(src, send, recv, i):
        return rdma(src, src, send, recv, mine, xl * side + lax.rem(y + 1 + i, side))

    parts = (part_a, part_b)

    def occ_x(n, i):
        return x_send(parts[n](quarter, y), ox_s.at[n, i], ox_r.at[n, quarter], i)

    def occ_y(n, i):
        return y_send(parts[n](quarter, y), oy_s.at[n, i], oy_r.at[n, y], i)

    def occ_xy(q, i):
        return y_send(part_a(q, y), fy_s.at[q, i], fy_r.at[q, y], i)

    def occ_yx(row, i):
        return x_send(part_b(quarter, row), fx_s.at[row, i], fx_r.at[quarter, row], i)

    for n in range(2):
        each(3, lambda i: occ_x(n, i).start())
        each(side - 1, lambda i: occ_y(1 - n, i).start())

    vir_t[c] = vir[c].T

    def t_copy(s, i):
        return rdma(t_mine.at[h, s], t_all.at[2 * j + s], t_s.at[s, i], t_r.at[s, j], 2 * deep(i) + c, b)

    def t_cross(s):
        return rdma(
            t_mine.at[1 - h, s], t_all.at[2 * j + s], t_s.at[s, depth - 1], t_r.at[s, j], 2 * partner + c, b
        )

    def t_forward(s, i):
        there = t_all.at[2 * partner + s]
        return rdma(there, there, f_s.at[s, i], t_r.at[s, partner], 2 * deep(i) + c, b)

    def t_landed(s, p):
        landed(t_all.at[2 * p + s], t_r.at[s, p])

    def t_make(s):
        products = []
        for e in (1 - h, h):
            part = block(e * half, half)
            value = jnp.dot(vir[s, part, :], trial_all[s], preferred_element_type=F32)
            t_mine[e, s] = value.astype(BF)
            if e is h:
                each(depth - 1, lambda i: t_copy(s, i).start())
                t_all[2 * j + s] = t_mine[h, s]
            else:
                t_cross(s).start()
            products.append(occ[s, part, :].astype(F32) * value)
        return products

    def tri_rest(s):
        for i in range(side - 1):
            tri_landed(s, beside(i))
            tri_landed(s, behind(i))

    tri_rest(c)
    local = t_make(c)
    rdma(vir.at[c], vir.at[o], x_s.at[0], x_r.at[0], other, b).wait_recv()
    rdma(occ.at[c], occ.at[o], x_s.at[1], x_r.at[1], other, b).wait_recv()
    tri_rest(o)
    tri_landed(o, b)
    local = [left + right for left, right in zip(local, t_make(o))]

    ones = jnp.ones((8, nocc), BF)
    for e, products in zip((1 - h, h), local):
        high = products.astype(BF)
        low = (products - high.astype(F32)).astype(BF)
        dens1[j, :, block(e * half, half, 128)] = lax.dot_general(
            ones, high, ALONG, preferred_element_type=F32
        ) + lax.dot_general(ones, low, ALONG, preferred_element_type=F32)

    def d1_copy(i):
        return rdma(dens1.at[j], dens1.at[j], d1_s.at[i], d1_r.at[j], 2 * chip_peer(i) + c, b)

    each(chips - 1, lambda i: d1_copy(i).start())

    def x_arrived(i):
        q = quarter ^ (i + 1)
        landed(part_a(q, y), ox_r.at[0, q])
        each(side - 1, lambda n: occ_xy(q, n).start())

    def y_arrived(i):
        row = lax.rem(y + 1 + i, side)
        landed(part_b(quarter, row), oy_r.at[1, row])
        each(3, lambda n: occ_yx(row, n).start())

    each(3, x_arrived)
    each(side - 1, y_arrived)

    def second_halves(i):
        row = lax.rem(y + 1 + i, side)
        landed(part_a(quarter, row), oy_r.at[0, row])

    def t_pass(s):
        t_landed(s, partner)
        each(depth - 1, lambda i: t_forward(s, i).start())

    t_pass(c)

    def occ3(n):
        q = quarter ^ (n // 2)
        there = occ_c.at[c, q, pl.ds(lax.rem(n, 2) * (depth // 2), depth // 2)]
        return rdma(there, there, o3_s.at[n], o3_r.at[n], other, b)

    each(side - 1, second_halves)
    occ3(0).start()
    occ3(1).start()
    t_pass(o)

    vir_t[o] = vir[o].T
    turn[...] = jnp.zeros_like(turn)
    loads[7].wait()
    loads[8].wait()
    turn[:, 0:width] = jnp.broadcast_to(vir_e[...], (nocc, width))
    gaps = turn[...].T[0:width] - occ_e[...]
    for v in range(2):
        out[v] = gaps * trial[v]

    def occ_rest(i):
        q = quarter ^ (i + 1)

        def from_y(n):
            row = lax.rem(y + 1 + n, side)
            landed(part_a(q, row), fy_r.at[q, row])

        def from_x(n):
            row = lax.rem(y + 1 + n, side)
            landed(part_b(q, row), fx_r.at[q, row])

        each(side - 1, from_y)
        occ3(2 * i + 2).start()
        each(side - 1, from_x)
        landed(part_b(q, y), ox_r.at[1, q])
        occ3(2 * i + 3).start()

    each(3, occ_rest)

    def d1_wait(i):
        p = chip_peer(i)
        rdma(dens1.at[p], dens1.at[p], d1_s.at[i], d1_r.at[p], 2 * p + c, b).wait_recv()

    each(chips - 1, d1_wait)
    total = dens1[0]
    for p in range(1, chips):
        total = total + dens1[p]
    dens2[b] = total

    def d2_copy(i):
        return rdma(dens2.at[b], dens2.at[b], d2_s.at[i], d2_r.at[b], mine, band_peer(i))

    each(bands - 1, lambda i: d2_copy(i).start())

    def t_rest(i):
        near = deep(i)
        far = lax.rem(near + depth, chips)
        for s in range(2):
            t_landed(s, near)
            t_landed(s, far)

    each(depth - 1, t_rest)

    def points_of(p, s, e):
        return occ_c[s, 2 * (p // depth) + e, lax.rem(p, depth)].reshape(rows, nocc)

    def pairs_of(s, column):
        for n in range(depth):
            p = column * depth + n
            for e in range(2):
                pairs[2 * p + s, :, e * rows : (e + 1) * rows] = lax.dot_general(
                    t_all[2 * p + s], points_of(p, s, e), ALONG, preferred_element_type=F32
                ).astype(BF)

    pairs_of(c, h)
    pairs_of(c, 1 - h)

    def occ3_wait(n):
        q = quarter ^ (n // 2)
        landed(occ_c.at[o, q, pl.ds(lax.rem(n, 2) * (depth // 2), depth // 2)], o3_r.at[n])

    each(4, occ3_wait)
    pairs_of(o, h)
    each(4, lambda n: occ3_wait(n + 4))

    pairs_of(o, 1 - h)
    loads[3].wait()
    loads[4].wait()
    loads[5].wait()

    tile = 16

    def u_copy(dest, s):
        return rdma(u_send.at[2 * dest + s], u_recv.at[j, s], u_s.at[s, dest], u_r.at[s, j], 2 * dest + c, b)

    def screen(offsets, s):
        dests = [j ^ m for m in offsets]

        def rows_step(r):
            for t in range(2):
                part = block((r * 2 + t) * tile, tile)
                for n, dest in enumerate(dests):
                    acc = jnp.zeros((tile, cols), F32)
                    for q in range(nk):
                        source = minus[2 * dest + s, q]
                        acc = acc + pairs[source, part, :].astype(F32) * k_bf[q, part, :].astype(F32)
                    s_bf[n, part, :] = acc.astype(BF)

        each(half // tile // 2, rows_step)
        sums = []
        for n, dest in enumerate(dests):
            left = jnp.dot(s_bf[n, :, :rows], points_of(dest, s, 0), preferred_element_type=F32)
            sums.append(left + jnp.dot(s_bf[n, :, rows:], points_of(dest, s, 1), preferred_element_type=F32))
        for n, dest in enumerate(dests):
            if offsets[n]:
                u_send[2 * dest + s] = sums[n].astype(BF)
                u_copy(dest, s).start()
            else:
                u_recv[j, s] = sums[n].astype(BF)

    def finish(s):
        def u_landed(i):
            p = chip_peer(i)
            landed(u_recv.at[p, s], u_r.at[s, p])

        each(chips - 1, u_landed)
        sides = []
        for e in range(2):
            total = u_recv[e * depth, s].astype(F32)
            for p in range(1, depth):
                total = total + u_recv[e * depth + p, s].astype(F32)
            sides.append((acc_w[s, e * half : (e + 1) * half, :] - total).astype(BF))
        weight = jnp.concatenate(sides, axis=0)
        for column in (1 - xl, xl):
            part = block(column * side * width, side * width)
            sig_send[s, part, :] = jnp.dot(vir_t[s, part, :], weight, preferred_element_type=F32).astype(BF)
            for n in range(side - 1, -1, -1):
                if column is xl and n == 0:
                    continue
                sig_copy(s, column * side + (y ^ n)).start()

        @pl.when(c == s)
        def _():
            sig_recv[c, b] = sig_send[s, own_cols, :]

        @pl.when(c != s)
        def _():
            sig_copy(s, b).start()

    def sig_copy(s, p):
        return rdma(
            sig_send.at[s, block(p * width, width)], sig_recv.at[c, b], g_s.at[s, p], g_r.at[c, b], 2 * j + s, p
        )

    for s in range(2):
        for m in range(depth - 1, -1, -1):
            screen((depth + m, m), s)

    def d2_wait(i):
        p = band_peer(i)
        rdma(dens2.at[p], dens2.at[p], d2_s.at[i], d2_r.at[p], mine, p).wait_recv()

    each(bands - 1, d2_wait)
    loads[6].wait()
    pot = jnp.zeros((rows, nocc), F32)
    for p in range(bands):
        line = jnp.broadcast_to(dens2[p][0:1, :].astype(BF), (nocc, rows))
        pot = pot + lax.dot_general(coul[:, p * rows : (p + 1) * rows], line, ALONG, preferred_element_type=F32)
    pot = pot * 2.0
    for s in range(2):
        acc_w[s] = pot * occ[s].astype(F32)

    finish(0)
    for w, n in tri_order:
        tri_out(w, n).wait_send()
    for s in range(2):
        for i in range(side - 1):
            tri_pass(s, i).wait_send()

    def occ1_sent(i):
        @pl.when((i != y) | (y != z))
        def _():
            occ1(i).wait_send()

    each(side, occ1_sent)
    send_vir.wait_send()
    send_occ.wait_send()
    for n in range(2):
        each(3, lambda i: occ_x(n, i).wait_send())
        each(side - 1, lambda i: occ_y(n, i).wait_send())

    def forwarded(i):
        each(side - 1, lambda n: occ_xy(quarter ^ (i + 1), n).wait_send())
        each(3, lambda n: occ_yx(lax.rem(y + 1 + i, side), n).wait_send())

    each(3, forwarded)
    each(8, lambda n: occ3(n).wait_send())
    each(chips - 1, lambda i: d1_copy(i).wait_send())
    each(bands - 1, lambda i: d2_copy(i).wait_send())
    for s in range(2):
        each(depth - 1, lambda i: t_copy(s, i).wait_send())
        t_cross(s).wait_send()
        each(depth - 1, lambda i: t_forward(s, i).wait_send())

    finish(1)

    def sig_sent(s):
        for n in range(1, bands):
            sig_copy(s, b ^ n).wait_send()

        @pl.when(c != s)
        def _():
            sig_copy(s, b).wait_send()

    for s in range(2):
        each(chips - 1, lambda i: u_copy(chip_peer(i), s).wait_send())
    sig_sent(0)

    def sig_wait_same(i):
        p = band_peer(i)
        rdma(sig_send.at[0, own_cols], sig_recv.at[c, p], g_s.at[0, i], g_r.at[c, p], mine, p).wait_recv()

    def sig_wait_cross(i):
        rdma(sig_send.at[0, own_cols], sig_recv.at[o, i], g_s.at[1, i], g_r.at[o, i], other, i).wait_recv()

    each(bands - 1, sig_wait_same)
    each(bands, sig_wait_cross)
    for v in range(2):
        sums = sig_recv[v, 0].astype(F32)
        for p in range(1, bands):
            sums = sums + sig_recv[v, p].astype(F32)
        out[v] = out[v] + sums

    sig_sent(1)


def solution(mesh):
    bands = mesh.shape["band"]
    chips = mesh.shape["ka"] // 2

    def per_device(occ, vir, trial, occ_energy, vir_energy, coulomb, exch, minus):
        nk, rows, aux = exch.shape
        nocc = occ.shape[2]
        nvir = vir.shape[2]
        width = trial.shape[3]
        half = rows // 2
        cols = 2 * rows
        turned = jnp.transpose(trial[0], (0, 2, 1))
        far = pl.BlockSpec(memory_space=pltpu.HBM)
        dma = pltpu.SemaphoreType.DMA
        operands = (minus, turned, occ[0], vir[0], coulomb, exch, occ_energy, vir_energy)
        result = pl.pallas_call(
            kernel,
            out_shape=jax.ShapeDtypeStruct((2, width, nocc), F32),
            in_specs=[far] * 8,
            out_specs=pl.BlockSpec(memory_space=pltpu.VMEM),
            scratch_shapes=[
                pltpu.SMEM((nk, nk), jnp.int32),
                pltpu.VMEM((2, width, nocc), F32),
                pltpu.VMEM((2, rows, nocc), BF),
                pltpu.VMEM((2, rows, nvir), BF),
                pltpu.VMEM((1, nocc), F32),
                pltpu.VMEM((1, width), F32),
                pltpu.VMEM((nocc, 128), F32),
                pltpu.VMEM((2, width, nocc), BF),
                pltpu.VMEM((2, nvir, nocc), BF),
                pltpu.VMEM((2, nvir, rows), BF),
                pltpu.VMEM((2, 2, half, nocc), BF),
                pltpu.VMEM((nk, half, nocc), BF),
                pltpu.VMEM((2, 4, chips // 2, bands // 2, 2 * rows // bands, nocc), BF),
                pltpu.VMEM((nk, half, cols), BF),
                pltpu.VMEM((nk, half, cols), BF),
                pltpu.VMEM((4, half, cols), BF),
                pltpu.VMEM((nk, half, nocc), BF),
                pltpu.VMEM((chips, 2, half, nocc), BF),
                pltpu.VMEM((2, rows, nocc), F32),
                pltpu.VMEM((chips, 8, rows), F32),
                pltpu.VMEM((bands, 8, rows), F32),
                pltpu.VMEM((rows, aux), BF),
                pltpu.VMEM((2, nvir, nocc), BF),
                pltpu.VMEM((2, bands, width, nocc), BF),
                dma((2, 5)), dma((2, bands)), dma((2, 3)),
                dma((2,)), dma((2,)),
                dma((bands // 2,)), dma((chips // 2,)),
                dma((2, 3)), dma((2, 4)),
                dma((2, 3)), dma((2, bands // 2)),
                dma((4, 3)), dma((4, bands // 2)),
                dma((bands // 2, 3)), dma((4, bands // 2)),
                dma((8,)), dma((8,)),
                dma((2, 4)), dma((2, 4)), dma((2, chips)),
                dma((chips,)), dma((chips,)),
                dma((bands,)), dma((bands,)),
                dma((2, chips)), dma((2, chips)),
                dma((2, bands)), dma((2, bands)),
                dma((9,)),
            ],
            compiler_params=pltpu.CompilerParams(
                collective_id=0, has_side_effects=True, vmem_limit_bytes=48 * 1024 * 1024
            ),
            name="sigma",
        )(*[pltpu.with_memory_space_constraint(a, pltpu.HBM) for a in operands])
        return jnp.transpose(result, (0, 2, 1))[None]

    in_specs = (
        P("ka", "band", None),
        P("ka", "band", None),
        P("ka", None, None, "band"),
        P("ka", None),
        P("ka", "band"),
        P("band", None),
        P(None, "band", None),
        P(),
    )
    return jax.shard_map(
        per_device,
        mesh=mesh,
        in_specs=in_specs,
        out_specs=P("ka", None, None, "band"),
        check_vma=False,
    )
```
